32 devices in a mesh: sector: 8 (over z, y), ops: 4 (over x, core).
Axes of the slice: x: 2, y: 2, z: 4, core: 2. Of those that a mesh axis runs over, the one named last changes fastest.
Arguments:
- wavefunction: float32 [8, 640, 640], P('sector'), may hold values from -160 to 160
- left_env: float32 [8, 16, 640, 640], P('sector', 'ops'), may hold values from -0.25 to 0.25
- right_env: float32 [8, 16, 640, 640], P('sector', 'ops'), may hold values from -0.25 to 0.25
- shift_map: int32 [4, 8], P('ops'), may hold values from 0 to 7, each once within a row
- op_counts: int32 [4, 8], P('ops', 'sector'), may hold values from 1 to 4
Outputs:
- updated_tensor: float32 [8, 640, 640], P('sector', None, 'ops')
- rotated_env: float32 [8, 16, 640, 640], P('sector', 'ops')
The draws below stay inside these ranges and needn't reach their ends.
Inputs may be any that keep to these rules, and one draw needn't show every extreme that they name: `shift_map`: each row lists every sector once.
All inputs are finite; a program needn't handle non-finite values.
Results may differ from the reference program's by a relative error of at most 0.0003.
Values sent between devices are 32-bit elements; how exact they have to be, the bound alone decides.
A program may use at most 128 MiB of HBM per device.

```python
import math
import jax
import jax.numpy as jnp
from jax import lax

MS = 640
OPS_DEV = 4
POLAR = 5
NSEC = 8
GROUPS = 4
OPS = 16


def draw_wavefunction(key, part):
    key_base = jax.random.fold_in(key, 11)
    sector_level = jnp.arange(NSEC, dtype=jnp.float32) / float(NSEC - 1)
    base_draw = jnp.clip(jax.random.normal(key_base, (NSEC, MS, MS), jnp.float32), -6.0, 6.0)
    sector_scale = 3.0 ** sector_level
    return base_draw * sector_scale[:, None, None]


def touch_ends(entries, rng, smallest, high):
    spot = [jax.random.randint(jax.random.fold_in(rng, axis), (), 0, length) for axis, length in enumerate(entries.shape)]
    main_axis = entries.shape.index(max(entries.shape))
    next_to = spot[:main_axis] + [(spot[main_axis] + 1) % entries.shape[main_axis]] + spot[main_axis + 1:]
    return entries.at[tuple(spot)].set(smallest).at[tuple(next_to)].set(high)


def levels(stream_key, extent, cuts, least, top_value):
    level = 1.0
    for dim, shards_of in cuts:
        heights = jax.random.uniform(jax.random.fold_in(jax.random.fold_in(stream_key, 6), dim), (shards_of,), jnp.float32, least / len(cuts), top_value / len(cuts))
        level = level * jnp.repeat(jnp.exp(heights), extent[dim] // shards_of).reshape((-1,) + (1,) * (len(extent) - 1 - dim))
    return level


def scatter_about(rng, dims, deviation, limit, cuts=(), kind=jnp.bfloat16):
    result = deviation * jax.random.normal(rng, dims, jnp.float32)
    if cuts:
        result = result * levels(rng, dims, cuts, -0.22, 0.18)
    return jnp.clip(result, -limit, limit).astype(kind)


def setup_inputs(seed: int = 0) -> dict:
    seeds = jax.random.split(jax.random.key(seed), 6)
    wavefunction = draw_wavefunction(jax.random.fold_in(seeds[5], 71), 0)
    left_env = scatter_about(seeds[1], (NSEC, OPS, MS, MS), MS ** -0.5, 0.25, ((0, 8), (1, 4)), jnp.float32)
    right_env = scatter_about(seeds[2], (NSEC, OPS, MS, MS), MS ** -0.5, 0.25, ((0, 8), (1, 4)), jnp.float32)
    shift_map = jax.vmap(lambda own: jax.random.permutation(own, NSEC))(jax.random.split(seeds[3], GROUPS)).reshape((GROUPS, NSEC)).astype(jnp.int32)
    op_counts = touch_ends(jax.random.randint(seeds[4], (GROUPS, NSEC), 1, OPS_DEV + 1), jax.random.fold_in(seeds[4], 1), 1, OPS_DEV).astype(jnp.int32)
    return {"wavefunction": wavefunction, "left_env": left_env, "right_env": right_env, "shift_map": shift_map, "op_counts": op_counts}


precise = lax.Precision.HIGHEST

def reference(wavefunction, left_env, right_env, shift_map, op_counts):
    sector_ids = jnp.arange(NSEC, dtype=jnp.int32)
    slots = jnp.arange(OPS, dtype=jnp.int32) % OPS_DEV

    def sector_sigma(sector_id):
        sources = shift_map[:, sector_id]
        blocks = jnp.repeat(wavefunction[sources], OPS_DEV, axis=0)
        limits = jnp.repeat(op_counts[:, sector_id], OPS_DEV, axis=0)
        active = (slots < limits).astype(jnp.float32)
        left_psi = jnp.einsum('wab,wbc->wac', left_env[sector_id], blocks, precision=precise)
        op_terms = jnp.einsum('wac,wcd->wad', left_psi, right_env[sector_id], precision=precise)
        return jnp.einsum('w,wad->ad', active, op_terms, precision=precise)
    sigma = lax.map(sector_sigma, sector_ids)
    mean_sq = lax.optimization_barrier(jnp.sum(sigma * sigma, axis=(1, 2))) / float(MS * MS)
    factor = lax.rsqrt(MS * mean_sq + 1e-06) / 2.2
    iterate = sigma * factor[:, None, None]
    for repeat_index in range(POLAR):
        gram_matrix = jnp.einsum('sab,scb->sac', iterate, iterate, precision=precise)
        iterate = 1.5 * iterate - 0.5 * jnp.einsum('sac,scb->sab', gram_matrix, iterate, precision=precise)
    updated = iterate * math.sqrt(MS)

    def rotate(sector_id):
        sources = shift_map[:, sector_id]
        rights = jnp.repeat(updated[sources], OPS_DEV, axis=0)
        half_rotated = jnp.einsum('ba,wbc->wac', updated[sector_id], left_env[sector_id], precision=precise)
        return jnp.einsum('wac,wcd->wad', half_rotated, rights, precision=precise)
    rotated = lax.map(rotate, sector_ids)
    return (updated, rotated)
```

```python
import functools
import math

import jax
import jax.numpy as jnp
from jax import lax
from jax.experimental import pallas as pl
from jax.experimental.pallas import tpu as pltpu
from jax.sharding import PartitionSpec as P

POLAR = 5
LANES, SUBLANES = 128, 8
CORES = 2
MESH = pl.DeviceIdType.MESH
F32, BF16 = jnp.float32, jnp.bfloat16

precise = lax.Precision.HIGH


def dot(a, b):
    return jnp.dot(a, b, precision=precise, preferred_element_type=jnp.float32)


def to_tiles(block, padded):
    rows, cols = block.shape
    tiles = block.reshape(rows // SUBLANES, SUBLANES, cols // LANES, LANES)
    tiles = tiles.transpose(0, 2, 1, 3).reshape(rows * cols // (SUBLANES * LANES), SUBLANES, LANES)
    return jnp.pad(tiles, ((0, padded - tiles.shape[0]), (0, 0), (0, 0)))


def from_tiles(tiles, rows, cols):
    tiles = tiles[: rows * cols // (SUBLANES * LANES)]
    tiles = tiles.reshape(rows // SUBLANES, cols // LANES, SUBLANES, LANES)
    return tiles.transpose(0, 2, 1, 3).reshape(rows, cols)


def swap(value, axis, bit):
    size = lax.axis_size(axis)
    return lax.ppermute(value, axis, [(i, i ^ bit) for i in range(size)])


def sum_scatter(tiles, axis):
    size, here = lax.axis_size(axis), lax.axis_index(axis)
    rest = tiles.reshape((size, tiles.shape[0] // size) + tiles.shape[1:])
    bit = 1
    while bit < size:
        mine = (here // bit) % 2
        pairs = rest.reshape((rest.shape[0] // 2, 2) + rest.shape[1:])
        keep = lax.dynamic_index_in_dim(pairs, mine, 1, keepdims=False)
        give = lax.dynamic_index_in_dim(pairs, 1 - mine, 1, keepdims=False)
        rest = keep + swap(give, axis, bit)
        bit *= 2
    return rest[0]


def gather_whole(quarter, axis):
    size, here = lax.axis_size(axis), lax.axis_index(axis)
    held = quarter[None]
    bit = size // 2
    while bit:
        mine = (here // bit) % 2
        other = swap(held, axis, bit)
        first = jnp.where(mine == 0, held, other)
        second = jnp.where(mine == 0, other, held)
        held = jnp.stack([first, second], axis=1).reshape((-1,) + quarter.shape)
        bit //= 2
    return held.reshape((-1,) + quarter.shape[1:])


def polar(sigma_block):
    states = sigma_block.shape[0]
    mean_sq = jnp.sum(sigma_block * sigma_block) / float(states * states)
    iterate = sigma_block * (lax.rsqrt(states * mean_sq + 1e-06) / 2.2)

    def step(_, iterate):
        gram_matrix = jnp.einsum("ab,cb->ac", iterate, iterate, precision=precise)
        return 1.5 * iterate - 0.5 * dot(gram_matrix, iterate)

    return lax.fori_loop(0, POLAR, step, iterate) * math.sqrt(states)


def shards_general(wavefunction, left_env, right_env, shift_map, op_counts):
    sector_count = lax.axis_size("sector")
    group_size = lax.axis_size("ops")
    group_here = lax.axis_index("ops")
    states = wavefunction.shape[1]
    ops_here = left_env.shape[1]
    parts = sector_count * group_size
    piece = -(-states * states // (SUBLANES * LANES * parts))
    padded = piece * parts
    quarter = piece * sector_count

    whole_map = lax.all_gather(shift_map[0], "ops").reshape(parts)

    def fetch_from_quarter(own_quarter):
        pieces = own_quarter.reshape(sector_count, piece, SUBLANES, LANES)
        spread = lax.all_to_all(pieces, "sector", split_axis=0, concat_axis=0, tiled=True)
        picked = jnp.take(spread, whole_map, axis=0)
        landed = lax.all_to_all(picked, ("ops", "sector"), split_axis=0, concat_axis=0, tiled=True)
        return from_tiles(landed.reshape(padded, SUBLANES, LANES), states, states)

    psi_tiles = to_tiles(wavefunction[0], padded)
    psi_quarter = lax.dynamic_slice_in_dim(psi_tiles, group_here * quarter, quarter, 0)
    moved_block = fetch_from_quarter(psi_quarter)

    left, right = left_env[0], right_env[0]
    count = op_counts[0, 0]
    active = (jnp.arange(ops_here) < count).astype(jnp.float32)
    left_psi = jnp.einsum("wab,bc->wac", left, moved_block, precision=precise) * active[:, None, None]
    partial_sigma = jnp.einsum("wac,wcd->ad", left_psi, right, precision=precise)

    sigma_quarter = sum_scatter(to_tiles(partial_sigma, padded), "ops")
    source_sigma = fetch_from_quarter(sigma_quarter)
    sigma_block = from_tiles(gather_whole(sigma_quarter, "ops"), states, states)

    whole_tensor = polar(sigma_block)
    column_width = states // group_size
    own_columns = lax.dynamic_slice_in_dim(whole_tensor, group_here * column_width, column_width, 1)
    half_rotated = jnp.einsum("ba,wbc->wac", whole_tensor, left, precision=precise)
    source_tensor = polar(source_sigma)
    rotated = jnp.einsum("wac,cd->wad", half_rotated, source_tensor, precision=precise)
    return (own_columns[None], rotated[None])


def halves(value):
    high = value.astype(BF16)
    return high, (value - high.astype(F32)).astype(BF16)


def bdot(a, b):
    return jnp.dot(a, b, preferred_element_type=F32)


class Place:
    def __init__(self, nsec, nops, ny, states):
        self.nsec, self.nops, self.ny, self.nz = nsec, nops, ny, nsec // ny
        self.states = states
        self.chunks = states // LANES
        self.parts = nops * ny
        self.rows = states // self.parts
        self.quarter = states // nops
        self.dests = nops * ny

    def locate(self):
        self.s, self.o = lax.axis_index("sector"), lax.axis_index("ops")
        self.z, self.y = self.s // self.ny, lax.rem(self.s, self.ny)
        self.part = self.o * self.ny + self.y

    def plane_peer(self, index, sign=1):
        dy, do = index // self.nops, index % self.nops
        if sign < 0:
            dy, do = (self.ny - dy) % self.ny, (self.nops - do) % self.nops
        return lax.rem(self.y + dy, self.ny), lax.rem(self.o + do, self.nops)

    def greet(self):
        barrier = pltpu.get_barrier_semaphore()
        for index in range(1, self.dests):
            y, o = self.plane_peer(index)
            pl.semaphore_signal(barrier, inc=1, device_id=(self.z * self.ny + y, o), device_id_type=MESH)

        @pl.when(self.z > 0)
        def _():
            pl.semaphore_signal(barrier, inc=1, device_id=(self.s - self.ny, self.o), device_id_type=MESH)

        @pl.when(self.z < self.nz - 1)
        def _():
            pl.semaphore_signal(barrier, inc=1, device_id=(self.s + self.ny, self.o), device_id_type=MESH)

        line = (self.z > 0).astype(jnp.int32) + (self.z < self.nz - 1).astype(jnp.int32)
        pl.semaphore_wait(barrier, self.dests - 1 + line)


class Maps:
    def __init__(self, place, own_ref, rows_ref, scalars_ref, sems):
        self.place, self.own, self.rows, self.scalars, self.sems = place, own_ref, rows_ref, scalars_ref, sems

    @staticmethod
    def scratch(place):
        return [
            pltpu.VMEM((place.nops, 1, LANES), jnp.int32),
            pltpu.SMEM((place.nops, 1, LANES), jnp.int32),
            pltpu.SemaphoreType.DMA((3, place.nops)),
        ]

    def copy(self, offset, sign):
        p = self.place
        peer = lax.rem(p.o + offset, p.nops)
        slot = p.o if sign > 0 else lax.rem(p.o + p.nops - offset, p.nops)
        return pltpu.make_async_remote_copy(
            self.own, self.rows.at[slot], self.sems.at[0, offset], self.sems.at[1, offset],
            device_id=(p.s, peer), device_id_type=MESH)

    def start(self):
        for offset in range(1, self.place.nops):
            self.copy(offset, 1).start()
        pltpu.make_async_copy(self.own, self.rows.at[self.place.o], self.sems.at[2, 0]).start()

    def finish(self):
        for offset in range(1, self.place.nops):
            self.copy(offset, 1).wait_send()
            self.copy(offset, -1).wait_recv()
        pltpu.make_async_copy(self.own, self.rows.at[self.place.o], self.sems.at[2, 0]).wait()
        landed = pltpu.make_async_copy(self.rows, self.scalars, self.sems.at[2, 1])
        landed.start()
        landed.wait()

    def want(self, y, o):
        return self.scalars[o, 0, self.place.z * self.place.ny + y]


class Fetch:
    def __init__(self, place, maps, piece, held, stage, landed, up, down, across, within, local):
        self.place, self.maps, self.piece = place, maps, piece
        self.held, self.stage, self.landed = held, stage, landed
        self.up, self.down, self.across, self.within, self.local = up, down, across, within, local

    @staticmethod
    def scratch(place):
        c, dma = place.chunks, pltpu.SemaphoreType.DMA
        return (
            [pltpu.VMEM((place.nsec, place.rows, LANES), F32) for _ in range(c)],
            pltpu.VMEM((c, place.dests, place.rows, LANES), F32),
            dma((2, c, place.nz - 1)),
            dma((2, c, place.nz - 1)),
            dma((2, c, place.ny)),
            dma((2, c, place.dests)),
            dma((c,)),
        )

    def across_copy(self, j, dy, sign):
        p = self.place
        y = lax.rem(p.y + dy, p.ny)
        slot = p.s if sign > 0 else p.z * p.ny + lax.rem(p.y + p.ny - dy, p.ny)
        return pltpu.make_async_remote_copy(
            self.piece(j, y), self.held[j].at[slot], self.across.at[0, j, dy], self.across.at[1, j, dy],
            device_id=(p.z * p.ny + y, p.o), device_id_type=MESH)

    def own_copy(self, j):
        p = self.place
        return pltpu.make_async_copy(self.piece(j, p.y), self.held[j].at[p.s], self.local.at[j])

    def begin(self, j):
        for dy in range(1, self.place.ny):
            self.across_copy(j, dy, 1).start()
        self.own_copy(j).start()

    def line_copy(self, j, k, direction):
        p = self.place
        slab = self.held[j].at[pl.ds((p.z - direction * k) * p.ny, p.ny)]
        sems = self.up if direction > 0 else self.down
        return pltpu.make_async_remote_copy(
            slab, slab, sems.at[0, j, k], sems.at[1, j, k],
            device_id=(p.s + direction * p.ny, p.o), device_id_type=MESH)

    def line_wait(self, j, k, direction):
        p = self.place
        slab = self.held[j].at[pl.ds((p.z - direction * k) * p.ny, p.ny)]
        sems = self.up if direction > 0 else self.down
        pltpu.make_async_remote_copy(
            slab, slab, sems.at[0, j, k - 1], sems.at[1, j, k - 1],
            device_id=(p.s - direction * p.ny, p.o), device_id_type=MESH).wait_recv()

    def has(self, k, direction):
        return self.place.z >= k if direction > 0 else self.place.z < self.place.nz - k

    def more(self, direction):
        return self.place.z < self.place.nz - 1 if direction > 0 else self.place.z > 0

    def send_own(self, j):
        for dy in range(1, self.place.ny):
            self.across_copy(j, dy, -1).wait_recv()
        self.own_copy(j).wait()
        for direction in (1, -1):
            @pl.when(self.more(direction))
            def _():
                self.line_copy(j, 0, direction).start()

    def forward(self, j, k):
        for direction in (1, -1):
            @pl.when(self.has(k, direction))
            def _():
                self.line_wait(j, k, direction)

            if k < self.place.nz - 1:
                @pl.when(self.has(k, direction) & self.more(direction))
                def _():
                    self.line_copy(j, k, direction).start()

    def within_copy(self, j, index, sign):
        p = self.place
        y, o = p.plane_peer(index, sign)
        part = p.part if sign > 0 else o * p.ny + y
        return pltpu.make_async_remote_copy(
            self.stage.at[j, index], self.landed.at[j, pl.ds(part * p.rows, p.rows)],
            self.within.at[0, j, index], self.within.at[1, j, index],
            device_id=(p.z * p.ny + y, o), device_id_type=MESH)

    def hand_out(self, j):
        p = self.place
        order = sorted(range(p.dests), key=lambda index: -((index // p.nops > 0) + (index % p.nops > 0)))
        for index in order:
            y, o = p.plane_peer(index)
            picked = self.held[j][self.maps.want(y, o)]
            if index == 0:
                self.landed[j, pl.ds(p.part * p.rows, p.rows)] = picked
            else:
                self.stage[j, index] = picked
                self.within_copy(j, index, 1).start()

    def receive(self, j):
        for index in range(1, self.place.dests):
            self.within_copy(j, index, -1).wait_recv()

    def drain(self):
        for j in range(self.place.chunks):
            for dy in range(1, self.place.ny):
                self.across_copy(j, dy, 1).wait_send()
            for direction in (1, -1):
                for k in range(self.place.nz - 1):
                    @pl.when(self.has(k, direction) & self.more(direction))
                    def _():
                        self.line_copy(j, k, direction).wait_send()
            for index in range(1, self.place.dests):
                self.within_copy(j, index, 1).wait_send()


def sigma_kernel(place, ops_here, psi, left, right, own_map, counts, out, rows, scalars, map_sems, *rest):
    c, n = place.chunks, place.states
    held, (stage, up, down, across, within, local), rest = rest[:c], rest[c:c + 6], rest[c + 6:]
    landed, lefts, rights, block, envs, env_sems, lp_high, lp_low, sigma, first, second, pair, sum_sems = rest
    place.locate()
    p = place

    loads = [(left, w, lefts) for w in range(ops_here)] + [(right, w, rights) for w in range(ops_here)]

    def load(i):
        ref, w, _ = loads[i]
        return pltpu.make_async_copy(ref.at[w], envs.at[i % 2], env_sems.at[i % 2])

    load(0).start()
    load(1).start()
    place.greet()
    maps = Maps(place, own_map, rows, scalars, map_sems)
    fetch = Fetch(
        place, maps,
        lambda j, y: psi.at[pl.ds((p.o * p.ny + y) * p.rows, p.rows), pl.ds(j * LANES, LANES)],
        held, stage, landed, up, down, across, within, local)
    maps.start()
    for j in range(c):
        fetch.begin(j)
    maps.finish()
    for j in range(c):
        fetch.send_own(j)
    count = counts[0, 0]
    sigma[...] = jnp.zeros((n, n), F32)
    block[pl.ds(n, n), pl.ds(LANES, LANES)] = jnp.zeros((n, LANES), BF16)

    def convert(i):
        _, w, kind = loads[i]
        load(i).wait()
        value = envs[i % 2]
        if kind is lefts:
            value = value * (w < count).astype(F32)
        high, low = halves(value)
        if kind is lefts:
            lefts[pl.ds(w * n, n), pl.ds(0, n)] = high
            lefts[pl.ds(w * n, n), pl.ds(n, n)] = low
        else:
            for j in range(c):
                rights[j, pl.ds(w * LANES, LANES), pl.ds(0, n)] = high[j * LANES:(j + 1) * LANES]
                rights[j, pl.ds(w * LANES, LANES), pl.ds(n, n)] = low[j * LANES:(j + 1) * LANES]
        if i + 2 < len(loads):
            load(i + 2).start()

    todo = list(range(len(loads)))
    for k in range(1, p.nz - 1):
        if k == 1:
            for j in range(c):
                fetch.forward(j, k)
                if todo:
                    convert(todo.pop(0))
    while todo:
        convert(todo.pop(0))

    def products(j):
        high, low = halves(landed[j])
        block[pl.ds(0, n), pl.ds(0, LANES)] = high
        block[pl.ds(n, n), pl.ds(0, LANES)] = high
        block[pl.ds(0, n), pl.ds(LANES, LANES)] = low
        for w in range(ops_here):
            both = bdot(lefts[pl.ds(w * n, n)], block[...])
            high, low = halves(both[:, :LANES] + both[:, LANES:])
            lp_high[:, pl.ds(w * LANES, LANES)] = high
            lp_low[:, pl.ds(w * LANES, LANES)] = low
        both = bdot(lp_high[...], rights[j])
        sigma[...] += both[:, :n] + (both[:, n:] + bdot(lp_low[...], rights[j, :, pl.ds(0, n)]))

    for j in range(c):
        for k in range(2, p.nz):
            fetch.forward(j, k)
        fetch.hand_out(j)
        if j:
            fetch.receive(j - 1)
            products(j - 1)
    fetch.receive(c - 1)
    products(c - 1)

    side, core = p.o // CORES, lax.rem(p.o, CORES)
    mate = side * CORES + 1 - core
    facing = (1 - side) * CORES + core
    q = p.quarter

    def swap_cores(i, far):
        rows_of = (far * CORES + 1 - core) * q
        return pltpu.make_async_remote_copy(
            sigma.at[pl.ds(rows_of, q)], first.at[i], sum_sems.at[0, i], sum_sems.at[1, i],
            device_id=(p.s, mate), device_id_type=MESH)

    for i, far in ((0, 1 - side), (1, side)):
        swap_cores(i, far).start()
    swap_cores(0, 1 - side).wait_recv()
    pair[...] = sigma[pl.ds(((1 - side) * CORES + core) * q, q)] + first[0]
    over = pltpu.make_async_remote_copy(
        pair, second, sum_sems.at[0, 2], sum_sems.at[1, 2], device_id=(p.s, facing), device_id_type=MESH)
    over.start()
    swap_cores(1, side).wait_recv()
    over.wait_recv()
    out[...] = sigma[pl.ds(p.o * q, q)] + first[1] + second[...]
    fetch.drain()
    for i, far in ((0, 1 - side), (1, side)):
        swap_cores(i, far).wait_send()
    over.wait_send()


def vmem():
    return pl.BlockSpec(memory_space=pltpu.VMEM)


def sigma_quarter_of(place, psi, left, right, shift_map, op_counts):
    c, n, ops_here = place.chunks, place.states, left.shape[0]
    held, stage, *sems = Fetch.scratch(place)
    own_map = jnp.pad(shift_map, ((0, 0), (0, LANES - shift_map.shape[1])))
    return pl.pallas_call(
        functools.partial(sigma_kernel, place, ops_here),
        out_shape=jax.ShapeDtypeStruct((place.quarter, n), F32),
        in_specs=[vmem(), pl.BlockSpec(memory_space=pl.ANY), pl.BlockSpec(memory_space=pl.ANY), vmem(),
                  pl.BlockSpec(memory_space=pltpu.SMEM)],
        out_specs=vmem(),
        scratch_shapes=[
            *Maps.scratch(place), *held, stage, *sems,
            pltpu.VMEM((c, n, LANES), F32),
            pltpu.VMEM((ops_here * n, 2 * n), BF16),
            pltpu.VMEM((c, ops_here * LANES, 2 * n), BF16),
            pltpu.VMEM((2 * n, 2 * LANES), BF16),
            pltpu.VMEM((2, n, n), F32),
            pltpu.SemaphoreType.DMA((2,)),
            pltpu.VMEM((n, ops_here * LANES), BF16),
            pltpu.VMEM((n, ops_here * LANES), BF16),
            pltpu.VMEM((n, n), F32),
            pltpu.VMEM((2, place.quarter, n), F32),
            pltpu.VMEM((place.quarter, n), F32),
            pltpu.VMEM((place.quarter, n), F32),
            pltpu.SemaphoreType.DMA((2, 3)),
        ],
        compiler_params=pltpu.CompilerParams(collective_id=0, has_side_effects=True, vmem_limit_bytes=60 * 2**20),
    )(psi, left, right, own_map, op_counts)


def shards_planes(place, wavefunction, left_env, right_env, shift_map, op_counts):
    sector_count = lax.axis_size("sector")
    group_size = lax.axis_size("ops")
    group_here = lax.axis_index("ops")
    states = wavefunction.shape[1]
    left, right = left_env[0], right_env[0]
    quarter_rows = sigma_quarter_of(place, wavefunction[0], left, right, shift_map, op_counts)

    parts = sector_count * group_size
    piece = -(-states * states // (SUBLANES * LANES * parts))
    padded = piece * parts
    whole_map = lax.all_gather(shift_map[0], "ops").reshape(parts)
    sigma_block = lax.all_gather(quarter_rows, "ops").reshape(states, states)
    quarter = piece * sector_count
    sq = lax.dynamic_slice_in_dim(to_tiles(sigma_block, padded), group_here * quarter, quarter, 0)
    pieces = sq.reshape(sector_count, piece, SUBLANES, LANES)
    spread = lax.all_to_all(pieces, "sector", split_axis=0, concat_axis=0, tiled=True)
    picked = jnp.take(spread, whole_map, axis=0)
    landed = lax.all_to_all(picked, ("ops", "sector"), split_axis=0, concat_axis=0, tiled=True)
    source_sigma = from_tiles(landed.reshape(padded, SUBLANES, LANES), states, states)

    whole_tensor = polar(sigma_block)
    column_width = states // group_size
    own_columns = lax.dynamic_slice_in_dim(whole_tensor, group_here * column_width, column_width, 1)
    half_rotated = jnp.einsum("ba,wbc->wac", whole_tensor, left, precision=precise)
    source_tensor = polar(source_sigma)
    rotated = jnp.einsum("wac,cd->wad", half_rotated, source_tensor, precision=precise)
    return (own_columns[None], rotated[None])


def line_split(sector_count):
    rows = 1
    while rows * 2 * rows * 2 <= sector_count and sector_count % (rows * 2) == 0:
        rows *= 2
    return rows


def solution(mesh):
    def shards(wavefunction, left_env, right_env, shift_map, op_counts):
        nsec, nops = mesh.shape["sector"], mesh.shape["ops"]
        states = wavefunction.shape[1]
        ny = line_split(nsec)
        fits = nops == 2 * CORES and ny == 2 and states % LANES == 0 and states % (nops * ny * SUBLANES) == 0
        if not fits:
            return shards_general(wavefunction, left_env, right_env, shift_map, op_counts)
        place = Place(nsec, nops, ny, states)
        return shards_planes(place, wavefunction, left_env, right_env, shift_map, op_counts)

    return jax.shard_map(
        shards,
        mesh=mesh,
        in_specs=(
            P("sector", None, None),
            P("sector", "ops", None, None),
            P("sector", "ops", None, None),
            P("ops", None),
            P("ops", "sector"),
        ),
        out_specs=(P("sector", None, "ops"), P("sector", "ops", None, None)),
        check_vma=False,
    )
```

```python
import functools
import math

import jax
import jax.numpy as jnp
from jax import lax
from jax.experimental import pallas as pl
from jax.experimental.pallas import tpu as pltpu
from jax.sharding import PartitionSpec as P

POLAR = 5
LANES, SUBLANES = 128, 8
CORES = 2
MESH = pl.DeviceIdType.MESH
F32, BF16 = jnp.float32, jnp.bfloat16

precise = lax.Precision.HIGH


def dot(a, b):
    return jnp.dot(a, b, precision=precise, preferred_element_type=jnp.float32)


def to_tiles(block, padded):
    rows, cols = block.shape
    tiles = block.reshape(rows // SUBLANES, SUBLANES, cols // LANES, LANES)
    tiles = tiles.transpose(0, 2, 1, 3).reshape(rows * cols // (SUBLANES * LANES), SUBLANES, LANES)
    return jnp.pad(tiles, ((0, padded - tiles.shape[0]), (0, 0), (0, 0)))


def from_tiles(tiles, rows, cols):
    tiles = tiles[: rows * cols // (SUBLANES * LANES)]
    tiles = tiles.reshape(rows // SUBLANES, cols // LANES, SUBLANES, LANES)
    return tiles.transpose(0, 2, 1, 3).reshape(rows, cols)


def swap(value, axis, bit):
    size = lax.axis_size(axis)
    return lax.ppermute(value, axis, [(i, i ^ bit) for i in range(size)])


def sum_scatter(tiles, axis):
    size, here = lax.axis_size(axis), lax.axis_index(axis)
    rest = tiles.reshape((size, tiles.shape[0] // size) + tiles.shape[1:])
    bit = 1
    while bit < size:
        mine = (here // bit) % 2
        pairs = rest.reshape((rest.shape[0] // 2, 2) + rest.shape[1:])
        keep = lax.dynamic_index_in_dim(pairs, mine, 1, keepdims=False)
        give = lax.dynamic_index_in_dim(pairs, 1 - mine, 1, keepdims=False)
        rest = keep + swap(give, axis, bit)
        bit *= 2
    return rest[0]


def gather_whole(quarter, axis):
    size, here = lax.axis_size(axis), lax.axis_index(axis)
    held = quarter[None]
    bit = size // 2
    while bit:
        mine = (here // bit) % 2
        other = swap(held, axis, bit)
        first = jnp.where(mine == 0, held, other)
        second = jnp.where(mine == 0, other, held)
        held = jnp.stack([first, second], axis=1).reshape((-1,) + quarter.shape)
        bit //= 2
    return held.reshape((-1,) + quarter.shape[1:])


def polar(sigma_block):
    states = sigma_block.shape[0]
    mean_sq = jnp.sum(sigma_block * sigma_block) / float(states * states)
    iterate = sigma_block * (lax.rsqrt(states * mean_sq + 1e-06) / 2.2)

    def step(_, iterate):
        gram_matrix = jnp.einsum("ab,cb->ac", iterate, iterate, precision=precise)
        return 1.5 * iterate - 0.5 * dot(gram_matrix, iterate)

    return lax.fori_loop(0, POLAR, step, iterate) * math.sqrt(states)


def shards_general(wavefunction, left_env, right_env, shift_map, op_counts):
    sector_count = lax.axis_size("sector")
    group_size = lax.axis_size("ops")
    group_here = lax.axis_index("ops")
    states = wavefunction.shape[1]
    ops_here = left_env.shape[1]
    parts = sector_count * group_size
    piece = -(-states * states // (SUBLANES * LANES * parts))
    padded = piece * parts
    quarter = piece * sector_count

    whole_map = lax.all_gather(shift_map[0], "ops").reshape(parts)

    def fetch_from_quarter(own_quarter):
        pieces = own_quarter.reshape(sector_count, piece, SUBLANES, LANES)
        spread = lax.all_to_all(pieces, "sector", split_axis=0, concat_axis=0, tiled=True)
        picked = jnp.take(spread, whole_map, axis=0)
        landed = lax.all_to_all(picked, ("ops", "sector"), split_axis=0, concat_axis=0, tiled=True)
        return from_tiles(landed.reshape(padded, SUBLANES, LANES), states, states)

    psi_tiles = to_tiles(wavefunction[0], padded)
    psi_quarter = lax.dynamic_slice_in_dim(psi_tiles, group_here * quarter, quarter, 0)
    moved_block = fetch_from_quarter(psi_quarter)

    left, right = left_env[0], right_env[0]
    count = op_counts[0, 0]
    active = (jnp.arange(ops_here) < count).astype(jnp.float32)
    left_psi = jnp.einsum("wab,bc->wac", left, moved_block, precision=precise) * active[:, None, None]
    partial_sigma = jnp.einsum("wac,wcd->ad", left_psi, right, precision=precise)

    sigma_quarter = sum_scatter(to_tiles(partial_sigma, padded), "ops")
    source_sigma = fetch_from_quarter(sigma_quarter)
    sigma_block = from_tiles(gather_whole(sigma_quarter, "ops"), states, states)

    whole_tensor = polar(sigma_block)
    column_width = states // group_size
    own_columns = lax.dynamic_slice_in_dim(whole_tensor, group_here * column_width, column_width, 1)
    half_rotated = jnp.einsum("ba,wbc->wac", whole_tensor, left, precision=precise)
    source_tensor = polar(source_sigma)
    rotated = jnp.einsum("wac,cd->wad", half_rotated, source_tensor, precision=precise)
    return (own_columns[None], rotated[None])


def halves(value):
    high = value.astype(BF16)
    return high, (value - high.astype(F32)).astype(BF16)


def bdot(a, b):
    return jnp.dot(a, b, preferred_element_type=F32)


class Place:
    def __init__(self, nsec, nops, ny, states):
        self.nsec, self.nops, self.ny, self.nz = nsec, nops, ny, nsec // ny
        self.states = states
        self.chunks = states // LANES
        self.parts = nops * ny
        self.rows = states // self.parts
        self.quarter = states // nops
        self.dests = nops * ny

    def locate(self):
        self.s, self.o = lax.axis_index("sector"), lax.axis_index("ops")
        self.z, self.y = self.s // self.ny, lax.rem(self.s, self.ny)
        self.part = self.o * self.ny + self.y

    def plane_peer(self, index, sign=1):
        dy, do = index // self.nops, index % self.nops
        if sign < 0:
            dy, do = (self.ny - dy) % self.ny, (self.nops - do) % self.nops
        return lax.rem(self.y + dy, self.ny), lax.rem(self.o + do, self.nops)

    def greet(self):
        barrier = pltpu.get_barrier_semaphore()
        for index in range(1, self.dests):
            y, o = self.plane_peer(index)
            pl.semaphore_signal(barrier, inc=1, device_id=(self.z * self.ny + y, o), device_id_type=MESH)

        @pl.when(self.z > 0)
        def _():
            pl.semaphore_signal(barrier, inc=1, device_id=(self.s - self.ny, self.o), device_id_type=MESH)

        @pl.when(self.z < self.nz - 1)
        def _():
            pl.semaphore_signal(barrier, inc=1, device_id=(self.s + self.ny, self.o), device_id_type=MESH)

        line = (self.z > 0).astype(jnp.int32) + (self.z < self.nz - 1).astype(jnp.int32)
        pl.semaphore_wait(barrier, self.dests - 1 + line)


class Maps:
    def __init__(self, place, own_ref, rows_ref, scalars_ref, sems):
        self.place, self.own, self.rows, self.scalars, self.sems = place, own_ref, rows_ref, scalars_ref, sems

    @staticmethod
    def scratch(place):
        return [
            pltpu.VMEM((place.nops, 1, LANES), jnp.int32),
            pltpu.SMEM((place.nops, 1, LANES), jnp.int32),
            pltpu.SemaphoreType.DMA((3, place.nops)),
        ]

    def copy(self, offset, sign):
        p = self.place
        peer = lax.rem(p.o + offset, p.nops)
        slot = p.o if sign > 0 else lax.rem(p.o + p.nops - offset, p.nops)
        return pltpu.make_async_remote_copy(
            self.own, self.rows.at[slot], self.sems.at[0, offset], self.sems.at[1, offset],
            device_id=(p.s, peer), device_id_type=MESH)

    def start(self):
        for offset in range(1, self.place.nops):
            self.copy(offset, 1).start()
        pltpu.make_async_copy(self.own, self.rows.at[self.place.o], self.sems.at[2, 0]).start()

    def finish(self):
        for offset in range(1, self.place.nops):
            self.copy(offset, 1).wait_send()
            self.copy(offset, -1).wait_recv()
        pltpu.make_async_copy(self.own, self.rows.at[self.place.o], self.sems.at[2, 0]).wait()
        landed = pltpu.make_async_copy(self.rows, self.scalars, self.sems.at[2, 1])
        landed.start()
        landed.wait()

    def want(self, y, o):
        return self.scalars[o, 0, self.place.z * self.place.ny + y]


class Fetch:
    def __init__(self, place, maps, piece, held, stage, landed, up, down, across, within, local):
        self.place, self.maps, self.piece = place, maps, piece
        self.held, self.stage, self.landed = held, stage, landed
        self.up, self.down, self.across, self.within, self.local = up, down, across, within, local

    @staticmethod
    def scratch(place):
        c, dma = place.chunks, pltpu.SemaphoreType.DMA
        return (
            [pltpu.VMEM((place.nsec, place.rows, LANES), F32) for _ in range(c)],
            pltpu.VMEM((c, place.dests, place.rows, LANES), F32),
            dma((2, c, place.nz - 1)),
            dma((2, c, place.nz - 1)),
            dma((2, c, place.ny)),
            dma((2, c, place.dests)),
            dma((c,)),
        )

    def across_copy(self, j, dy, sign):
        p = self.place
        y = lax.rem(p.y + dy, p.ny)
        slot = p.s if sign > 0 else p.z * p.ny + lax.rem(p.y + p.ny - dy, p.ny)
        return pltpu.make_async_remote_copy(
            self.piece(j, y), self.held[j].at[slot], self.across.at[0, j, dy], self.across.at[1, j, dy],
            device_id=(p.z * p.ny + y, p.o), device_id_type=MESH)

    def own_copy(self, j):
        p = self.place
        return pltpu.make_async_copy(self.piece(j, p.y), self.held[j].at[p.s], self.local.at[j])

    def begin(self, j):
        for dy in range(1, self.place.ny):
            self.across_copy(j, dy, 1).start()
        self.own_copy(j).start()

    def line_copy(self, j, k, direction):
        p = self.place
        slab = self.held[j].at[pl.ds((p.z - direction * k) * p.ny, p.ny)]
        sems = self.up if direction > 0 else self.down
        return pltpu.make_async_remote_copy(
            slab, slab, sems.at[0, j, k], sems.at[1, j, k],
            device_id=(p.s + direction * p.ny, p.o), device_id_type=MESH)

    def line_wait(self, j, k, direction):
        p = self.place
        slab = self.held[j].at[pl.ds((p.z - direction * k) * p.ny, p.ny)]
        sems = self.up if direction > 0 else self.down
        pltpu.make_async_remote_copy(
            slab, slab, sems.at[0, j, k - 1], sems.at[1, j, k - 1],
            device_id=(p.s - direction * p.ny, p.o), device_id_type=MESH).wait_recv()

    def has(self, k, direction):
        return self.place.z >= k if direction > 0 else self.place.z < self.place.nz - k

    def more(self, direction):
        return self.place.z < self.place.nz - 1 if direction > 0 else self.place.z > 0

    def send_own(self, j):
        for dy in range(1, self.place.ny):
            self.across_copy(j, dy, -1).wait_recv()
        self.own_copy(j).wait()
        for direction in (1, -1):
            @pl.when(self.more(direction))
            def _():
                self.line_copy(j, 0, direction).start()

    def forward(self, j, k):
        for direction in (1, -1):
            @pl.when(self.has(k, direction))
            def _():
                self.line_wait(j, k, direction)

            if k < self.place.nz - 1:
                @pl.when(self.has(k, direction) & self.more(direction))
                def _():
                    self.line_copy(j, k, direction).start()

    def within_copy(self, j, index, sign):
        p = self.place
        y, o = p.plane_peer(index, sign)
        part = p.part if sign > 0 else o * p.ny + y
        return pltpu.make_async_remote_copy(
            self.stage.at[j, index], self.landed.at[j, pl.ds(part * p.rows, p.rows)],
            self.within.at[0, j, index], self.within.at[1, j, index],
            device_id=(p.z * p.ny + y, o), device_id_type=MESH)

    def hand_out(self, j):
        p = self.place
        order = sorted(range(p.dests), key=lambda index: -((index // p.nops > 0) + (index % p.nops > 0)))
        for index in order:
            y, o = p.plane_peer(index)
            picked = self.held[j][self.maps.want(y, o)]
            if index == 0:
                self.landed[j, pl.ds(p.part * p.rows, p.rows)] = picked
            else:
                self.stage[j, index] = picked
                self.within_copy(j, index, 1).start()

    def receive(self, j):
        for index in range(1, self.place.dests):
            self.within_copy(j, index, -1).wait_recv()

    def drain(self):
        for j in range(self.place.chunks):
            for dy in range(1, self.place.ny):
                self.across_copy(j, dy, 1).wait_send()
            for direction in (1, -1):
                for k in range(self.place.nz - 1):
                    @pl.when(self.has(k, direction) & self.more(direction))
                    def _():
                        self.line_copy(j, k, direction).wait_send()
            for index in range(1, self.place.dests):
                self.within_copy(j, index, 1).wait_send()


def tdot(a, b):
    return lax.dot_general(a, b, (((1,), (1,)), ((), ())), preferred_element_type=F32)


class Polar:
    def __init__(self, n, block, cols, rows, gram):
        self.n, self.block, self.cols, self.rows, self.gram = n, block, cols, rows, gram

    @staticmethod
    def scratch(n):
        return [pltpu.VMEM((n, 2 * n), BF16), pltpu.VMEM((2 * n, n), BF16), pltpu.VMEM((2 * n, n), BF16)]

    def normalise(self, sigma):
        n = self.n
        squares = jnp.sum(jnp.sum(sigma * sigma, axis=0, keepdims=True), axis=1, keepdims=True)
        self.block[...] = sigma * (lax.rsqrt(n * (squares / float(n * n)) + 1e-06) / 2.2)

    def form_gram(self):
        n = self.n
        high, low = halves(self.block[...])
        self.cols[:, pl.ds(0, n)] = high
        self.cols[:, pl.ds(n, n)] = low
        self.rows[pl.ds(0, n)] = high
        self.rows[pl.ds(n, n)] = low
        both = tdot(high, self.rows[...])
        cross = both[:, n:]
        self.gram[pl.ds(0, n)], self.gram[pl.ds(n, n)] = halves(both[:, :n] + (cross + cross.T))

    def apply(self, scale=None):
        n = self.n
        both = bdot(self.gram[pl.ds(0, n)], self.cols[...])
        moved = both[:, :n] + (both[:, n:] + bdot(self.gram[pl.ds(n, n)], self.cols[:, pl.ds(0, n)]))
        value = 1.5 * self.block[...] - 0.5 * moved
        self.block[...] = value if scale is None else value * scale


def site_kernel(place, ops_here, psi, left, right, own_map, counts, own_columns, half_out, source_out, rows, scalars,
                map_sems, *rest):
    c, n = place.chunks, place.states
    groups = []
    for _ in range(2):
        groups.append((rest[:c], rest[c:c + 6], rest[c + 6]))
        rest = rest[c + 7:]
    (lefts, rights, block, envs, env_sems, lp_high, lp_low, sigma, first, second, pair, sum_sems,
     quarter, gather_sems, polar_block, cols, doubled, gram, out_sems) = rest
    place.locate()
    p = place

    loads = [(left, w, lefts) for w in range(ops_here)] + [(right, w, rights) for w in range(ops_here)]

    def load(i):
        ref, w, _ = loads[i]
        return pltpu.make_async_copy(ref.at[w], envs.at[i % 2], env_sems.at[i % 2])

    load(0).start()
    load(1).start()
    place.greet()
    maps = Maps(place, own_map, rows, scalars, map_sems)

    def fetch_of(piece, group):
        held, (stage, up, down, across, within, local), landed = group
        return Fetch(place, maps, piece, held, stage, landed, up, down, across, within, local)

    fetch = fetch_of(lambda j, y: psi.at[pl.ds((p.o * p.ny + y) * p.rows, p.rows), pl.ds(j * LANES, LANES)], groups[0])
    again = fetch_of(lambda j, y: quarter.at[pl.ds(y * p.rows, p.rows), pl.ds(j * LANES, LANES)], groups[1])
    maps.start()
    for j in range(c):
        fetch.begin(j)
    maps.finish()
    for j in range(c):
        fetch.send_own(j)
    count = counts[0, 0]
    sigma[...] = jnp.zeros((n, n), F32)
    block[pl.ds(n, n), pl.ds(LANES, LANES)] = jnp.zeros((n, LANES), BF16)

    def convert(i):
        _, w, kind = loads[i]
        load(i).wait()
        value = envs[i % 2]
        if kind is rights:
            value = value * (w < count).astype(F32)
        high, low = halves(value)
        if kind is lefts:
            lefts[pl.ds(w * n, n), pl.ds(0, n)] = high
            lefts[pl.ds(w * n, n), pl.ds(n, n)] = low
        else:
            for j in range(c):
                at = pl.ds((j * ops_here + w) * LANES, LANES)
                rights[at, pl.ds(0, n)] = high[j * LANES:(j + 1) * LANES]
                rights[at, pl.ds(n, n)] = low[j * LANES:(j + 1) * LANES]
        if i + 2 < len(loads):
            load(i + 2).start()

    todo = list(range(len(loads)))
    for j in range(c):
        fetch.forward(j, 1)
        if todo:
            convert(todo.pop(0))
    while todo:
        convert(todo.pop(0))

    def products(j):
        high, low = halves(fetch.landed[j])
        block[pl.ds(0, n), pl.ds(0, LANES)] = high
        block[pl.ds(n, n), pl.ds(0, LANES)] = high
        block[pl.ds(0, n), pl.ds(LANES, LANES)] = low
        for w in range(ops_here):
            both = bdot(lefts[pl.ds(w * n, n)], block[...])
            high, low = halves(both[:, :LANES] + both[:, LANES:])
            lp_high[:, pl.ds(w * LANES, LANES)] = high
            lp_low[:, pl.ds(w * LANES, LANES)] = low
        deep = pl.ds(j * ops_here * LANES, ops_here * LANES)
        both = bdot(lp_high[...], rights[deep])
        sigma[...] += both[:, :n] + (both[:, n:] + bdot(lp_low[...], rights[deep, pl.ds(0, n)]))

    for j in range(c):
        for k in range(2, p.nz):
            fetch.forward(j, k)
        fetch.hand_out(j)
        if j:
            fetch.receive(j - 1)
            products(j - 1)
    fetch.receive(c - 1)
    products(c - 1)

    side, core = p.o // CORES, lax.rem(p.o, CORES)
    mate = side * CORES + 1 - core
    facing = (1 - side) * CORES + core
    across_mate = (1 - side) * CORES + 1 - core
    q = p.quarter

    def swap_cores(i, far):
        rows_of = (far * CORES + 1 - core) * q
        return pltpu.make_async_remote_copy(
            sigma.at[pl.ds(rows_of, q)], first.at[i], sum_sems.at[0, i], sum_sems.at[1, i],
            device_id=(p.s, mate), device_id_type=MESH)

    for i, far in ((0, 1 - side), (1, side)):
        swap_cores(i, far).start()
    swap_cores(0, 1 - side).wait_recv()
    pair[...] = sigma[pl.ds(((1 - side) * CORES + core) * q, q)] + first[0]
    over = pltpu.make_async_remote_copy(
        pair, second, sum_sems.at[0, 2], sum_sems.at[1, 2], device_id=(p.s, facing), device_id_type=MESH)
    over.start()
    swap_cores(1, side).wait_recv()
    over.wait_recv()
    quarter[...] = sigma[pl.ds(p.o * q, q)] + first[1] + second[...]
    for i, far in ((0, 1 - side), (1, side)):
        swap_cores(i, far).wait_send()
    over.wait_send()

    whole = polar_block
    polar = Polar(n, whole, cols, doubled, gram)

    def gather(i, sender, target):
        rows_of = pl.ds(sender * q, q)
        source = quarter if i < 2 else whole.at[rows_of]
        return pltpu.make_async_remote_copy(
            source, whole.at[rows_of], gather_sems.at[0, i], gather_sems.at[1, i],
            device_id=(p.s, target), device_id_type=MESH)

    gather(1, p.o, facing).start()
    gather(0, p.o, mate).start()
    for j in range(c):
        again.begin(j)
    whole[pl.ds(p.o * q, q)] = quarter[...]
    for j in range(c):
        again.send_own(j)
    gather(1, facing, facing).wait_recv()
    gather(2, facing, mate).start()
    for j in range(c):
        again.forward(j, 1)
    gather(0, mate, mate).wait_recv()
    gather(2, across_mate, mate).wait_recv()
    gather(2, facing, mate).wait_send()
    polar.normalise(whole[...])

    def pass_on(i):
        if i < c:
            for k in range(2, p.nz - 1):
                again.forward(i, k)
        if 0 < i <= c:
            again.forward(i - 1, p.nz - 1)
            again.hand_out(i - 1)

    events = list(range(c + 1))
    for step in range(POLAR):
        polar.form_gram()
        if events:
            pass_on(events.pop(0))
        polar.apply(math.sqrt(n) if step == POLAR - 1 else None)

    for side_of in range(p.nops):
        @pl.when(p.o == side_of)
        def _():
            own_columns[...] = whole[:, pl.ds(side_of * q, q)]

    gram[pl.ds(0, n)], gram[pl.ds(n, n)] = halves(whole[...].T)
    for w in range(ops_here):
        at = pl.ds(w * n, n)
        both = bdot(gram[pl.ds(0, n)], lefts[at])
        turned = both[:, :n] + (both[:, n:] + bdot(gram[pl.ds(n, n)], lefts[at, pl.ds(0, n)]))
        rights[at, pl.ds(0, n)], rights[at, pl.ds(n, n)] = halves(turned)
        pltpu.make_async_copy(rights.at[at], half_out.at[at], out_sems.at[w]).start()
        if events:
            pass_on(events.pop(0))
    while events:
        pass_on(events.pop(0))
    for j in range(c):
        again.receive(j)
    save = pltpu.make_async_copy(again.landed, source_out, out_sems.at[ops_here])
    save.start()
    for w in range(ops_here):
        at = pl.ds(w * n, n)
        pltpu.make_async_copy(rights.at[at], half_out.at[at], out_sems.at[w]).wait()
    fetch.drain()
    again.drain()
    gather(1, p.o, facing).wait_send()
    gather(0, p.o, mate).wait_send()
    save.wait()


def last_kernel(n, ops_here, chunks, source, half, columns, own_columns, rotated, block, cols, doubled, gram, halves_in,
                products, in_sems, out_sems):
    def load(w):
        at = pl.ds(w * n, n)
        return pltpu.make_async_copy(half.at[at], halves_in.at[at], in_sems.at[w])

    def store(w):
        return pltpu.make_async_copy(products.at[w], rotated.at[w], out_sems.at[w])

    for w in range(ops_here):
        load(w).start()
    own_columns[...] = columns[...]
    polar = Polar(n, block, cols, doubled, gram)
    polar.normalise(jnp.concatenate([source[j] for j in range(chunks)], axis=1))

    def step(_, carry):
        polar.form_gram()
        polar.apply()
        return carry

    lax.fori_loop(0, POLAR, step, 0)
    high, low = halves(block[...] * math.sqrt(n))
    cols[:, pl.ds(0, n)] = high
    cols[:, pl.ds(n, n)] = low
    for w in range(ops_here):
        load(w).wait()
        at = pl.ds(w * n, n)
        both = bdot(halves_in[at, pl.ds(0, n)], cols[...])
        products[w] = both[:, :n] + (both[:, n:] + bdot(halves_in[at, pl.ds(n, n)], cols[:, pl.ds(0, n)]))
        store(w).start()
    for w in range(ops_here):
        store(w).wait()


def vmem():
    return pl.BlockSpec(memory_space=pltpu.VMEM)


def anywhere():
    return pl.BlockSpec(memory_space=pl.ANY)


def shards_planes(place, wavefunction, left_env, right_env, shift_map, op_counts):
    c, n, q, ops_here = place.chunks, place.states, place.quarter, left_env.shape[1]
    own_map = jnp.pad(shift_map, ((0, 0), (0, LANES - shift_map.shape[1])))
    fetches = []
    for _ in range(2):
        held, stage, *sems = Fetch.scratch(place)
        fetches += [*held, stage, *sems, pltpu.VMEM((c, n, LANES), F32)]
    columns, half, source = pl.pallas_call(
        functools.partial(site_kernel, place, ops_here),
        out_shape=(
            jax.ShapeDtypeStruct((n, q), F32),
            jax.ShapeDtypeStruct((ops_here * n, 2 * n), BF16),
            jax.ShapeDtypeStruct((c, n, LANES), F32),
        ),
        in_specs=[vmem(), anywhere(), anywhere(), vmem(), pl.BlockSpec(memory_space=pltpu.SMEM)],
        out_specs=(vmem(), anywhere(), anywhere()),
        scratch_shapes=[
            *Maps.scratch(place), *fetches,
            pltpu.VMEM((ops_here * n, 2 * n), BF16),
            pltpu.VMEM((ops_here * n, 2 * n), BF16),
            pltpu.VMEM((2 * n, 2 * LANES), BF16),
            pltpu.VMEM((2, n, n), F32),
            pltpu.SemaphoreType.DMA((2,)),
            pltpu.VMEM((n, ops_here * LANES), BF16),
            pltpu.VMEM((n, ops_here * LANES), BF16),
            pltpu.VMEM((n, n), F32),
            pltpu.VMEM((2, q, n), F32),
            pltpu.VMEM((q, n), F32),
            pltpu.VMEM((q, n), F32),
            pltpu.SemaphoreType.DMA((2, 3)),
            pltpu.VMEM((q, n), F32),
            pltpu.SemaphoreType.DMA((2, 3)),
            pltpu.VMEM((n, n), F32),
            *Polar.scratch(n),
            pltpu.SemaphoreType.DMA((ops_here + 1,)),
        ],
        compiler_params=pltpu.CompilerParams(collective_id=0, has_side_effects=True, vmem_limit_bytes=60 * 2**20),
    )(wavefunction[0], left_env[0], right_env[0], own_map, op_counts)
    own_columns, rotated = pl.pallas_call(
        functools.partial(last_kernel, n, ops_here, c),
        out_shape=(jax.ShapeDtypeStruct((n, q), F32), jax.ShapeDtypeStruct((ops_here, n, n), F32)),
        in_specs=[vmem(), anywhere(), vmem()],
        out_specs=(vmem(), anywhere()),
        scratch_shapes=[
            pltpu.VMEM((n, n), F32),
            *Polar.scratch(n),
            pltpu.VMEM((ops_here * n, 2 * n), BF16),
            pltpu.VMEM((ops_here, n, n), F32),
            pltpu.SemaphoreType.DMA((ops_here,)),
            pltpu.SemaphoreType.DMA((ops_here,)),
        ],
        compiler_params=pltpu.CompilerParams(vmem_limit_bytes=60 * 2**20),
    )(source, half, columns)
    return own_columns[None], rotated[None]


def line_split(sector_count):
    rows = 1
    while rows * 2 * rows * 2 <= sector_count and sector_count % (rows * 2) == 0:
        rows *= 2
    return rows


def solution(mesh):
    def shards(wavefunction, left_env, right_env, shift_map, op_counts):
        nsec, nops = mesh.shape["sector"], mesh.shape["ops"]
        states = wavefunction.shape[1]
        ny = line_split(nsec)
        fits = nops == 2 * CORES and ny == 2 and states % LANES == 0 and states % (nops * ny * SUBLANES) == 0
        if not fits:
            return shards_general(wavefunction, left_env, right_env, shift_map, op_counts)
        place = Place(nsec, nops, ny, states)
        return shards_planes(place, wavefunction, left_env, right_env, shift_map, op_counts)

    return jax.shard_map(
        shards,
        mesh=mesh,
        in_specs=(
            P("sector", None, None),
            P("sector", "ops", None, None),
            P("sector", "ops", None, None),
            P("ops", None),
            P("ops", "sector"),
        ),
        out_specs=(P("sector", None, "ops"), P("sector", "ops", None, None)),
        check_vma=False,
    )
```

```python
import functools
import math

import jax
import jax.numpy as jnp
from jax import lax
from jax.experimental import pallas as pl
from jax.experimental.pallas import tpu as pltpu
from jax.sharding import PartitionSpec as P

POLAR = 5
LANES, SUBLANES = 128, 8
CORES = 2
AHEAD = 3
MESH = pl.DeviceIdType.MESH
F32, BF16 = jnp.float32, jnp.bfloat16

precise = lax.Precision.HIGH


def dot(a, b):
    return jnp.dot(a, b, precision=precise, preferred_element_type=jnp.float32)


def to_tiles(block, padded):
    rows, cols = block.shape
    tiles = block.reshape(rows // SUBLANES, SUBLANES, cols // LANES, LANES)
    tiles = tiles.transpose(0, 2, 1, 3).reshape(rows * cols // (SUBLANES * LANES), SUBLANES, LANES)
    return jnp.pad(tiles, ((0, padded - tiles.shape[0]), (0, 0), (0, 0)))


def from_tiles(tiles, rows, cols):
    tiles = tiles[: rows * cols // (SUBLANES * LANES)]
    tiles = tiles.reshape(rows // SUBLANES, cols // LANES, SUBLANES, LANES)
    return tiles.transpose(0, 2, 1, 3).reshape(rows, cols)


def swap(value, axis, bit):
    size = lax.axis_size(axis)
    return lax.ppermute(value, axis, [(i, i ^ bit) for i in range(size)])


def sum_scatter(tiles, axis):
    size, here = lax.axis_size(axis), lax.axis_index(axis)
    rest = tiles.reshape((size, tiles.shape[0] // size) + tiles.shape[1:])
    bit = 1
    while bit < size:
        mine = (here // bit) % 2
        pairs = rest.reshape((rest.shape[0] // 2, 2) + rest.shape[1:])
        keep = lax.dynamic_index_in_dim(pairs, mine, 1, keepdims=False)
        give = lax.dynamic_index_in_dim(pairs, 1 - mine, 1, keepdims=False)
        rest = keep + swap(give, axis, bit)
        bit *= 2
    return rest[0]


def gather_whole(quarter, axis):
    size, here = lax.axis_size(axis), lax.axis_index(axis)
    held = quarter[None]
    bit = size // 2
    while bit:
        mine = (here // bit) % 2
        other = swap(held, axis, bit)
        first = jnp.where(mine == 0, held, other)
        second = jnp.where(mine == 0, other, held)
        held = jnp.stack([first, second], axis=1).reshape((-1,) + quarter.shape)
        bit //= 2
    return held.reshape((-1,) + quarter.shape[1:])


def polar(sigma_block):
    states = sigma_block.shape[0]
    mean_sq = jnp.sum(sigma_block * sigma_block) / float(states * states)
    iterate = sigma_block * (lax.rsqrt(states * mean_sq + 1e-06) / 2.2)

    def step(_, iterate):
        gram_matrix = jnp.einsum("ab,cb->ac", iterate, iterate, precision=precise)
        return 1.5 * iterate - 0.5 * dot(gram_matrix, iterate)

    return lax.fori_loop(0, POLAR, step, iterate) * math.sqrt(states)


def shards_general(wavefunction, left_env, right_env, shift_map, op_counts):
    sector_count = lax.axis_size("sector")
    group_size = lax.axis_size("ops")
    group_here = lax.axis_index("ops")
    states = wavefunction.shape[1]
    ops_here = left_env.shape[1]
    parts = sector_count * group_size
    piece = -(-states * states // (SUBLANES * LANES * parts))
    padded = piece * parts
    quarter = piece * sector_count

    whole_map = lax.all_gather(shift_map[0], "ops").reshape(parts)

    def fetch_from_quarter(own_quarter):
        pieces = own_quarter.reshape(sector_count, piece, SUBLANES, LANES)
        spread = lax.all_to_all(pieces, "sector", split_axis=0, concat_axis=0, tiled=True)
        picked = jnp.take(spread, whole_map, axis=0)
        landed = lax.all_to_all(picked, ("ops", "sector"), split_axis=0, concat_axis=0, tiled=True)
        return from_tiles(landed.reshape(padded, SUBLANES, LANES), states, states)

    psi_tiles = to_tiles(wavefunction[0], padded)
    psi_quarter = lax.dynamic_slice_in_dim(psi_tiles, group_here * quarter, quarter, 0)
    moved_block = fetch_from_quarter(psi_quarter)

    left, right = left_env[0], right_env[0]
    count = op_counts[0, 0]
    active = (jnp.arange(ops_here) < count).astype(jnp.float32)
    left_psi = jnp.einsum("wab,bc->wac", left, moved_block, precision=precise) * active[:, None, None]
    partial_sigma = jnp.einsum("wac,wcd->ad", left_psi, right, precision=precise)

    sigma_quarter = sum_scatter(to_tiles(partial_sigma, padded), "ops")
    source_sigma = fetch_from_quarter(sigma_quarter)
    sigma_block = from_tiles(gather_whole(sigma_quarter, "ops"), states, states)

    whole_tensor = polar(sigma_block)
    column_width = states // group_size
    own_columns = lax.dynamic_slice_in_dim(whole_tensor, group_here * column_width, column_width, 1)
    half_rotated = jnp.einsum("ba,wbc->wac", whole_tensor, left, precision=precise)
    source_tensor = polar(source_sigma)
    rotated = jnp.einsum("wac,cd->wad", half_rotated, source_tensor, precision=precise)
    return (own_columns[None], rotated[None])


def halves(value):
    high = value.astype(BF16)
    return high, (value - high.astype(F32)).astype(BF16)


def bdot(a, b):
    return jnp.dot(a, b, preferred_element_type=F32)


class Place:
    def __init__(self, nsec, nops, ny, states):
        self.nsec, self.nops, self.ny, self.nz = nsec, nops, ny, nsec // ny
        self.states = states
        self.chunks = states // LANES
        self.parts = nops * ny
        self.rows = states // self.parts
        self.quarter = states // nops
        self.dests = nops * ny

    def locate(self):
        self.s, self.o = lax.axis_index("sector"), lax.axis_index("ops")
        self.z, self.y = self.s // self.ny, lax.rem(self.s, self.ny)
        self.part = self.o * self.ny + self.y

    def plane_peer(self, index, sign=1):
        dy, do = index // self.nops, index % self.nops
        if sign < 0:
            dy, do = (self.ny - dy) % self.ny, (self.nops - do) % self.nops
        return lax.rem(self.y + dy, self.ny), lax.rem(self.o + do, self.nops)

    def greet(self):
        barrier = pltpu.get_barrier_semaphore()
        for index in range(1, self.dests):
            y, o = self.plane_peer(index)
            pl.semaphore_signal(barrier, inc=1, device_id=(self.z * self.ny + y, o), device_id_type=MESH)

        @pl.when(self.z > 0)
        def _():
            pl.semaphore_signal(barrier, inc=1, device_id=(self.s - self.ny, self.o), device_id_type=MESH)

        @pl.when(self.z < self.nz - 1)
        def _():
            pl.semaphore_signal(barrier, inc=1, device_id=(self.s + self.ny, self.o), device_id_type=MESH)

        line = (self.z > 0).astype(jnp.int32) + (self.z < self.nz - 1).astype(jnp.int32)
        pl.semaphore_wait(barrier, self.dests - 1 + line)


class Maps:
    def __init__(self, place, own_ref, rows_ref, scalars_ref, sems):
        self.place, self.own, self.rows, self.scalars, self.sems = place, own_ref, rows_ref, scalars_ref, sems

    @staticmethod
    def scratch(place):
        return [
            pltpu.VMEM((place.nops, 1, LANES), jnp.int32),
            pltpu.SMEM((place.nops, 1, LANES), jnp.int32),
            pltpu.SemaphoreType.DMA((3, place.nops)),
        ]

    def copy(self, offset, sign):
        p = self.place
        peer = lax.rem(p.o + offset, p.nops)
        slot = p.o if sign > 0 else lax.rem(p.o + p.nops - offset, p.nops)
        return pltpu.make_async_remote_copy(
            self.own, self.rows.at[slot], self.sems.at[0, offset], self.sems.at[1, offset],
            device_id=(p.s, peer), device_id_type=MESH)

    def start(self):
        for offset in range(1, self.place.nops):
            self.copy(offset, 1).start()
        pltpu.make_async_copy(self.own, self.rows.at[self.place.o], self.sems.at[2, 0]).start()

    def finish(self):
        for offset in range(1, self.place.nops):
            self.copy(offset, 1).wait_send()
            self.copy(offset, -1).wait_recv()
        pltpu.make_async_copy(self.own, self.rows.at[self.place.o], self.sems.at[2, 0]).wait()
        landed = pltpu.make_async_copy(self.rows, self.scalars, self.sems.at[2, 1])
        landed.start()
        landed.wait()

    def want(self, y, o):
        return self.scalars[o, 0, self.place.z * self.place.ny + y]


class Fetch:
    def __init__(self, place, maps, piece, held, stage, landed, up, down, across, within, local):
        self.place, self.maps, self.piece = place, maps, piece
        self.held, self.stage, self.landed = held, stage, landed
        self.up, self.down, self.across, self.within, self.local = up, down, across, within, local

    @staticmethod
    def scratch(place):
        c, dma = place.chunks, pltpu.SemaphoreType.DMA
        return (
            [pltpu.VMEM((place.nsec, place.rows, LANES), F32) for _ in range(c)],
            pltpu.VMEM((c, place.dests, place.rows, LANES), F32),
            dma((2, c, place.nz - 1)),
            dma((2, c, place.nz - 1)),
            dma((2, c, place.ny)),
            dma((2, c, place.dests)),
            dma((c,)),
        )

    def across_copy(self, j, dy, sign):
        p = self.place
        y = lax.rem(p.y + dy, p.ny)
        slot = p.s if sign > 0 else p.z * p.ny + lax.rem(p.y + p.ny - dy, p.ny)
        return pltpu.make_async_remote_copy(
            self.piece(j, y), self.held[j].at[slot], self.across.at[0, j, dy], self.across.at[1, j, dy],
            device_id=(p.z * p.ny + y, p.o), device_id_type=MESH)

    def own_copy(self, j):
        p = self.place
        return pltpu.make_async_copy(self.piece(j, p.y), self.held[j].at[p.s], self.local.at[j])

    def begin(self, j):
        for dy in range(1, self.place.ny):
            self.across_copy(j, dy, 1).start()
        self.own_copy(j).start()

    def line_copy(self, j, k, direction):
        p = self.place
        slab = self.held[j].at[pl.ds((p.z - direction * k) * p.ny, p.ny)]
        sems = self.up if direction > 0 else self.down
        return pltpu.make_async_remote_copy(
            slab, slab, sems.at[0, j, k], sems.at[1, j, k],
            device_id=(p.s + direction * p.ny, p.o), device_id_type=MESH)

    def line_wait(self, j, k, direction):
        p = self.place
        slab = self.held[j].at[pl.ds((p.z - direction * k) * p.ny, p.ny)]
        sems = self.up if direction > 0 else self.down
        pltpu.make_async_remote_copy(
            slab, slab, sems.at[0, j, k - 1], sems.at[1, j, k - 1],
            device_id=(p.s - direction * p.ny, p.o), device_id_type=MESH).wait_recv()

    def has(self, k, direction):
        return self.place.z >= k if direction > 0 else self.place.z < self.place.nz - k

    def more(self, direction):
        return self.place.z < self.place.nz - 1 if direction > 0 else self.place.z > 0

    def send_own(self, j):
        for dy in range(1, self.place.ny):
            self.across_copy(j, dy, -1).wait_recv()
        self.own_copy(j).wait()
        for direction in (1, -1):
            @pl.when(self.more(direction))
            def _():
                self.line_copy(j, 0, direction).start()

    def forward(self, j, k):
        for direction in (1, -1):
            @pl.when(self.has(k, direction))
            def _():
                self.line_wait(j, k, direction)

            if k < self.place.nz - 1:
                @pl.when(self.has(k, direction) & self.more(direction))
                def _():
                    self.line_copy(j, k, direction).start()

    def within_copy(self, j, index, sign):
        p = self.place
        y, o = p.plane_peer(index, sign)
        part = p.part if sign > 0 else o * p.ny + y
        return pltpu.make_async_remote_copy(
            self.stage.at[j, index], self.landed.at[j, pl.ds(part * p.rows, p.rows)],
            self.within.at[0, j, index], self.within.at[1, j, index],
            device_id=(p.z * p.ny + y, o), device_id_type=MESH)

    def hand_out(self, j):
        p = self.place
        order = sorted(range(p.dests), key=lambda index: -((index // p.nops > 0) + (index % p.nops > 0)))
        for index in order:
            y, o = p.plane_peer(index)
            picked = self.held[j][self.maps.want(y, o)]
            if index == 0:
                self.landed[j, pl.ds(p.part * p.rows, p.rows)] = picked
            else:
                self.stage[j, index] = picked
                self.within_copy(j, index, 1).start()

    def receive(self, j):
        for index in range(1, self.place.dests):
            self.within_copy(j, index, -1).wait_recv()

    def drain(self):
        for j in range(self.place.chunks):
            for dy in range(1, self.place.ny):
                self.across_copy(j, dy, 1).wait_send()
            for direction in (1, -1):
                for k in range(self.place.nz - 1):
                    @pl.when(self.has(k, direction) & self.more(direction))
                    def _():
                        self.line_copy(j, k, direction).wait_send()
            for index in range(1, self.place.dests):
                self.within_copy(j, index, 1).wait_send()


def tdot(a, b):
    return lax.dot_general(a, b, (((1,), (1,)), ((), ())), preferred_element_type=F32)


class Polar:
    def __init__(self, n, block, cols, rows, gram):
        self.n, self.block, self.cols, self.rows, self.gram = n, block, cols, rows, gram

    @staticmethod
    def scratch(n):
        return [pltpu.VMEM((n, 2 * n), BF16), pltpu.VMEM((2 * n, n), BF16), pltpu.VMEM((2 * n, n), BF16)]

    def normalise(self, sigma):
        n = self.n
        squares = jnp.sum(jnp.sum(sigma * sigma, axis=0, keepdims=True), axis=1, keepdims=True)
        self.block[...] = sigma * (lax.rsqrt(n * (squares / float(n * n)) + 1e-06) / 2.2)

    def form_gram(self):
        n = self.n
        high, low = halves(self.block[...])
        self.cols[:, pl.ds(0, n)] = high
        self.cols[:, pl.ds(n, n)] = low
        self.rows[pl.ds(0, n)] = high
        self.rows[pl.ds(n, n)] = low
        both = tdot(high, self.rows[...])
        cross = both[:, n:]
        self.gram[pl.ds(0, n)], self.gram[pl.ds(n, n)] = halves(both[:, :n] + (cross + cross.T))

    def apply(self, scale=None):
        n = self.n
        both = bdot(self.gram[pl.ds(0, n)], self.cols[...])
        moved = both[:, :n] + (both[:, n:] + bdot(self.gram[pl.ds(n, n)], self.cols[:, pl.ds(0, n)]))
        value = 1.5 * self.block[...] - 0.5 * moved
        self.block[...] = value if scale is None else value * scale


def site_kernel(place, ops_here, psi, left, right, own_map, counts, own_columns, half_out, source_out, rows, scalars,
                map_sems, *rest):
    c, n = place.chunks, place.states
    groups = []
    for _ in range(2):
        groups.append((rest[:c], rest[c:c + 6], rest[c + 6]))
        rest = rest[c + 7:]
    (lefts, rights, block, envs, env_sems, lp_high, lp_low, sigma, first, second, pair, sum_sems,
     quarter, gather_sems, polar_block, cols, doubled, gram, out_sems) = rest
    place.locate()
    p = place

    def load(ref, w):
        slot = w % 2 if isinstance(w, int) else lax.rem(w, 2)
        return pltpu.make_async_copy(ref.at[w], envs.at[slot], env_sems.at[slot])

    load(left, 0).start()
    load(left, 1).start()
    place.greet()
    maps = Maps(place, own_map, rows, scalars, map_sems)

    def fetch_of(piece, group):
        held, (stage, up, down, across, within, local), landed = group
        return Fetch(place, maps, piece, held, stage, landed, up, down, across, within, local)

    fetch = fetch_of(lambda j, y: psi.at[pl.ds((p.o * p.ny + y) * p.rows, p.rows), pl.ds(j * LANES, LANES)], groups[0])
    again = fetch_of(lambda j, y: quarter.at[pl.ds(y * p.rows, p.rows), pl.ds(j * LANES, LANES)], groups[1])
    maps.start()
    for j in range(c):
        fetch.begin(j)
    for j in range(min(AHEAD, c)):
        fetch.send_own(j)
    count = counts[0, 0]
    sigma[...] = jnp.zeros((n, n), F32)
    block[pl.ds(n, n), pl.ds(LANES, LANES)] = jnp.zeros((n, LANES), BF16)

    def at(index, events):
        for turn, event in events:
            pl.when(index == turn)(event)

    def line(which, *steps):
        def event():
            for j, k in steps:
                if j < c:
                    which.send_own(j) if k == 0 else which.forward(j, k)
        return event

    def turn_in(which, j):
        def event():
            if j < c:
                which.forward(j, p.nz - 1)
                which.hand_out(j)
        return event

    def middle(j):
        return [(j, k) for k in range(2, p.nz - 1)]

    def convert_left(w, carry):
        load(left, w).wait()
        high, low = halves(envs[lax.rem(w, 2)])
        rows_of = pl.ds(pl.multiple_of(w * n, n), n)
        lefts[rows_of, pl.ds(0, n)] = high
        lefts[rows_of, pl.ds(n, n)] = low

        @pl.when(w < ops_here - 2)
        def _():
            load(left, w + 2).start()

        @pl.when(w >= ops_here - 2)
        def _():
            load(right, w + 2 - ops_here).start()

        at(w, [(1, line(fetch, (0, 1))), (2, line(fetch, (AHEAD, 0), (1, 1))), (2, maps.finish)])
        return carry

    def convert_right(w, carry):
        load(right, w).wait()
        high, low = halves(envs[lax.rem(w, 2)] * (w < count).astype(F32))
        for j in range(c):
            rows_of = pl.ds(pl.multiple_of((j * ops_here + w) * LANES, LANES), LANES)
            rights[rows_of, pl.ds(0, n)] = high[j * LANES:(j + 1) * LANES]
            rights[rows_of, pl.ds(n, n)] = low[j * LANES:(j + 1) * LANES]

        @pl.when(w < ops_here - 2)
        def _():
            load(right, w + 2).start()

        at(w, [(0, line(fetch, *middle(0))), (1, line(fetch, (AHEAD + 1, 0), (2, 1))), (3, line(fetch, *middle(1)))])
        return carry

    lax.fori_loop(0, ops_here, convert_left, 0)
    lax.fori_loop(0, ops_here, convert_right, 0)
    for j in range(AHEAD + 2, c):
        fetch.send_own(j)
    turn_in(fetch, 0)()

    def products(j, carry):
        for turn in range(c):
            @pl.when(j == turn)
            def _():
                line(fetch, (turn + 3, 1), *middle(turn + 2))()
                if turn < c - 2:
                    turn_in(fetch, turn + 1)()
                fetch.receive(turn)

        high, low = halves(fetch.landed[j])
        block[pl.ds(0, n), pl.ds(0, LANES)] = high
        block[pl.ds(n, n), pl.ds(0, LANES)] = high
        block[pl.ds(0, n), pl.ds(LANES, LANES)] = low
        for w in range(ops_here):
            both = bdot(lefts[pl.ds(w * n, n)], block[...])
            high, low = halves(both[:, :LANES] + both[:, LANES:])
            lp_high[:, pl.ds(w * LANES, LANES)] = high
            lp_low[:, pl.ds(w * LANES, LANES)] = low

        @pl.when(j == max(c - 3, 0))
        def _():
            if c > 1:
                turn_in(fetch, c - 1)()

        deep = pl.ds(pl.multiple_of(j * ops_here * LANES, LANES), ops_here * LANES)
        both = bdot(lp_high[...], rights[deep])
        sigma[...] += both[:, :n] + (both[:, n:] + bdot(lp_low[...], rights[deep, pl.ds(0, n)]))
        return carry

    lax.fori_loop(0, c, products, 0)

    side, core = p.o // CORES, lax.rem(p.o, CORES)
    mate = side * CORES + 1 - core
    facing = (1 - side) * CORES + core
    across_mate = (1 - side) * CORES + 1 - core
    q = p.quarter

    def swap_cores(i, far):
        rows_of = (far * CORES + 1 - core) * q
        return pltpu.make_async_remote_copy(
            sigma.at[pl.ds(rows_of, q)], first.at[i], sum_sems.at[0, i], sum_sems.at[1, i],
            device_id=(p.s, mate), device_id_type=MESH)

    for i, far in ((0, 1 - side), (1, side)):
        swap_cores(i, far).start()
    swap_cores(0, 1 - side).wait_recv()
    pair[...] = sigma[pl.ds(((1 - side) * CORES + core) * q, q)] + first[0]
    over = pltpu.make_async_remote_copy(
        pair, second, sum_sems.at[0, 2], sum_sems.at[1, 2], device_id=(p.s, facing), device_id_type=MESH)
    over.start()
    swap_cores(1, side).wait_recv()
    over.wait_recv()
    quarter[...] = sigma[pl.ds(p.o * q, q)] + first[1] + second[...]
    for i, far in ((0, 1 - side), (1, side)):
        swap_cores(i, far).wait_send()
    over.wait_send()

    whole = polar_block
    polar = Polar(n, whole, cols, doubled, gram)

    def gather(i, sender, target):
        rows_of = pl.ds(sender * q, q)
        source = quarter if i < 2 else whole.at[rows_of]
        return pltpu.make_async_remote_copy(
            source, whole.at[rows_of], gather_sems.at[0, i], gather_sems.at[1, i],
            device_id=(p.s, target), device_id_type=MESH)

    gather(1, p.o, facing).start()
    gather(0, p.o, mate).start()
    for j in range(c):
        again.begin(j)
    whole[pl.ds(p.o * q, q)] = quarter[...]
    for j in range(min(AHEAD, c)):
        again.send_own(j)
    line(again, (0, 1), (AHEAD, 0), (1, 1))()
    gather(1, facing, facing).wait_recv()
    gather(2, facing, mate).start()
    line(again, *middle(0))()
    for j in range(AHEAD + 1, c):
        again.send_own(j)
    gather(0, mate, mate).wait_recv()
    gather(2, across_mate, mate).wait_recv()
    gather(2, facing, mate).wait_send()
    polar.normalise(whole[...])

    def group(turn):
        def event():
            line(again, (turn + 1, 1), *middle(turn))()
            turn_in(again, turn - 1)()
        return event

    def own_step(step, carry):
        polar.form_gram()
        polar.apply()
        at(step, [(turn - 1, group(turn)) for turn in range(1, min(c, POLAR) + 1)])
        return carry

    lax.fori_loop(0, POLAR, own_step, 0)
    for turn in range(POLAR + 1, c + 1):
        group(turn)()
    tensor = (whole[...] * math.sqrt(n)).T
    whole[...] = tensor
    own_columns[...] = whole[pl.ds(pl.multiple_of(p.o * q, q), q)]
    gram[pl.ds(0, n)], gram[pl.ds(n, n)] = halves(tensor)

    def half_rotate(w, carry):
        rows_of = pl.ds(pl.multiple_of(w * n, n), n)
        both = bdot(gram[pl.ds(0, n)], lefts[rows_of])
        turned = both[:, :n] + (both[:, n:] + bdot(gram[pl.ds(n, n)], lefts[rows_of, pl.ds(0, n)]))
        rights[rows_of, pl.ds(0, n)], rights[rows_of, pl.ds(n, n)] = halves(turned)
        pltpu.make_async_copy(rights.at[rows_of], half_out.at[rows_of], out_sems.at[w]).start()
        return carry

    lax.fori_loop(0, ops_here, half_rotate, 0)
    for j in range(c):
        again.receive(j)
    save = pltpu.make_async_copy(again.landed, source_out, out_sems.at[ops_here])
    save.start()
    for w in range(ops_here):
        rows_of = pl.ds(w * n, n)
        pltpu.make_async_copy(rights.at[rows_of], half_out.at[rows_of], out_sems.at[w]).wait()
    fetch.drain()
    again.drain()
    gather(1, p.o, facing).wait_send()
    gather(0, p.o, mate).wait_send()
    save.wait()


def last_kernel(n, ops_here, chunks, source, half, columns, own_columns, rotated, block, cols, doubled, gram, halves_in,
                products, in_sems, out_sems):
    def load(w):
        at = pl.ds(w * n, n)
        return pltpu.make_async_copy(half.at[at], halves_in.at[at], in_sems.at[w])

    def store(w):
        return pltpu.make_async_copy(products.at[w], rotated.at[w], out_sems.at[w])

    for w in range(ops_here):
        load(w).start()
    own_columns[...] = columns[...]
    polar = Polar(n, block, cols, doubled, gram)
    polar.normalise(jnp.concatenate([source[j] for j in range(chunks)], axis=1))

    def step(_, carry):
        polar.form_gram()
        polar.apply()
        return carry

    lax.fori_loop(0, POLAR, step, 0)
    high, low = halves(block[...] * math.sqrt(n))
    cols[:, pl.ds(0, n)] = high
    cols[:, pl.ds(n, n)] = low

    def rotate(w, carry):
        load(w).wait()
        rows_of = pl.ds(pl.multiple_of(w * n, n), n)
        both = bdot(halves_in[rows_of, pl.ds(0, n)], cols[...])
        products[w] = both[:, :n] + (both[:, n:] + bdot(halves_in[rows_of, pl.ds(n, n)], cols[:, pl.ds(0, n)]))
        store(w).start()
        return carry

    lax.fori_loop(0, ops_here, rotate, 0)
    for w in range(ops_here):
        store(w).wait()


def vmem():
    return pl.BlockSpec(memory_space=pltpu.VMEM)


def anywhere():
    return pl.BlockSpec(memory_space=pl.ANY)


def shards_planes(place, wavefunction, left_env, right_env, shift_map, op_counts):
    c, n, q, ops_here = place.chunks, place.states, place.quarter, left_env.shape[1]
    own_map = jnp.pad(shift_map, ((0, 0), (0, LANES - shift_map.shape[1])))
    fetches = []
    for _ in range(2):
        held, stage, *sems = Fetch.scratch(place)
        fetches += [*held, stage, *sems, pltpu.VMEM((c, n, LANES), F32)]
    columns, half, source = pl.pallas_call(
        functools.partial(site_kernel, place, ops_here),
        out_shape=(
            jax.ShapeDtypeStruct((q, n), F32),
            jax.ShapeDtypeStruct((ops_here * n, 2 * n), BF16),
            jax.ShapeDtypeStruct((c, n, LANES), F32),
        ),
        in_specs=[vmem(), anywhere(), anywhere(), vmem(), pl.BlockSpec(memory_space=pltpu.SMEM)],
        out_specs=(vmem(), anywhere(), anywhere()),
        scratch_shapes=[
            *Maps.scratch(place), *fetches,
            pltpu.VMEM((ops_here * n, 2 * n), BF16),
            pltpu.VMEM((ops_here * n, 2 * n), BF16),
            pltpu.VMEM((2 * n, 2 * LANES), BF16),
            pltpu.VMEM((2, n, n), F32),
            pltpu.SemaphoreType.DMA((2,)),
            pltpu.VMEM((n, ops_here * LANES), BF16),
            pltpu.VMEM((n, ops_here * LANES), BF16),
            pltpu.VMEM((n, n), F32),
            pltpu.VMEM((2, q, n), F32),
            pltpu.VMEM((q, n), F32),
            pltpu.VMEM((q, n), F32),
            pltpu.SemaphoreType.DMA((2, 3)),
            pltpu.VMEM((q, n), F32),
            pltpu.SemaphoreType.DMA((2, 3)),
            pltpu.VMEM((n, n), F32),
            *Polar.scratch(n),
            pltpu.SemaphoreType.DMA((ops_here + 1,)),
        ],
        compiler_params=pltpu.CompilerParams(collective_id=0, has_side_effects=True, vmem_limit_bytes=60 * 2**20),
    )(wavefunction[0], left_env[0], right_env[0], own_map, op_counts)
    own_columns, rotated = pl.pallas_call(
        functools.partial(last_kernel, n, ops_here, c),
        out_shape=(jax.ShapeDtypeStruct((q, n), F32), jax.ShapeDtypeStruct((ops_here, n, n), F32)),
        in_specs=[vmem(), anywhere(), vmem()],
        out_specs=(vmem(), anywhere()),
        scratch_shapes=[
            pltpu.VMEM((n, n), F32),
            *Polar.scratch(n),
            pltpu.VMEM((ops_here * n, 2 * n), BF16),
            pltpu.VMEM((ops_here, n, n), F32),
            pltpu.SemaphoreType.DMA((ops_here,)),
            pltpu.SemaphoreType.DMA((ops_here,)),
        ],
        compiler_params=pltpu.CompilerParams(vmem_limit_bytes=60 * 2**20),
    )(source, half, columns)
    return own_columns.T[None], rotated[None]


def line_split(sector_count):
    rows = 1
    while rows * 2 * rows * 2 <= sector_count and sector_count % (rows * 2) == 0:
        rows *= 2
    return rows


def solution(mesh):
    def shards(wavefunction, left_env, right_env, shift_map, op_counts):
        nsec, nops = mesh.shape["sector"], mesh.shape["ops"]
        states = wavefunction.shape[1]
        ny = line_split(nsec)
        fits = nops == 2 * CORES and ny == 2 and states % LANES == 0 and states % (nops * ny * SUBLANES) == 0
        if not fits:
            return shards_general(wavefunction, left_env, right_env, shift_map, op_counts)
        place = Place(nsec, nops, ny, states)
        return shards_planes(place, wavefunction, left_env, right_env, shift_map, op_counts)

    return jax.shard_map(
        shards,
        mesh=mesh,
        in_specs=(
            P("sector", None, None),
            P("sector", "ops", None, None),
            P("sector", "ops", None, None),
            P("ops", None),
            P("ops", "sector"),
        ),
        out_specs=(P("sector", None, "ops"), P("sector", "ops", None, None)),
        check_vma=False,
    )
```

```python
import functools
import math

import jax
import jax.numpy as jnp
from jax import lax
from jax.experimental import pallas as pl
from jax.experimental.pallas import tpu as pltpu
from jax.sharding import PartitionSpec as P

POLAR = 5
LANES, SUBLANES = 128, 8
CORES = 2
AHEAD = 3
MESH = pl.DeviceIdType.MESH
F32, BF16 = jnp.float32, jnp.bfloat16

precise = lax.Precision.HIGH


def dot(a, b):
    return jnp.dot(a, b, precision=precise, preferred_element_type=jnp.float32)


def to_tiles(block, padded):
    rows, cols = block.shape
    tiles = block.reshape(rows // SUBLANES, SUBLANES, cols // LANES, LANES)
    tiles = tiles.transpose(0, 2, 1, 3).reshape(rows * cols // (SUBLANES * LANES), SUBLANES, LANES)
    return jnp.pad(tiles, ((0, padded - tiles.shape[0]), (0, 0), (0, 0)))


def from_tiles(tiles, rows, cols):
    tiles = tiles[: rows * cols // (SUBLANES * LANES)]
    tiles = tiles.reshape(rows // SUBLANES, cols // LANES, SUBLANES, LANES)
    return tiles.transpose(0, 2, 1, 3).reshape(rows, cols)


def swap(value, axis, bit):
    size = lax.axis_size(axis)
    return lax.ppermute(value, axis, [(i, i ^ bit) for i in range(size)])


def sum_scatter(tiles, axis):
    size, here = lax.axis_size(axis), lax.axis_index(axis)
    rest = tiles.reshape((size, tiles.shape[0] // size) + tiles.shape[1:])
    bit = 1
    while bit < size:
        mine = (here // bit) % 2
        pairs = rest.reshape((rest.shape[0] // 2, 2) + rest.shape[1:])
        keep = lax.dynamic_index_in_dim(pairs, mine, 1, keepdims=False)
        give = lax.dynamic_index_in_dim(pairs, 1 - mine, 1, keepdims=False)
        rest = keep + swap(give, axis, bit)
        bit *= 2
    return rest[0]


def gather_whole(quarter, axis):
    size, here = lax.axis_size(axis), lax.axis_index(axis)
    held = quarter[None]
    bit = size // 2
    while bit:
        mine = (here // bit) % 2
        other = swap(held, axis, bit)
        first = jnp.where(mine == 0, held, other)
        second = jnp.where(mine == 0, other, held)
        held = jnp.stack([first, second], axis=1).reshape((-1,) + quarter.shape)
        bit //= 2
    return held.reshape((-1,) + quarter.shape[1:])


def polar(sigma_block):
    states = sigma_block.shape[0]
    mean_sq = jnp.sum(sigma_block * sigma_block) / float(states * states)
    iterate = sigma_block * (lax.rsqrt(states * mean_sq + 1e-06) / 2.2)

    def step(_, iterate):
        gram_matrix = jnp.einsum("ab,cb->ac", iterate, iterate, precision=precise)
        return 1.5 * iterate - 0.5 * dot(gram_matrix, iterate)

    return lax.fori_loop(0, POLAR, step, iterate) * math.sqrt(states)


def shards_general(wavefunction, left_env, right_env, shift_map, op_counts):
    sector_count = lax.axis_size("sector")
    group_size = lax.axis_size("ops")
    group_here = lax.axis_index("ops")
    states = wavefunction.shape[1]
    ops_here = left_env.shape[1]
    parts = sector_count * group_size
    piece = -(-states * states // (SUBLANES * LANES * parts))
    padded = piece * parts
    quarter = piece * sector_count

    whole_map = lax.all_gather(shift_map[0], "ops").reshape(parts)

    def fetch_from_quarter(own_quarter):
        pieces = own_quarter.reshape(sector_count, piece, SUBLANES, LANES)
        spread = lax.all_to_all(pieces, "sector", split_axis=0, concat_axis=0, tiled=True)
        picked = jnp.take(spread, whole_map, axis=0)
        landed = lax.all_to_all(picked, ("ops", "sector"), split_axis=0, concat_axis=0, tiled=True)
        return from_tiles(landed.reshape(padded, SUBLANES, LANES), states, states)

    psi_tiles = to_tiles(wavefunction[0], padded)
    psi_quarter = lax.dynamic_slice_in_dim(psi_tiles, group_here * quarter, quarter, 0)
    moved_block = fetch_from_quarter(psi_quarter)

    left, right = left_env[0], right_env[0]
    count = op_counts[0, 0]
    active = (jnp.arange(ops_here) < count).astype(jnp.float32)
    left_psi = jnp.einsum("wab,bc->wac", left, moved_block, precision=precise) * active[:, None, None]
    partial_sigma = jnp.einsum("wac,wcd->ad", left_psi, right, precision=precise)

    sigma_quarter = sum_scatter(to_tiles(partial_sigma, padded), "ops")
    source_sigma = fetch_from_quarter(sigma_quarter)
    sigma_block = from_tiles(gather_whole(sigma_quarter, "ops"), states, states)

    whole_tensor = polar(sigma_block)
    column_width = states // group_size
    own_columns = lax.dynamic_slice_in_dim(whole_tensor, group_here * column_width, column_width, 1)
    half_rotated = jnp.einsum("ba,wbc->wac", whole_tensor, left, precision=precise)
    source_tensor = polar(source_sigma)
    rotated = jnp.einsum("wac,cd->wad", half_rotated, source_tensor, precision=precise)
    return (own_columns[None], rotated[None])


def halves(value):
    high = value.astype(BF16)
    return high, (value - high.astype(F32)).astype(BF16)


def bdot(a, b):
    return jnp.dot(a, b, preferred_element_type=F32)


class Place:
    def __init__(self, nsec, nops, ny, states):
        self.nsec, self.nops, self.ny, self.nz = nsec, nops, ny, nsec // ny
        self.states = states
        self.chunks = states // LANES
        self.parts = nops * ny
        self.rows = states // self.parts
        self.quarter = states // nops
        self.dests = nops * ny

    def locate(self):
        self.s, self.o = lax.axis_index("sector"), lax.axis_index("ops")
        self.z, self.y = self.s // self.ny, lax.rem(self.s, self.ny)
        self.part = self.o * self.ny + self.y

    def plane_peer(self, index, sign=1):
        dy, do = index // self.nops, index % self.nops
        if sign < 0:
            dy, do = (self.ny - dy) % self.ny, (self.nops - do) % self.nops
        return lax.rem(self.y + dy, self.ny), lax.rem(self.o + do, self.nops)

    def greet(self):
        barrier = pltpu.get_barrier_semaphore()
        for index in range(1, self.dests):
            y, o = self.plane_peer(index)
            pl.semaphore_signal(barrier, inc=1, device_id=(self.z * self.ny + y, o), device_id_type=MESH)

        @pl.when(self.z > 0)
        def _():
            pl.semaphore_signal(barrier, inc=1, device_id=(self.s - self.ny, self.o), device_id_type=MESH)

        @pl.when(self.z < self.nz - 1)
        def _():
            pl.semaphore_signal(barrier, inc=1, device_id=(self.s + self.ny, self.o), device_id_type=MESH)

        line = (self.z > 0).astype(jnp.int32) + (self.z < self.nz - 1).astype(jnp.int32)
        pl.semaphore_wait(barrier, self.dests - 1 + line)


class Maps:
    def __init__(self, place, table, own_ref, rows_ref, scalars_ref, sems):
        self.place, self.table = place, table
        self.own, self.rows, self.scalars, self.sems = own_ref, rows_ref, scalars_ref, sems

    @staticmethod
    def scratch(place):
        return [
            pltpu.VMEM((1, LANES), jnp.int32),
            pltpu.VMEM((place.nops, 1, LANES), jnp.int32),
            pltpu.SMEM((place.nops, 1, LANES), jnp.int32),
            pltpu.SemaphoreType.DMA((3, place.nops)),
        ]

    def write(self):
        lane = lax.broadcasted_iota(jnp.int32, (1, LANES), 1)
        row = jnp.zeros((1, LANES), jnp.int32)
        for sector in range(self.place.nsec):
            row = jnp.where(lane == sector, self.table[0, sector], row)
        self.own[...] = row

    def copy(self, offset, sign):
        p = self.place
        peer = lax.rem(p.o + offset, p.nops)
        slot = p.o if sign > 0 else lax.rem(p.o + p.nops - offset, p.nops)
        return pltpu.make_async_remote_copy(
            self.own, self.rows.at[slot], self.sems.at[0, offset], self.sems.at[1, offset],
            device_id=(p.s, peer), device_id_type=MESH)

    def start(self):
        for offset in range(1, self.place.nops):
            self.copy(offset, 1).start()
        pltpu.make_async_copy(self.own, self.rows.at[self.place.o], self.sems.at[2, 0]).start()

    def finish(self):
        for offset in range(1, self.place.nops):
            self.copy(offset, 1).wait_send()
            self.copy(offset, -1).wait_recv()
        pltpu.make_async_copy(self.own, self.rows.at[self.place.o], self.sems.at[2, 0]).wait()
        landed = pltpu.make_async_copy(self.rows, self.scalars, self.sems.at[2, 1])
        landed.start()
        landed.wait()

    def want(self, y, o):
        return self.scalars[o, 0, self.place.z * self.place.ny + y]


class Fetch:
    def __init__(self, place, maps, piece, held, stage, landed, up, down, across, within, local):
        self.place, self.maps, self.piece = place, maps, piece
        self.held, self.stage, self.landed = held, stage, landed
        self.up, self.down, self.across, self.within, self.local = up, down, across, within, local

    @staticmethod
    def scratch(place):
        c, dma = place.chunks, pltpu.SemaphoreType.DMA
        return (
            [pltpu.VMEM((place.nsec, place.rows, LANES), F32) for _ in range(c)],
            pltpu.VMEM((c, place.dests, place.rows, LANES), F32),
            dma((2, c, place.nz - 1)),
            dma((2, c, place.nz - 1)),
            dma((2, c, place.ny)),
            dma((2, c, place.dests)),
            dma((c,)),
        )

    def across_copy(self, j, dy, sign):
        p = self.place
        y = lax.rem(p.y + dy, p.ny)
        slot = p.s if sign > 0 else p.z * p.ny + lax.rem(p.y + p.ny - dy, p.ny)
        return pltpu.make_async_remote_copy(
            self.piece(j, y), self.held[j].at[slot], self.across.at[0, j, dy], self.across.at[1, j, dy],
            device_id=(p.z * p.ny + y, p.o), device_id_type=MESH)

    def own_copy(self, j):
        p = self.place
        return pltpu.make_async_copy(self.piece(j, p.y), self.held[j].at[p.s], self.local.at[j])

    def begin(self, j):
        for dy in range(1, self.place.ny):
            self.across_copy(j, dy, 1).start()
        self.own_copy(j).start()

    def line_copy(self, j, k, direction):
        p = self.place
        slab = self.held[j].at[pl.ds((p.z - direction * k) * p.ny, p.ny)]
        sems = self.up if direction > 0 else self.down
        return pltpu.make_async_remote_copy(
            slab, slab, sems.at[0, j, k], sems.at[1, j, k],
            device_id=(p.s + direction * p.ny, p.o), device_id_type=MESH)

    def line_wait(self, j, k, direction):
        p = self.place
        slab = self.held[j].at[pl.ds((p.z - direction * k) * p.ny, p.ny)]
        sems = self.up if direction > 0 else self.down
        pltpu.make_async_remote_copy(
            slab, slab, sems.at[0, j, k - 1], sems.at[1, j, k - 1],
            device_id=(p.s - direction * p.ny, p.o), device_id_type=MESH).wait_recv()

    def has(self, k, direction):
        return self.place.z >= k if direction > 0 else self.place.z < self.place.nz - k

    def more(self, direction):
        return self.place.z < self.place.nz - 1 if direction > 0 else self.place.z > 0

    def send_own(self, j):
        for dy in range(1, self.place.ny):
            self.across_copy(j, dy, -1).wait_recv()
        self.own_copy(j).wait()
        for direction in (1, -1):
            @pl.when(self.more(direction))
            def _():
                self.line_copy(j, 0, direction).start()

    def forward(self, j, k):
        for direction in (1, -1):
            @pl.when(self.has(k, direction))
            def _():
                self.line_wait(j, k, direction)

            if k < self.place.nz - 1:
                @pl.when(self.has(k, direction) & self.more(direction))
                def _():
                    self.line_copy(j, k, direction).start()

    def within_copy(self, j, index, sign):
        p = self.place
        y, o = p.plane_peer(index, sign)
        part = p.part if sign > 0 else o * p.ny + y
        return pltpu.make_async_remote_copy(
            self.stage.at[j, index], self.landed.at[j, pl.ds(part * p.rows, p.rows)],
            self.within.at[0, j, index], self.within.at[1, j, index],
            device_id=(p.z * p.ny + y, o), device_id_type=MESH)

    def hand_out(self, j):
        p = self.place
        order = sorted(range(p.dests), key=lambda index: -((index // p.nops > 0) + (index % p.nops > 0)))
        for index in order:
            y, o = p.plane_peer(index)
            picked = self.held[j][self.maps.want(y, o)]
            if index == 0:
                self.landed[j, pl.ds(p.part * p.rows, p.rows)] = picked
            else:
                self.stage[j, index] = picked
        for index in order:
            if index:
                self.within_copy(j, index, 1).start()

    def receive(self, j):
        for index in range(1, self.place.dests):
            self.within_copy(j, index, -1).wait_recv()

    def drain(self):
        for j in range(self.place.chunks):
            for dy in range(1, self.place.ny):
                self.across_copy(j, dy, 1).wait_send()
            for direction in (1, -1):
                for k in range(self.place.nz - 1):
                    @pl.when(self.has(k, direction) & self.more(direction))
                    def _():
                        self.line_copy(j, k, direction).wait_send()
            for index in range(1, self.place.dests):
                self.within_copy(j, index, 1).wait_send()


def tdot(a, b):
    return lax.dot_general(a, b, (((1,), (1,)), ((), ())), preferred_element_type=F32)


class Polar:
    def __init__(self, n, block, cols, rows, gram):
        self.n, self.block, self.cols, self.rows, self.gram = n, block, cols, rows, gram

    @staticmethod
    def scratch(n):
        return [pltpu.VMEM((n, 2 * n), BF16), pltpu.VMEM((2 * n, n), BF16), pltpu.VMEM((2 * n, n), BF16)]

    def normalise(self, sigma):
        n = self.n
        squares = jnp.sum(jnp.sum(sigma * sigma, axis=0, keepdims=True), axis=1, keepdims=True)
        self.block[...] = sigma * (lax.rsqrt(n * (squares / float(n * n)) + 1e-06) / 2.2)

    def form_gram(self):
        n = self.n
        high, low = halves(self.block[...])
        self.cols[:, pl.ds(0, n)] = high
        self.cols[:, pl.ds(n, n)] = low
        self.rows[pl.ds(0, n)] = high
        self.rows[pl.ds(n, n)] = low
        both = tdot(high, self.rows[...])
        cross = both[:, n:]
        self.gram[pl.ds(0, n)], self.gram[pl.ds(n, n)] = halves(both[:, :n] + (cross + cross.T))

    def apply(self, scale=None):
        n = self.n
        both = bdot(self.gram[pl.ds(0, n)], self.cols[...])
        moved = both[:, :n] + (both[:, n:] + bdot(self.gram[pl.ds(n, n)], self.cols[:, pl.ds(0, n)]))
        value = 1.5 * self.block[...] - 0.5 * moved
        self.block[...] = value if scale is None else value * scale


def site_kernel(place, ops_here, psi, left, right, table, counts, own_columns, half_out, source_out, map_row, rows,
                scalars, map_sems, *rest):
    c, n = place.chunks, place.states
    groups = []
    for _ in range(2):
        groups.append((rest[:c], rest[c:c + 6], rest[c + 6]))
        rest = rest[c + 7:]
    (lefts, rights, block, envs, env_sems, lp_high, lp_low, sigma, first, second, pair, sum_sems,
     quarter, gather_sems, polar_block, cols, doubled, gram, out_sems) = rest
    place.locate()
    p = place

    def load(ref, w):
        slot = w % 2 if isinstance(w, int) else lax.rem(w, 2)
        return pltpu.make_async_copy(ref.at[w], envs.at[slot], env_sems.at[slot])

    load(left, 0).start()
    load(left, 1).start()
    maps = Maps(place, table, map_row, rows, scalars, map_sems)
    maps.write()
    place.greet()

    def fetch_of(piece, group):
        held, (stage, up, down, across, within, local), landed = group
        return Fetch(place, maps, piece, held, stage, landed, up, down, across, within, local)

    fetch = fetch_of(lambda j, y: psi.at[pl.ds((p.o * p.ny + y) * p.rows, p.rows), pl.ds(j * LANES, LANES)], groups[0])
    again = fetch_of(lambda j, y: quarter.at[pl.ds(y * p.rows, p.rows), pl.ds(j * LANES, LANES)], groups[1])
    maps.start()
    for j in range(c):
        fetch.begin(j)
    for j in range(min(AHEAD, c)):
        fetch.send_own(j)
    count = counts[0, 0]
    sigma[...] = jnp.zeros((n, n), F32)
    block[pl.ds(n, n), pl.ds(LANES, LANES)] = jnp.zeros((n, LANES), BF16)

    def at(index, events):
        for turn, event in events:
            pl.when(index == turn)(event)

    def line(which, *steps):
        def event():
            for j, k in steps:
                if j < c:
                    which.send_own(j) if k == 0 else which.forward(j, k)
        return event

    def turn_in(which, j):
        def event():
            if j < c:
                which.forward(j, p.nz - 1)
                which.hand_out(j)
        return event

    def middle(j):
        return [(j, k) for k in range(2, p.nz - 1)]

    def convert_left(w, carry):
        load(left, w).wait()
        high, low = halves(envs[lax.rem(w, 2)])
        rows_of = pl.ds(pl.multiple_of(w * n, n), n)
        lefts[rows_of, pl.ds(0, n)] = high
        lefts[rows_of, pl.ds(n, n)] = low

        @pl.when(w < ops_here - 2)
        def _():
            load(left, w + 2).start()

        @pl.when(w >= ops_here - 2)
        def _():
            load(right, w + 2 - ops_here).start()

        at(w, [(1, line(fetch, (0, 1))), (2, line(fetch, (AHEAD, 0), (1, 1))), (2, maps.finish)])
        return carry

    def convert_right(w, carry):
        load(right, w).wait()
        high, low = halves(envs[lax.rem(w, 2)] * (w < count).astype(F32))
        for j in range(c):
            rows_of = pl.ds(pl.multiple_of((j * ops_here + w) * LANES, LANES), LANES)
            rights[rows_of, pl.ds(0, n)] = high[j * LANES:(j + 1) * LANES]
            rights[rows_of, pl.ds(n, n)] = low[j * LANES:(j + 1) * LANES]

        @pl.when(w < ops_here - 2)
        def _():
            load(right, w + 2).start()

        at(w, [(0, line(fetch, *middle(0))), (1, line(fetch, (AHEAD + 1, 0), (2, 1))), (3, line(fetch, *middle(1)))])
        return carry

    lax.fori_loop(0, ops_here, convert_left, 0)
    lax.fori_loop(0, ops_here, convert_right, 0)
    for j in range(AHEAD + 2, c):
        fetch.send_own(j)
    turn_in(fetch, 0)()

    def products(j, carry):
        for turn in range(c):
            @pl.when(j == turn)
            def _():
                line(fetch, (turn + 3, 1), *middle(turn + 2))()
                if turn < c - 2:
                    turn_in(fetch, turn + 1)()
                fetch.receive(turn)

        high, low = halves(fetch.landed[j])
        block[pl.ds(0, n), pl.ds(0, LANES)] = high
        block[pl.ds(n, n), pl.ds(0, LANES)] = high
        block[pl.ds(0, n), pl.ds(LANES, LANES)] = low
        for w in range(ops_here):
            both = bdot(lefts[pl.ds(w * n, n)], block[...])
            high, low = halves(both[:, :LANES] + both[:, LANES:])
            lp_high[:, pl.ds(w * LANES, LANES)] = high
            lp_low[:, pl.ds(w * LANES, LANES)] = low

        @pl.when(j == max(c - 3, 0))
        def _():
            if c > 1:
                turn_in(fetch, c - 1)()

        deep = pl.ds(pl.multiple_of(j * ops_here * LANES, LANES), ops_here * LANES)
        both = bdot(lp_high[...], rights[deep])
        sigma[...] += both[:, :n] + (both[:, n:] + bdot(lp_low[...], rights[deep, pl.ds(0, n)]))
        return carry

    lax.fori_loop(0, c, products, 0)

    side, core = p.o // CORES, lax.rem(p.o, CORES)
    mate = side * CORES + 1 - core
    facing = (1 - side) * CORES + core
    across_mate = (1 - side) * CORES + 1 - core
    q = p.quarter

    whole = polar_block
    polar = Polar(n, whole, cols, doubled, gram)

    def swap_cores(i, far, j):
        rows_of, at_cols = pl.ds((far * CORES + 1 - core) * q, q), pl.ds(j * LANES, LANES)
        return pltpu.make_async_remote_copy(
            sigma.at[rows_of, at_cols], first.at[i, :, at_cols], sum_sems.at[0, i, j], sum_sems.at[1, i, j],
            device_id=(p.s, mate), device_id_type=MESH)

    def over(j):
        at_cols = pl.ds(j * LANES, LANES)
        return pltpu.make_async_remote_copy(
            pair.at[:, at_cols], second.at[:, at_cols], sum_sems.at[0, 2, j], sum_sems.at[1, 2, j],
            device_id=(p.s, facing), device_id_type=MESH)

    def gather(i, sender, target, j):
        rows_of, at_cols = pl.ds(sender * q, q), pl.ds(j * LANES, LANES)
        source = quarter.at[:, at_cols] if i < 2 else whole.at[rows_of, at_cols]
        return pltpu.make_async_remote_copy(
            source, whole.at[rows_of, at_cols], gather_sems.at[0, i, j], gather_sems.at[1, i, j],
            device_id=(p.s, target), device_id_type=MESH)

    for j in range(c):
        swap_cores(0, 1 - side, j).start()
        swap_cores(1, side, j).start()
    for j in range(c + 1):
        if j < c:
            at_cols = pl.ds(j * LANES, LANES)
            swap_cores(0, 1 - side, j).wait_recv()
            pair[:, at_cols] = sigma[pl.ds(((1 - side) * CORES + core) * q, q), at_cols] + first[0, :, at_cols]
        if j:
            over(j - 1).start()
    for j in range(c + 1):
        if j < c:
            at_cols = pl.ds(j * LANES, LANES)
            swap_cores(1, side, j).wait_recv()
            over(j).wait_recv()
            quarter[:, at_cols] = sigma[pl.ds(p.o * q, q), at_cols] + first[1, :, at_cols] + second[:, at_cols]
            whole[pl.ds(p.o * q, q), at_cols] = quarter[:, at_cols]
        if j:
            again.begin(j - 1)
            gather(1, p.o, facing, j - 1).start()
            gather(0, p.o, mate, j - 1).start()
        if j > 1:
            again.send_own(j - 2)
    again.send_own(c - 1)
    for j in range(c):
        gather(1, facing, facing, j).wait_recv()
        gather(2, facing, mate, j).start()
        if j < 2:
            line(again, (j, 1), *middle(j))()
    for j in range(c):
        gather(0, mate, mate, j).wait_recv()
        gather(2, across_mate, mate, j).wait_recv()
        gather(2, facing, mate, j).wait_send()
    polar.normalise(whole[...])

    def group(turn):
        def event():
            line(again, (turn + 2, 1), *middle(turn + 2))()
            turn_in(again, turn)()
        return event

    def own_step(step, carry):
        polar.form_gram()
        polar.apply()
        at(step, [(turn, group(turn)) for turn in range(min(c, POLAR))])
        return carry

    lax.fori_loop(0, POLAR, own_step, 0)
    for turn in range(POLAR, c):
        group(turn)()
    tensor = (whole[...] * math.sqrt(n)).T
    whole[...] = tensor
    own_columns[...] = whole[pl.ds(pl.multiple_of(p.o * q, q), q)]
    gram[pl.ds(0, n)], gram[pl.ds(n, n)] = halves(tensor)

    def half_rotate(w, carry):
        rows_of = pl.ds(pl.multiple_of(w * n, n), n)
        both = bdot(gram[pl.ds(0, n)], lefts[rows_of])
        turned = both[:, :n] + (both[:, n:] + bdot(gram[pl.ds(n, n)], lefts[rows_of, pl.ds(0, n)]))
        rights[rows_of, pl.ds(0, n)], rights[rows_of, pl.ds(n, n)] = halves(turned)
        pltpu.make_async_copy(rights.at[rows_of], half_out.at[rows_of], out_sems.at[w]).start()
        return carry

    lax.fori_loop(0, ops_here, half_rotate, 0)
    for j in range(c):
        again.receive(j)
    save = pltpu.make_async_copy(again.landed, source_out, out_sems.at[ops_here])
    save.start()
    for w in range(ops_here):
        rows_of = pl.ds(w * n, n)
        pltpu.make_async_copy(rights.at[rows_of], half_out.at[rows_of], out_sems.at[w]).wait()
    fetch.drain()
    again.drain()
    for j in range(c):
        swap_cores(0, 1 - side, j).wait_send()
        swap_cores(1, side, j).wait_send()
        over(j).wait_send()
        gather(1, p.o, facing, j).wait_send()
        gather(0, p.o, mate, j).wait_send()
    save.wait()


def last_kernel(n, ops_here, chunks, source, half, columns, own_columns, rotated, block, cols, doubled, gram, halves_in,
                products, in_sems, out_sems):
    def load(w):
        at = pl.ds(w * n, n)
        return pltpu.make_async_copy(half.at[at], halves_in.at[at], in_sems.at[w])

    def store(w):
        return pltpu.make_async_copy(products.at[w], rotated.at[w], out_sems.at[w])

    for w in range(ops_here):
        load(w).start()
    own_columns[...] = columns[...]
    polar = Polar(n, block, cols, doubled, gram)
    polar.normalise(jnp.concatenate([source[j] for j in range(chunks)], axis=1))

    def step(_, carry):
        polar.form_gram()
        polar.apply()
        return carry

    lax.fori_loop(0, POLAR, step, 0)
    high, low = halves(block[...] * math.sqrt(n))
    cols[:, pl.ds(0, n)] = high
    cols[:, pl.ds(n, n)] = low

    def rotate(w, carry):
        load(w).wait()
        rows_of = pl.ds(pl.multiple_of(w * n, n), n)
        both = bdot(halves_in[rows_of, pl.ds(0, n)], cols[...])
        products[w] = both[:, :n] + (both[:, n:] + bdot(halves_in[rows_of, pl.ds(n, n)], cols[:, pl.ds(0, n)]))
        store(w).start()
        return carry

    lax.fori_loop(0, ops_here, rotate, 0)
    for w in range(ops_here):
        store(w).wait()


def vmem():
    return pl.BlockSpec(memory_space=pltpu.VMEM)


def scalar():
    return pl.BlockSpec(memory_space=pltpu.SMEM)


def anywhere():
    return pl.BlockSpec(memory_space=pl.ANY)


def shards_planes(place, wavefunction, left_env, right_env, shift_map, op_counts):
    c, n, q, ops_here = place.chunks, place.states, place.quarter, left_env.shape[1]
    fetches = []
    for _ in range(2):
        held, stage, *sems = Fetch.scratch(place)
        fetches += [*held, stage, *sems, pltpu.VMEM((c, n, LANES), F32)]
    columns, half, source = pl.pallas_call(
        functools.partial(site_kernel, place, ops_here),
        out_shape=(
            jax.ShapeDtypeStruct((q, n), F32),
            jax.ShapeDtypeStruct((ops_here * n, 2 * n), BF16),
            jax.ShapeDtypeStruct((c, n, LANES), F32),
        ),
        in_specs=[anywhere(), anywhere(), anywhere(), scalar(), scalar()],
        out_specs=(vmem(), anywhere(), anywhere()),
        scratch_shapes=[
            *Maps.scratch(place), *fetches,
            pltpu.VMEM((ops_here * n, 2 * n), BF16),
            pltpu.VMEM((ops_here * n, 2 * n), BF16),
            pltpu.VMEM((2 * n, 2 * LANES), BF16),
            pltpu.VMEM((2, n, n), F32),
            pltpu.SemaphoreType.DMA((2,)),
            pltpu.VMEM((n, ops_here * LANES), BF16),
            pltpu.VMEM((n, ops_here * LANES), BF16),
            pltpu.VMEM((n, n), F32),
            pltpu.VMEM((2, q, n), F32),
            pltpu.VMEM((q, n), F32),
            pltpu.VMEM((q, n), F32),
            pltpu.SemaphoreType.DMA((2, 3, c)),
            pltpu.VMEM((q, n), F32),
            pltpu.SemaphoreType.DMA((2, 3, c)),
            pltpu.VMEM((n, n), F32),
            *Polar.scratch(n),
            pltpu.SemaphoreType.DMA((ops_here + 1,)),
        ],
        compiler_params=pltpu.CompilerParams(collective_id=0, has_side_effects=True, vmem_limit_bytes=60 * 2**20),
    )(wavefunction[0], left_env[0], right_env[0], shift_map, op_counts)
    own_columns, rotated = pl.pallas_call(
        functools.partial(last_kernel, n, ops_here, c),
        out_shape=(jax.ShapeDtypeStruct((q, n), F32), jax.ShapeDtypeStruct((ops_here, n, n), F32)),
        in_specs=[vmem(), anywhere(), vmem()],
        out_specs=(vmem(), anywhere()),
        scratch_shapes=[
            pltpu.VMEM((n, n), F32),
            *Polar.scratch(n),
            pltpu.VMEM((ops_here * n, 2 * n), BF16),
            pltpu.VMEM((ops_here, n, n), F32),
            pltpu.SemaphoreType.DMA((ops_here,)),
            pltpu.SemaphoreType.DMA((ops_here,)),
        ],
        compiler_params=pltpu.CompilerParams(vmem_limit_bytes=60 * 2**20),
    )(source, half, columns)
    return own_columns.T[None], rotated[None]


def line_split(sector_count):
    rows = 1
    while rows * 2 * rows * 2 <= sector_count and sector_count % (rows * 2) == 0:
        rows *= 2
    return rows


def solution(mesh):
    def shards(wavefunction, left_env, right_env, shift_map, op_counts):
        nsec, nops = mesh.shape["sector"], mesh.shape["ops"]
        states = wavefunction.shape[1]
        ny = line_split(nsec)
        fits = nops == 2 * CORES and ny == 2 and states % LANES == 0 and states % (nops * ny * SUBLANES) == 0
        if not fits:
            return shards_general(wavefunction, left_env, right_env, shift_map, op_counts)
        place = Place(nsec, nops, ny, states)
        return shards_planes(place, wavefunction, left_env, right_env, shift_map, op_counts)

    return jax.shard_map(
        shards,
        mesh=mesh,
        in_specs=(
            P("sector", None, None),
            P("sector", "ops", None, None),
            P("sector", "ops", None, None),
            P("ops", None),
            P("ops", "sector"),
        ),
        out_specs=(P("sector", None, "ops"), P("sector", "ops", None, None)),
        check_vma=False,
    )
```

```python
import functools
import math

import jax
import jax.numpy as jnp
from jax import lax
from jax.experimental import pallas as pl
from jax.experimental.pallas import tpu as pltpu
from jax.sharding import PartitionSpec as P

POLAR = 5
LANES, SUBLANES = 128, 8
CORES = 2
AHEAD = 3
MESH = pl.DeviceIdType.MESH
F32, BF16 = jnp.float32, jnp.bfloat16

precise = lax.Precision.HIGH


def dot(a, b):
    return jnp.dot(a, b, precision=precise, preferred_element_type=jnp.float32)


def to_tiles(block, padded):
    rows, cols = block.shape
    tiles = block.reshape(rows // SUBLANES, SUBLANES, cols // LANES, LANES)
    tiles = tiles.transpose(0, 2, 1, 3).reshape(rows * cols // (SUBLANES * LANES), SUBLANES, LANES)
    return jnp.pad(tiles, ((0, padded - tiles.shape[0]), (0, 0), (0, 0)))


def from_tiles(tiles, rows, cols):
    tiles = tiles[: rows * cols // (SUBLANES * LANES)]
    tiles = tiles.reshape(rows // SUBLANES, cols // LANES, SUBLANES, LANES)
    return tiles.transpose(0, 2, 1, 3).reshape(rows, cols)


def swap(value, axis, bit):
    size = lax.axis_size(axis)
    return lax.ppermute(value, axis, [(i, i ^ bit) for i in range(size)])


def sum_scatter(tiles, axis):
    size, here = lax.axis_size(axis), lax.axis_index(axis)
    rest = tiles.reshape((size, tiles.shape[0] // size) + tiles.shape[1:])
    bit = 1
    while bit < size:
        mine = (here // bit) % 2
        pairs = rest.reshape((rest.shape[0] // 2, 2) + rest.shape[1:])
        keep = lax.dynamic_index_in_dim(pairs, mine, 1, keepdims=False)
        give = lax.dynamic_index_in_dim(pairs, 1 - mine, 1, keepdims=False)
        rest = keep + swap(give, axis, bit)
        bit *= 2
    return rest[0]


def gather_whole(quarter, axis):
    size, here = lax.axis_size(axis), lax.axis_index(axis)
    held = quarter[None]
    bit = size // 2
    while bit:
        mine = (here // bit) % 2
        other = swap(held, axis, bit)
        first = jnp.where(mine == 0, held, other)
        second = jnp.where(mine == 0, other, held)
        held = jnp.stack([first, second], axis=1).reshape((-1,) + quarter.shape)
        bit //= 2
    return held.reshape((-1,) + quarter.shape[1:])


def polar(sigma_block):
    states = sigma_block.shape[0]
    mean_sq = jnp.sum(sigma_block * sigma_block) / float(states * states)
    iterate = sigma_block * (lax.rsqrt(states * mean_sq + 1e-06) / 2.2)

    def step(_, iterate):
        gram_matrix = jnp.einsum("ab,cb->ac", iterate, iterate, precision=precise)
        return 1.5 * iterate - 0.5 * dot(gram_matrix, iterate)

    return lax.fori_loop(0, POLAR, step, iterate) * math.sqrt(states)


def shards_general(wavefunction, left_env, right_env, shift_map, op_counts):
    sector_count = lax.axis_size("sector")
    group_size = lax.axis_size("ops")
    group_here = lax.axis_index("ops")
    states = wavefunction.shape[1]
    ops_here = left_env.shape[1]
    parts = sector_count * group_size
    piece = -(-states * states // (SUBLANES * LANES * parts))
    padded = piece * parts
    quarter = piece * sector_count

    whole_map = lax.all_gather(shift_map[0], "ops").reshape(parts)

    def fetch_from_quarter(own_quarter):
        pieces = own_quarter.reshape(sector_count, piece, SUBLANES, LANES)
        spread = lax.all_to_all(pieces, "sector", split_axis=0, concat_axis=0, tiled=True)
        picked = jnp.take(spread, whole_map, axis=0)
        landed = lax.all_to_all(picked, ("ops", "sector"), split_axis=0, concat_axis=0, tiled=True)
        return from_tiles(landed.reshape(padded, SUBLANES, LANES), states, states)

    psi_tiles = to_tiles(wavefunction[0], padded)
    psi_quarter = lax.dynamic_slice_in_dim(psi_tiles, group_here * quarter, quarter, 0)
    moved_block = fetch_from_quarter(psi_quarter)

    left, right = left_env[0], right_env[0]
    count = op_counts[0, 0]
    active = (jnp.arange(ops_here) < count).astype(jnp.float32)
    left_psi = jnp.einsum("wab,bc->wac", left, moved_block, precision=precise) * active[:, None, None]
    partial_sigma = jnp.einsum("wac,wcd->ad", left_psi, right, precision=precise)

    sigma_quarter = sum_scatter(to_tiles(partial_sigma, padded), "ops")
    source_sigma = fetch_from_quarter(sigma_quarter)
    sigma_block = from_tiles(gather_whole(sigma_quarter, "ops"), states, states)

    whole_tensor = polar(sigma_block)
    column_width = states // group_size
    own_columns = lax.dynamic_slice_in_dim(whole_tensor, group_here * column_width, column_width, 1)
    half_rotated = jnp.einsum("ba,wbc->wac", whole_tensor, left, precision=precise)
    source_tensor = polar(source_sigma)
    rotated = jnp.einsum("wac,cd->wad", half_rotated, source_tensor, precision=precise)
    return (own_columns[None], rotated[None])


def halves(value):
    high = value.astype(BF16)
    return high, (value - high.astype(F32)).astype(BF16)


def bdot(a, b):
    return jnp.dot(a, b, preferred_element_type=F32)


class Place:
    def __init__(self, nsec, nops, ny, states):
        self.nsec, self.nops, self.ny, self.nz = nsec, nops, ny, nsec // ny
        self.states = states
        self.chunks = states // LANES
        self.parts = nops * ny
        self.rows = states // self.parts
        self.quarter = states // nops
        self.dests = nops * ny

    def locate(self):
        self.s, self.o = lax.axis_index("sector"), lax.axis_index("ops")
        self.z, self.y = self.s // self.ny, lax.rem(self.s, self.ny)
        self.part = self.o * self.ny + self.y

    def plane_peer(self, index, sign=1):
        dy, do = index // self.nops, index % self.nops
        if sign < 0:
            dy, do = (self.ny - dy) % self.ny, (self.nops - do) % self.nops
        return lax.rem(self.y + dy, self.ny), lax.rem(self.o + do, self.nops)

    def greet(self):
        barrier = pltpu.get_barrier_semaphore()
        for index in range(1, self.dests):
            y, o = self.plane_peer(index)
            pl.semaphore_signal(barrier, inc=1, device_id=(self.z * self.ny + y, o), device_id_type=MESH)

        @pl.when(self.z > 0)
        def _():
            pl.semaphore_signal(barrier, inc=1, device_id=(self.s - self.ny, self.o), device_id_type=MESH)

        @pl.when(self.z < self.nz - 1)
        def _():
            pl.semaphore_signal(barrier, inc=1, device_id=(self.s + self.ny, self.o), device_id_type=MESH)

        line = (self.z > 0).astype(jnp.int32) + (self.z < self.nz - 1).astype(jnp.int32)
        pl.semaphore_wait(barrier, self.dests - 1 + line)


class Maps:
    def __init__(self, place, table, own_ref, rows_ref, scalars_ref, sems):
        self.place, self.table = place, table
        self.own, self.rows, self.scalars, self.sems = own_ref, rows_ref, scalars_ref, sems

    @staticmethod
    def scratch(place):
        return [
            pltpu.VMEM((1, LANES), jnp.int32),
            pltpu.VMEM((place.nops, 1, LANES), jnp.int32),
            pltpu.SMEM((place.nops, 1, LANES), jnp.int32),
            pltpu.SemaphoreType.DMA((3, place.nops)),
        ]

    def write(self):
        lane = lax.broadcasted_iota(jnp.int32, (1, LANES), 1)
        row = jnp.zeros((1, LANES), jnp.int32)
        for sector in range(self.place.nsec):
            row = jnp.where(lane == sector, self.table[0, sector], row)
        self.own[...] = row

    def copy(self, offset, sign):
        p = self.place
        peer = lax.rem(p.o + offset, p.nops)
        slot = p.o if sign > 0 else lax.rem(p.o + p.nops - offset, p.nops)
        return pltpu.make_async_remote_copy(
            self.own, self.rows.at[slot], self.sems.at[0, offset], self.sems.at[1, offset],
            device_id=(p.s, peer), device_id_type=MESH)

    def start(self):
        for offset in range(1, self.place.nops):
            self.copy(offset, 1).start()
        pltpu.make_async_copy(self.own, self.rows.at[self.place.o], self.sems.at[2, 0]).start()

    def finish(self):
        for offset in range(1, self.place.nops):
            self.copy(offset, 1).wait_send()
            self.copy(offset, -1).wait_recv()
        pltpu.make_async_copy(self.own, self.rows.at[self.place.o], self.sems.at[2, 0]).wait()
        landed = pltpu.make_async_copy(self.rows, self.scalars, self.sems.at[2, 1])
        landed.start()
        landed.wait()

    def want(self, y, o):
        return self.scalars[o, 0, self.place.z * self.place.ny + y]


class Fetch:
    def __init__(self, place, maps, piece, held, stage, landed, up, down, across, within, local):
        self.place, self.maps, self.piece = place, maps, piece
        self.held, self.stage, self.landed = held, stage, landed
        self.up, self.down, self.across, self.within, self.local = up, down, across, within, local

    @staticmethod
    def scratch(place):
        c, dma = place.chunks, pltpu.SemaphoreType.DMA
        return (
            [pltpu.VMEM((place.nsec, place.rows, LANES), F32) for _ in range(c)],
            pltpu.VMEM((c, place.dests, place.rows, LANES), F32),
            dma((2, c, place.nz - 1)),
            dma((2, c, place.nz - 1)),
            dma((2, c, place.ny)),
            dma((2, c, place.dests)),
            dma((c,)),
        )

    def across_copy(self, j, dy, sign):
        p = self.place
        y = lax.rem(p.y + dy, p.ny)
        slot = p.s if sign > 0 else p.z * p.ny + lax.rem(p.y + p.ny - dy, p.ny)
        return pltpu.make_async_remote_copy(
            self.piece(j, y), self.held[j].at[slot], self.across.at[0, j, dy], self.across.at[1, j, dy],
            device_id=(p.z * p.ny + y, p.o), device_id_type=MESH)

    def own_copy(self, j):
        p = self.place
        return pltpu.make_async_copy(self.piece(j, p.y), self.held[j].at[p.s], self.local.at[j])

    def begin(self, j):
        for dy in range(1, self.place.ny):
            self.across_copy(j, dy, 1).start()
        self.own_copy(j).start()

    def line_copy(self, j, k, direction):
        p = self.place
        slab = self.held[j].at[pl.ds((p.z - direction * k) * p.ny, p.ny)]
        sems = self.up if direction > 0 else self.down
        return pltpu.make_async_remote_copy(
            slab, slab, sems.at[0, j, k], sems.at[1, j, k],
            device_id=(p.s + direction * p.ny, p.o), device_id_type=MESH)

    def line_wait(self, j, k, direction):
        p = self.place
        slab = self.held[j].at[pl.ds((p.z - direction * k) * p.ny, p.ny)]
        sems = self.up if direction > 0 else self.down
        pltpu.make_async_remote_copy(
            slab, slab, sems.at[0, j, k - 1], sems.at[1, j, k - 1],
            device_id=(p.s - direction * p.ny, p.o), device_id_type=MESH).wait_recv()

    def has(self, k, direction):
        return self.place.z >= k if direction > 0 else self.place.z < self.place.nz - k

    def more(self, direction):
        return self.place.z < self.place.nz - 1 if direction > 0 else self.place.z > 0

    def send_own(self, j):
        for dy in range(1, self.place.ny):
            self.across_copy(j, dy, -1).wait_recv()
        self.own_copy(j).wait()
        for direction in (1, -1):
            @pl.when(self.more(direction))
            def _():
                self.line_copy(j, 0, direction).start()

    def forward(self, j, k):
        for direction in (1, -1):
            @pl.when(self.has(k, direction))
            def _():
                self.line_wait(j, k, direction)

            if k < self.place.nz - 1:
                @pl.when(self.has(k, direction) & self.more(direction))
                def _():
                    self.line_copy(j, k, direction).start()

    def within_copy(self, j, index, sign):
        p = self.place
        y, o = p.plane_peer(index, sign)
        part = p.part if sign > 0 else o * p.ny + y
        return pltpu.make_async_remote_copy(
            self.stage.at[j, index], self.landed.at[j, pl.ds(part * p.rows, p.rows)],
            self.within.at[0, j, index], self.within.at[1, j, index],
            device_id=(p.z * p.ny + y, o), device_id_type=MESH)

    def hand_out(self, j):
        p = self.place
        order = sorted(range(p.dests), key=lambda index: -((index // p.nops > 0) + (index % p.nops > 0)))
        for index in order:
            y, o = p.plane_peer(index)
            picked = self.held[j][self.maps.want(y, o)]
            if index == 0:
                self.landed[j, pl.ds(p.part * p.rows, p.rows)] = picked
            else:
                self.stage[j, index] = picked
        for index in order:
            if index:
                self.within_copy(j, index, 1).start()

    def receive(self, j):
        for index in range(1, self.place.dests):
            self.within_copy(j, index, -1).wait_recv()

    def drain(self):
        for j in range(self.place.chunks):
            for dy in range(1, self.place.ny):
                self.across_copy(j, dy, 1).wait_send()
            for direction in (1, -1):
                for k in range(self.place.nz - 1):
                    @pl.when(self.has(k, direction) & self.more(direction))
                    def _():
                        self.line_copy(j, k, direction).wait_send()
            for index in range(1, self.place.dests):
                self.within_copy(j, index, 1).wait_send()


def tdot(a, b):
    return lax.dot_general(a, b, (((1,), (1,)), ((), ())), preferred_element_type=F32)


class Polar:
    def __init__(self, n, block, cols, rows, gram):
        self.n, self.block, self.cols, self.rows, self.gram = n, block, cols, rows, gram

    @staticmethod
    def scratch(n):
        return [pltpu.VMEM((n, 2 * n), BF16), pltpu.VMEM((2 * n, n), BF16), pltpu.VMEM((2 * n, n), BF16)]

    def normalise(self, sigma):
        n = self.n
        squares = jnp.sum(jnp.sum(sigma * sigma, axis=0, keepdims=True), axis=1, keepdims=True)
        self.block[...] = sigma * (lax.rsqrt(n * (squares / float(n * n)) + 1e-06) / 2.2)

    def form_gram(self):
        n = self.n
        high, low = halves(self.block[...])
        self.cols[:, pl.ds(0, n)] = high
        self.cols[:, pl.ds(n, n)] = low
        self.rows[pl.ds(0, n)] = high
        self.rows[pl.ds(n, n)] = low
        both = tdot(high, self.rows[...])
        cross = both[:, n:]
        self.gram[pl.ds(0, n)], self.gram[pl.ds(n, n)] = halves(both[:, :n] + (cross + cross.T))

    def apply(self, scale=None):
        n = self.n
        both = bdot(self.gram[pl.ds(0, n)], self.cols[...])
        moved = both[:, :n] + (both[:, n:] + bdot(self.gram[pl.ds(n, n)], self.cols[:, pl.ds(0, n)]))
        value = 1.5 * self.block[...] - 0.5 * moved
        self.block[...] = value if scale is None else value * scale


def site_kernel(place, ops_here, psi, left, right, table, counts, own_columns, half_out, source_out, map_row, rows,
                scalars, map_sems, *rest):
    c, n = place.chunks, place.states
    groups = []
    for _ in range(2):
        groups.append((rest[:c], rest[c:c + 6], rest[c + 6]))
        rest = rest[c + 7:]
    (lefts, rights, block, envs, env_sems, lp_high, lp_low, sigma, first, second, pair, sum_sems,
     quarter, gather_sems, polar_block, cols, doubled, gram, out_sems) = rest
    place.locate()
    p = place

    def load(ref, w):
        slot = w % 2 if isinstance(w, int) else lax.rem(w, 2)
        return pltpu.make_async_copy(ref.at[w], envs.at[slot], env_sems.at[slot])

    load(left, 0).start()
    load(left, 1).start()
    maps = Maps(place, table, map_row, rows, scalars, map_sems)
    maps.write()
    place.greet()

    def fetch_of(piece, group):
        held, (stage, up, down, across, within, local), landed = group
        return Fetch(place, maps, piece, held, stage, landed, up, down, across, within, local)

    fetch = fetch_of(lambda j, y: psi.at[pl.ds((p.o * p.ny + y) * p.rows, p.rows), pl.ds(j * LANES, LANES)], groups[0])
    again = fetch_of(lambda j, y: quarter.at[pl.ds(y * p.rows, p.rows), pl.ds(j * LANES, LANES)], groups[1])
    maps.start()
    for j in range(c):
        fetch.begin(j)
    for j in range(min(AHEAD, c)):
        fetch.send_own(j)
    count = counts[0, 0]
    sigma[...] = jnp.zeros((n, n), F32)
    block[pl.ds(n, n), pl.ds(LANES, LANES)] = jnp.zeros((n, LANES), BF16)

    def at(index, events):
        for turn, event in events:
            pl.when(index == turn)(event)

    def line(which, *steps):
        def event():
            for j, k in steps:
                if j < c:
                    which.send_own(j) if k == 0 else which.forward(j, k)
        return event

    def turn_in(which, j):
        def event():
            if j < c:
                which.forward(j, p.nz - 1)
                which.hand_out(j)
        return event

    def middle(j):
        return [(j, k) for k in range(2, p.nz - 1)]

    def convert_left(w, carry):
        load(left, w).wait()
        high, low = halves(envs[lax.rem(w, 2)])
        rows_of = pl.ds(pl.multiple_of(w * n, n), n)
        lefts[rows_of, pl.ds(0, n)] = high
        lefts[rows_of, pl.ds(n, n)] = low

        @pl.when(w < ops_here - 2)
        def _():
            load(left, w + 2).start()

        @pl.when(w >= ops_here - 2)
        def _():
            load(right, w + 2 - ops_here).start()

        at(w, [(1, line(fetch, (0, 1))), (2, line(fetch, (AHEAD, 0), (1, 1))), (2, maps.finish)])
        return carry

    def convert_right(w, carry):
        load(right, w).wait()
        high, low = halves(envs[lax.rem(w, 2)] * (w < count).astype(F32))
        for j in range(c):
            rows_of = pl.ds(pl.multiple_of((j * ops_here + w) * LANES, LANES), LANES)
            rights[rows_of, pl.ds(0, n)] = high[j * LANES:(j + 1) * LANES]
            rights[rows_of, pl.ds(n, n)] = low[j * LANES:(j + 1) * LANES]

        @pl.when(w < ops_here - 2)
        def _():
            load(right, w + 2).start()

        at(w, [(0, line(fetch, *middle(0))), (1, line(fetch, (AHEAD + 1, 0), (2, 1))), (3, line(fetch, *middle(1)))])
        return carry

    lax.fori_loop(0, ops_here, convert_left, 0)
    lax.fori_loop(0, ops_here, convert_right, 0)
    for j in range(AHEAD + 2, c):
        fetch.send_own(j)
    turn_in(fetch, 0)()

    def products(j, carry):
        for turn in range(c):
            @pl.when(j == turn)
            def _():
                line(fetch, (turn + 3, 1), *middle(turn + 2))()
                if turn < c - 2:
                    turn_in(fetch, turn + 1)()
                fetch.receive(turn)

        high, low = halves(fetch.landed[j])
        block[pl.ds(0, n), pl.ds(0, LANES)] = high
        block[pl.ds(n, n), pl.ds(0, LANES)] = high
        block[pl.ds(0, n), pl.ds(LANES, LANES)] = low
        for w in range(ops_here):
            both = bdot(lefts[pl.ds(w * n, n)], block[...])
            high, low = halves(both[:, :LANES] + both[:, LANES:])
            lp_high[:, pl.ds(w * LANES, LANES)] = high
            lp_low[:, pl.ds(w * LANES, LANES)] = low

        @pl.when(j == max(c - 3, 0))
        def _():
            if c > 1:
                turn_in(fetch, c - 1)()

        deep = pl.ds(pl.multiple_of(j * ops_here * LANES, LANES), ops_here * LANES)
        both = bdot(lp_high[...], rights[deep])
        sigma[...] += both[:, :n] + (both[:, n:] + bdot(lp_low[...], rights[deep, pl.ds(0, n)]))
        return carry

    lax.fori_loop(0, c, products, 0)

    side, core = p.o // CORES, lax.rem(p.o, CORES)
    mate = side * CORES + 1 - core
    facing = (1 - side) * CORES + core
    across_mate = (1 - side) * CORES + 1 - core
    q = p.quarter

    whole = polar_block
    polar = Polar(n, whole, cols, doubled, gram)

    def swap_cores(i, far, j):
        rows_of, at_cols = pl.ds((far * CORES + 1 - core) * q, q), pl.ds(j * LANES, LANES)
        return pltpu.make_async_remote_copy(
            sigma.at[rows_of, at_cols], first.at[i, :, at_cols], sum_sems.at[0, i, j], sum_sems.at[1, i, j],
            device_id=(p.s, mate), device_id_type=MESH)

    def over(j):
        at_cols = pl.ds(j * LANES, LANES)
        return pltpu.make_async_remote_copy(
            pair.at[:, at_cols], second.at[:, at_cols], sum_sems.at[0, 2, j], sum_sems.at[1, 2, j],
            device_id=(p.s, facing), device_id_type=MESH)

    def gather(i, sender, target, j):
        rows_of, at_cols = pl.ds(sender * q, q), pl.ds(j * LANES, LANES)
        source = quarter.at[:, at_cols] if i < 2 else whole.at[rows_of, at_cols]
        return pltpu.make_async_remote_copy(
            source, whole.at[rows_of, at_cols], gather_sems.at[0, i, j], gather_sems.at[1, i, j],
            device_id=(p.s, target), device_id_type=MESH)

    for j in range(c):
        swap_cores(0, 1 - side, j).start()
        swap_cores(1, side, j).start()
    for j in range(c + 1):
        if j < c:
            at_cols = pl.ds(j * LANES, LANES)
            swap_cores(0, 1 - side, j).wait_recv()
            pair[:, at_cols] = sigma[pl.ds(((1 - side) * CORES + core) * q, q), at_cols] + first[0, :, at_cols]
        if j:
            over(j - 1).start()
    for j in range(c + 1):
        if j < c:
            at_cols = pl.ds(j * LANES, LANES)
            swap_cores(1, side, j).wait_recv()
            over(j).wait_recv()
            quarter[:, at_cols] = sigma[pl.ds(p.o * q, q), at_cols] + first[1, :, at_cols] + second[:, at_cols]
            whole[pl.ds(p.o * q, q), at_cols] = quarter[:, at_cols]
        if j:
            again.begin(j - 1)
            gather(1, p.o, facing, j - 1).start()
            gather(0, p.o, mate, j - 1).start()
        if j > 1:
            again.send_own(j - 2)
    again.send_own(c - 1)
    for j in range(c):
        gather(1, facing, facing, j).wait_recv()
        gather(2, facing, mate, j).start()
        again.forward(j, 1)
    line(again, *middle(0), *middle(1))()
    for j in range(c):
        gather(0, mate, mate, j).wait_recv()
        gather(2, across_mate, mate, j).wait_recv()
        gather(2, facing, mate, j).wait_send()
    polar.normalise(whole[...])

    def group(turn):
        def event():
            line(again, *middle(turn + 2))()
            if turn:
                turn_in(again, turn - 1)()
        return event

    def own_step(step, carry):
        polar.form_gram()
        polar.apply()
        at(step, [(turn, group(turn)) for turn in range(min(c, POLAR))])
        return carry

    lax.fori_loop(0, POLAR, own_step, 0)
    for turn in range(POLAR, c):
        group(turn)()
    tensor = (whole[...] * math.sqrt(n)).T
    whole[...] = tensor
    own_columns[...] = whole[pl.ds(pl.multiple_of(p.o * q, q), q)]
    gram[pl.ds(0, n)], gram[pl.ds(n, n)] = halves(tensor)

    def half_rotate(w, carry):
        rows_of = pl.ds(pl.multiple_of(w * n, n), n)
        both = bdot(gram[pl.ds(0, n)], lefts[rows_of])
        turned = both[:, :n] + (both[:, n:] + bdot(gram[pl.ds(n, n)], lefts[rows_of, pl.ds(0, n)]))
        rights[rows_of, pl.ds(0, n)], rights[rows_of, pl.ds(n, n)] = halves(turned)
        pltpu.make_async_copy(rights.at[rows_of], half_out.at[rows_of], out_sems.at[w]).start()
        at(w, [(0, turn_in(again, c - 1))])
        return carry

    lax.fori_loop(0, ops_here, half_rotate, 0)
    for j in range(c):
        again.receive(j)
    save = pltpu.make_async_copy(again.landed, source_out, out_sems.at[ops_here])
    save.start()
    for w in range(ops_here):
        rows_of = pl.ds(w * n, n)
        pltpu.make_async_copy(rights.at[rows_of], half_out.at[rows_of], out_sems.at[w]).wait()
    fetch.drain()
    again.drain()
    for j in range(c):
        swap_cores(0, 1 - side, j).wait_send()
        swap_cores(1, side, j).wait_send()
        over(j).wait_send()
        gather(1, p.o, facing, j).wait_send()
        gather(0, p.o, mate, j).wait_send()
    save.wait()


def last_kernel(n, ops_here, chunks, source, half, columns, own_columns, rotated, block, cols, doubled, gram, halves_in,
                products, in_sems, out_sems):
    def load(w):
        at = pl.ds(w * n, n)
        return pltpu.make_async_copy(half.at[at], halves_in.at[at], in_sems.at[w])

    def store(w):
        return pltpu.make_async_copy(products.at[w], rotated.at[w], out_sems.at[w])

    for w in range(ops_here):
        load(w).start()
    own_columns[...] = columns[...]
    polar = Polar(n, block, cols, doubled, gram)
    polar.normalise(jnp.concatenate([source[j] for j in range(chunks)], axis=1))

    def step(_, carry):
        polar.form_gram()
        polar.apply()
        return carry

    lax.fori_loop(0, POLAR, step, 0)
    high, low = halves(block[...] * math.sqrt(n))
    cols[:, pl.ds(0, n)] = high
    cols[:, pl.ds(n, n)] = low

    def rotate(w, carry):
        load(w).wait()
        rows_of = pl.ds(pl.multiple_of(w * n, n), n)
        both = bdot(halves_in[rows_of, pl.ds(0, n)], cols[...])
        products[w] = both[:, :n] + (both[:, n:] + bdot(halves_in[rows_of, pl.ds(n, n)], cols[:, pl.ds(0, n)]))
        store(w).start()
        return carry

    lax.fori_loop(0, ops_here, rotate, 0)
    for w in range(ops_here):
        store(w).wait()


def vmem():
    return pl.BlockSpec(memory_space=pltpu.VMEM)


def scalar():
    return pl.BlockSpec(memory_space=pltpu.SMEM)


def anywhere():
    return pl.BlockSpec(memory_space=pl.ANY)


def shards_planes(place, wavefunction, left_env, right_env, shift_map, op_counts):
    c, n, q, ops_here = place.chunks, place.states, place.quarter, left_env.shape[1]
    fetches = []
    for _ in range(2):
        held, stage, *sems = Fetch.scratch(place)
        fetches += [*held, stage, *sems, pltpu.VMEM((c, n, LANES), F32)]
    columns, half, source = pl.pallas_call(
        functools.partial(site_kernel, place, ops_here),
        out_shape=(
            jax.ShapeDtypeStruct((q, n), F32),
            jax.ShapeDtypeStruct((ops_here * n, 2 * n), BF16),
            jax.ShapeDtypeStruct((c, n, LANES), F32),
        ),
        in_specs=[anywhere(), anywhere(), anywhere(), scalar(), scalar()],
        out_specs=(vmem(), anywhere(), anywhere()),
        scratch_shapes=[
            *Maps.scratch(place), *fetches,
            pltpu.VMEM((ops_here * n, 2 * n), BF16),
            pltpu.VMEM((ops_here * n, 2 * n), BF16),
            pltpu.VMEM((2 * n, 2 * LANES), BF16),
            pltpu.VMEM((2, n, n), F32),
            pltpu.SemaphoreType.DMA((2,)),
            pltpu.VMEM((n, ops_here * LANES), BF16),
            pltpu.VMEM((n, ops_here * LANES), BF16),
            pltpu.VMEM((n, n), F32),
            pltpu.VMEM((2, q, n), F32),
            pltpu.VMEM((q, n), F32),
            pltpu.VMEM((q, n), F32),
            pltpu.SemaphoreType.DMA((2, 3, c)),
            pltpu.VMEM((q, n), F32),
            pltpu.SemaphoreType.DMA((2, 3, c)),
            pltpu.VMEM((n, n), F32),
            *Polar.scratch(n),
            pltpu.SemaphoreType.DMA((ops_here + 1,)),
        ],
        compiler_params=pltpu.CompilerParams(collective_id=0, has_side_effects=True, vmem_limit_bytes=60 * 2**20),
    )(wavefunction[0], left_env[0], right_env[0], shift_map, op_counts)
    own_columns, rotated = pl.pallas_call(
        functools.partial(last_kernel, n, ops_here, c),
        out_shape=(jax.ShapeDtypeStruct((q, n), F32), jax.ShapeDtypeStruct((ops_here, n, n), F32)),
        in_specs=[vmem(), anywhere(), vmem()],
        out_specs=(vmem(), anywhere()),
        scratch_shapes=[
            pltpu.VMEM((n, n), F32),
            *Polar.scratch(n),
            pltpu.VMEM((ops_here * n, 2 * n), BF16),
            pltpu.VMEM((ops_here, n, n), F32),
            pltpu.SemaphoreType.DMA((ops_here,)),
            pltpu.SemaphoreType.DMA((ops_here,)),
        ],
        compiler_params=pltpu.CompilerParams(vmem_limit_bytes=60 * 2**20),
    )(source, half, columns)
    return own_columns.T[None], rotated[None]


def line_split(sector_count):
    rows = 1
    while rows * 2 * rows * 2 <= sector_count and sector_count % (rows * 2) == 0:
        rows *= 2
    return rows


def solution(mesh):
    def shards(wavefunction, left_env, right_env, shift_map, op_counts):
        nsec, nops = mesh.shape["sector"], mesh.shape["ops"]
        states = wavefunction.shape[1]
        ny = line_split(nsec)
        fits = nops == 2 * CORES and ny == 2 and states % LANES == 0 and states % (nops * ny * SUBLANES) == 0
        if not fits:
            return shards_general(wavefunction, left_env, right_env, shift_map, op_counts)
        place = Place(nsec, nops, ny, states)
        return shards_planes(place, wavefunction, left_env, right_env, shift_map, op_counts)

    return jax.shard_map(
        shards,
        mesh=mesh,
        in_specs=(
            P("sector", None, None),
            P("sector", "ops", None, None),
            P("sector", "ops", None, None),
            P("ops", None),
            P("ops", "sector"),
        ),
        out_specs=(P("sector", None, "ops"), P("sector", "ops", None, None)),
        check_vma=False,
    )
```

```python
import functools
import math

import jax
import jax.numpy as jnp
from jax import lax
from jax.experimental import pallas as pl
from jax.experimental.pallas import tpu as pltpu
from jax.sharding import PartitionSpec as P

POLAR = 5
LANES, SUBLANES = 128, 8
CORES = 2
AHEAD = 3
WIDE = 256
PAIR = 2
MESH = pl.DeviceIdType.MESH
F32, BF16 = jnp.float32, jnp.bfloat16

precise = lax.Precision.HIGH


def dot(a, b):
    return jnp.dot(a, b, precision=precise, preferred_element_type=jnp.float32)


def to_tiles(block, padded):
    rows, cols = block.shape
    tiles = block.reshape(rows // SUBLANES, SUBLANES, cols // LANES, LANES)
    tiles = tiles.transpose(0, 2, 1, 3).reshape(rows * cols // (SUBLANES * LANES), SUBLANES, LANES)
    return jnp.pad(tiles, ((0, padded - tiles.shape[0]), (0, 0), (0, 0)))


def from_tiles(tiles, rows, cols):
    tiles = tiles[: rows * cols // (SUBLANES * LANES)]
    tiles = tiles.reshape(rows // SUBLANES, cols // LANES, SUBLANES, LANES)
    return tiles.transpose(0, 2, 1, 3).reshape(rows, cols)


def swap(value, axis, bit):
    size = lax.axis_size(axis)
    return lax.ppermute(value, axis, [(i, i ^ bit) for i in range(size)])


def sum_scatter(tiles, axis):
    size, here = lax.axis_size(axis), lax.axis_index(axis)
    rest = tiles.reshape((size, tiles.shape[0] // size) + tiles.shape[1:])
    bit = 1
    while bit < size:
        mine = (here // bit) % 2
        pairs = rest.reshape((rest.shape[0] // 2, 2) + rest.shape[1:])
        keep = lax.dynamic_index_in_dim(pairs, mine, 1, keepdims=False)
        give = lax.dynamic_index_in_dim(pairs, 1 - mine, 1, keepdims=False)
        rest = keep + swap(give, axis, bit)
        bit *= 2
    return rest[0]


def gather_whole(quarter, axis):
    size, here = lax.axis_size(axis), lax.axis_index(axis)
    held = quarter[None]
    bit = size // 2
    while bit:
        mine = (here // bit) % 2
        other = swap(held, axis, bit)
        first = jnp.where(mine == 0, held, other)
        second = jnp.where(mine == 0, other, held)
        held = jnp.stack([first, second], axis=1).reshape((-1,) + quarter.shape)
        bit //= 2
    return held.reshape((-1,) + quarter.shape[1:])


def polar(sigma_block):
    states = sigma_block.shape[0]
    mean_sq = jnp.sum(sigma_block * sigma_block) / float(states * states)
    iterate = sigma_block * (lax.rsqrt(states * mean_sq + 1e-06) / 2.2)

    def step(_, iterate):
        gram_matrix = jnp.einsum("ab,cb->ac", iterate, iterate, precision=precise)
        return 1.5 * iterate - 0.5 * dot(gram_matrix, iterate)

    return lax.fori_loop(0, POLAR, step, iterate) * math.sqrt(states)


def shards_general(wavefunction, left_env, right_env, shift_map, op_counts):
    sector_count = lax.axis_size("sector")
    group_size = lax.axis_size("ops")
    group_here = lax.axis_index("ops")
    states = wavefunction.shape[1]
    ops_here = left_env.shape[1]
    parts = sector_count * group_size
    piece = -(-states * states // (SUBLANES * LANES * parts))
    padded = piece * parts
    quarter = piece * sector_count

    whole_map = lax.all_gather(shift_map[0], "ops").reshape(parts)

    def fetch_from_quarter(own_quarter):
        pieces = own_quarter.reshape(sector_count, piece, SUBLANES, LANES)
        spread = lax.all_to_all(pieces, "sector", split_axis=0, concat_axis=0, tiled=True)
        picked = jnp.take(spread, whole_map, axis=0)
        landed = lax.all_to_all(picked, ("ops", "sector"), split_axis=0, concat_axis=0, tiled=True)
        return from_tiles(landed.reshape(padded, SUBLANES, LANES), states, states)

    psi_tiles = to_tiles(wavefunction[0], padded)
    psi_quarter = lax.dynamic_slice_in_dim(psi_tiles, group_here * quarter, quarter, 0)
    moved_block = fetch_from_quarter(psi_quarter)

    left, right = left_env[0], right_env[0]
    count = op_counts[0, 0]
    active = (jnp.arange(ops_here) < count).astype(jnp.float32)
    left_psi = jnp.einsum("wab,bc->wac", left, moved_block, precision=precise) * active[:, None, None]
    partial_sigma = jnp.einsum("wac,wcd->ad", left_psi, right, precision=precise)

    sigma_quarter = sum_scatter(to_tiles(partial_sigma, padded), "ops")
    source_sigma = fetch_from_quarter(sigma_quarter)
    sigma_block = from_tiles(gather_whole(sigma_quarter, "ops"), states, states)

    whole_tensor = polar(sigma_block)
    column_width = states // group_size
    own_columns = lax.dynamic_slice_in_dim(whole_tensor, group_here * column_width, column_width, 1)
    half_rotated = jnp.einsum("ba,wbc->wac", whole_tensor, left, precision=precise)
    source_tensor = polar(source_sigma)
    rotated = jnp.einsum("wac,cd->wad", half_rotated, source_tensor, precision=precise)
    return (own_columns[None], rotated[None])


def halves(value):
    high = value.astype(BF16)
    return high, (value - high.astype(F32)).astype(BF16)


def bdot(a, b):
    return jnp.dot(a, b, preferred_element_type=F32)


class Place:
    def __init__(self, nsec, nops, ny, states):
        self.nsec, self.nops, self.ny, self.nz = nsec, nops, ny, nsec // ny
        self.states = states
        self.chunks = states // LANES
        self.parts = nops * ny
        self.rows = states // self.parts
        self.quarter = states // nops
        self.dests = nops * ny

    def locate(self):
        self.s, self.o = lax.axis_index("sector"), lax.axis_index("ops")
        self.z, self.y = self.s // self.ny, lax.rem(self.s, self.ny)
        self.part = self.o * self.ny + self.y

    def plane_peer(self, index, sign=1):
        dy, do = index // self.nops, index % self.nops
        if sign < 0:
            dy, do = (self.ny - dy) % self.ny, (self.nops - do) % self.nops
        return lax.rem(self.y + dy, self.ny), lax.rem(self.o + do, self.nops)

    def greet(self):
        barrier = pltpu.get_barrier_semaphore()
        for index in range(1, self.dests):
            y, o = self.plane_peer(index)
            pl.semaphore_signal(barrier, inc=1, device_id=(self.z * self.ny + y, o), device_id_type=MESH)

        @pl.when(self.z > 0)
        def _():
            pl.semaphore_signal(barrier, inc=1, device_id=(self.s - self.ny, self.o), device_id_type=MESH)

        @pl.when(self.z < self.nz - 1)
        def _():
            pl.semaphore_signal(barrier, inc=1, device_id=(self.s + self.ny, self.o), device_id_type=MESH)

        line = (self.z > 0).astype(jnp.int32) + (self.z < self.nz - 1).astype(jnp.int32)
        pl.semaphore_wait(barrier, self.dests - 1 + line)


class Maps:
    def __init__(self, place, table, own_ref, rows_ref, scalars_ref, sems):
        self.place, self.table = place, table
        self.own, self.rows, self.scalars, self.sems = own_ref, rows_ref, scalars_ref, sems

    @staticmethod
    def scratch(place):
        return [
            pltpu.VMEM((1, LANES), jnp.int32),
            pltpu.VMEM((place.nops, 1, LANES), jnp.int32),
            pltpu.SMEM((place.nops, 1, LANES), jnp.int32),
            pltpu.SemaphoreType.DMA((3, place.nops)),
        ]

    def write(self):
        lane = lax.broadcasted_iota(jnp.int32, (1, LANES), 1)
        row = jnp.zeros((1, LANES), jnp.int32)
        for sector in range(self.place.nsec):
            row = jnp.where(lane == sector, self.table[0, sector], row)
        self.own[...] = row

    def copy(self, offset, sign):
        p = self.place
        peer = lax.rem(p.o + offset, p.nops)
        slot = p.o if sign > 0 else lax.rem(p.o + p.nops - offset, p.nops)
        return pltpu.make_async_remote_copy(
            self.own, self.rows.at[slot], self.sems.at[0, offset], self.sems.at[1, offset],
            device_id=(p.s, peer), device_id_type=MESH)

    def start(self):
        for offset in range(1, self.place.nops):
            self.copy(offset, 1).start()
        pltpu.make_async_copy(self.own, self.rows.at[self.place.o], self.sems.at[2, 0]).start()

    def finish(self):
        for offset in range(1, self.place.nops):
            self.copy(offset, 1).wait_send()
            self.copy(offset, -1).wait_recv()
        pltpu.make_async_copy(self.own, self.rows.at[self.place.o], self.sems.at[2, 0]).wait()
        landed = pltpu.make_async_copy(self.rows, self.scalars, self.sems.at[2, 1])
        landed.start()
        landed.wait()

    def want(self, y, o):
        return self.scalars[o, 0, self.place.z * self.place.ny + y]


class Fetch:
    def __init__(self, place, maps, piece, held, stage, landed, up, down, across, within, local):
        self.place, self.maps, self.piece = place, maps, piece
        self.held, self.stage, self.landed = held, stage, landed
        self.up, self.down, self.across, self.within, self.local = up, down, across, within, local

    @staticmethod
    def scratch(place):
        c, dma = place.chunks, pltpu.SemaphoreType.DMA
        return (
            [pltpu.VMEM((place.nsec, place.rows, LANES), F32) for _ in range(c)],
            pltpu.VMEM((c, place.dests, place.rows, LANES), F32),
            dma((2, c, place.nz - 1)),
            dma((2, c, place.nz - 1)),
            dma((2, c, place.ny)),
            dma((2, c, place.dests)),
            dma((c,)),
        )

    def across_copy(self, j, dy, sign):
        p = self.place
        y = lax.rem(p.y + dy, p.ny)
        slot = p.s if sign > 0 else p.z * p.ny + lax.rem(p.y + p.ny - dy, p.ny)
        return pltpu.make_async_remote_copy(
            self.piece(j, y), self.held[j].at[slot], self.across.at[0, j, dy], self.across.at[1, j, dy],
            device_id=(p.z * p.ny + y, p.o), device_id_type=MESH)

    def own_copy(self, j):
        p = self.place
        return pltpu.make_async_copy(self.piece(j, p.y), self.held[j].at[p.s], self.local.at[j])

    def begin(self, j):
        for dy in range(1, self.place.ny):
            self.across_copy(j, dy, 1).start()
        self.own_copy(j).start()

    def line_copy(self, j, k, direction):
        p = self.place
        slab = self.held[j].at[pl.ds((p.z - direction * k) * p.ny, p.ny)]
        sems = self.up if direction > 0 else self.down
        return pltpu.make_async_remote_copy(
            slab, slab, sems.at[0, j, k], sems.at[1, j, k],
            device_id=(p.s + direction * p.ny, p.o), device_id_type=MESH)

    def line_wait(self, j, k, direction):
        p = self.place
        slab = self.held[j].at[pl.ds((p.z - direction * k) * p.ny, p.ny)]
        sems = self.up if direction > 0 else self.down
        pltpu.make_async_remote_copy(
            slab, slab, sems.at[0, j, k - 1], sems.at[1, j, k - 1],
            device_id=(p.s - direction * p.ny, p.o), device_id_type=MESH).wait_recv()

    def has(self, k, direction):
        return self.place.z >= k if direction > 0 else self.place.z < self.place.nz - k

    def more(self, direction):
        return self.place.z < self.place.nz - 1 if direction > 0 else self.place.z > 0

    def send_own(self, j):
        for dy in range(1, self.place.ny):
            self.across_copy(j, dy, -1).wait_recv()
        self.own_copy(j).wait()
        for direction in (1, -1):
            @pl.when(self.more(direction))
            def _():
                self.line_copy(j, 0, direction).start()

    def forward(self, j, k):
        for direction in (1, -1):
            @pl.when(self.has(k, direction))
            def _():
                self.line_wait(j, k, direction)

            if k < self.place.nz - 1:
                @pl.when(self.has(k, direction) & self.more(direction))
                def _():
                    self.line_copy(j, k, direction).start()

    def within_copy(self, j, index, sign):
        p = self.place
        y, o = p.plane_peer(index, sign)
        part = p.part if sign > 0 else o * p.ny + y
        return pltpu.make_async_remote_copy(
            self.stage.at[j, index], self.landed.at[j, pl.ds(part * p.rows, p.rows)],
            self.within.at[0, j, index], self.within.at[1, j, index],
            device_id=(p.z * p.ny + y, o), device_id_type=MESH)

    def hand_out(self, j):
        p = self.place
        order = sorted(range(p.dests), key=lambda index: -((index // p.nops > 0) + (index % p.nops > 0)))
        for index in order:
            y, o = p.plane_peer(index)
            picked = self.held[j][self.maps.want(y, o)]
            if index == 0:
                self.landed[j, pl.ds(p.part * p.rows, p.rows)] = picked
            else:
                self.stage[j, index] = picked
        for index in order:
            if index:
                self.within_copy(j, index, 1).start()

    def receive(self, j):
        for index in range(1, self.place.dests):
            self.within_copy(j, index, -1).wait_recv()

    def drain(self):
        for j in range(self.place.chunks):
            for dy in range(1, self.place.ny):
                self.across_copy(j, dy, 1).wait_send()
            for direction in (1, -1):
                for k in range(self.place.nz - 1):
                    @pl.when(self.has(k, direction) & self.more(direction))
                    def _():
                        self.line_copy(j, k, direction).wait_send()
            for index in range(1, self.place.dests):
                self.within_copy(j, index, 1).wait_send()


def tdot(a, b):
    return lax.dot_general(a, b, (((1,), (1,)), ((), ())), preferred_element_type=F32)


class Polar:
    def __init__(self, n, block, cols, rows, gram):
        self.n, self.block, self.cols, self.rows, self.gram = n, block, cols, rows, gram

    @staticmethod
    def scratch(n):
        return [pltpu.VMEM((n, 2 * n), BF16), pltpu.VMEM((2 * n, n), BF16), pltpu.VMEM((2 * n, n), BF16)]

    def normalise(self, sigma):
        n = self.n
        squares = jnp.sum(jnp.sum(sigma * sigma, axis=0, keepdims=True), axis=1, keepdims=True)
        self.block[...] = sigma * (lax.rsqrt(n * (squares / float(n * n)) + 1e-06) / 2.2)

    def form_gram(self):
        n = self.n
        high, low = halves(self.block[...])
        self.cols[:, pl.ds(0, n)] = high
        self.cols[:, pl.ds(n, n)] = low
        self.rows[pl.ds(0, n)] = high
        self.rows[pl.ds(n, n)] = low
        both = tdot(high, self.rows[...])
        cross = both[:, n:]
        self.gram[pl.ds(0, n)], self.gram[pl.ds(n, n)] = halves(both[:, :n] + (cross + cross.T))

    def apply(self, scale=None):
        n = self.n
        both = bdot(self.gram[pl.ds(0, n)], self.cols[...])
        moved = both[:, :n] + (both[:, n:] + bdot(self.gram[pl.ds(n, n)], self.cols[:, pl.ds(0, n)]))
        value = 1.5 * self.block[...] - 0.5 * moved
        self.block[...] = value if scale is None else value * scale


def site_kernel(place, ops_here, psi, left, right, table, counts, own_columns, half_out, source_out, map_row, rows,
                scalars, map_sems, *rest):
    c, n = place.chunks, place.states
    groups = []
    for _ in range(2):
        groups.append((rest[:c], rest[c:c + 6], rest[c + 6]))
        rest = rest[c + 7:]
    (lefts, rights, block, envs, env_sems, lp_high, lp_low, sigma, first, second, pair, sum_sems,
     quarter, gather_sems, polar_block, cols, doubled, gram, stacked, turned, out_sems) = rest
    place.locate()
    p = place

    def load(ref, w):
        slot = w % 2 if isinstance(w, int) else lax.rem(w, 2)
        return pltpu.make_async_copy(ref.at[w], envs.at[slot], env_sems.at[slot])

    load(left, 0).start()
    load(left, 1).start()
    maps = Maps(place, table, map_row, rows, scalars, map_sems)
    maps.write()
    place.greet()

    def fetch_of(piece, group):
        held, (stage, up, down, across, within, local), landed = group
        return Fetch(place, maps, piece, held, stage, landed, up, down, across, within, local)

    fetch = fetch_of(lambda j, y: psi.at[pl.ds((p.o * p.ny + y) * p.rows, p.rows), pl.ds(j * LANES, LANES)], groups[0])
    again = fetch_of(lambda j, y: quarter.at[pl.ds(y * p.rows, p.rows), pl.ds(j * LANES, LANES)], groups[1])
    maps.start()
    for j in range(c):
        fetch.begin(j)
    for j in range(min(AHEAD, c)):
        fetch.send_own(j)
    count = counts[0, 0]
    sigma[...] = jnp.zeros((n, n), F32)
    block[pl.ds(n, n), pl.ds(LANES, LANES)] = jnp.zeros((n, LANES), BF16)

    def at(index, events):
        for turn, event in events:
            pl.when(index == turn)(event)

    def line(which, *steps):
        def event():
            for j, k in steps:
                if j < c:
                    which.send_own(j) if k == 0 else which.forward(j, k)
        return event

    def turn_in(which, j):
        def event():
            if j < c:
                which.forward(j, p.nz - 1)
                which.hand_out(j)
        return event

    def middle(j):
        return [(j, k) for k in range(2, p.nz - 1)]

    def convert_left(w, carry):
        load(left, w).wait()
        high, low = halves(envs[lax.rem(w, 2)])
        rows_of = pl.ds(pl.multiple_of(w * n, n), n)
        lefts[rows_of, pl.ds(0, n)] = high
        lefts[rows_of, pl.ds(n, n)] = low
        beside = pl.ds(pl.multiple_of(lax.rem(w, PAIR) * n, LANES), n)
        for third, value in enumerate((high, low, high)):
            stacked[w // PAIR, pl.ds(third * n, n), beside] = value

        @pl.when(w < ops_here - 2)
        def _():
            load(left, w + 2).start()

        @pl.when(w >= ops_here - 2)
        def _():
            load(right, w + 2 - ops_here).start()

        at(w, [(1, line(fetch, (0, 1))), (2, line(fetch, (AHEAD, 0), (1, 1))), (2, maps.finish)])
        return carry

    def convert_right(w, carry):
        load(right, w).wait()
        high, low = halves(envs[lax.rem(w, 2)] * (w < count).astype(F32))
        for j in range(c):
            rows_of = pl.ds(pl.multiple_of((j * ops_here + w) * LANES, LANES), LANES)
            rights[rows_of, pl.ds(0, n)] = high[j * LANES:(j + 1) * LANES]
            rights[rows_of, pl.ds(n, n)] = low[j * LANES:(j + 1) * LANES]

        @pl.when(w < ops_here - 2)
        def _():
            load(right, w + 2).start()

        at(w, [(0, line(fetch, *middle(0))), (1, line(fetch, (AHEAD + 1, 0), (2, 1))), (3, line(fetch, *middle(1)))])
        return carry

    lax.fori_loop(0, ops_here, convert_left, 0)
    lax.fori_loop(0, ops_here, convert_right, 0)
    for j in range(AHEAD + 2, c):
        fetch.send_own(j)
    turn_in(fetch, 0)()

    def products(j, carry):
        for turn in range(c):
            @pl.when(j == turn)
            def _():
                line(fetch, (turn + 3, 1), *middle(turn + 2))()
                if turn < c - 2:
                    turn_in(fetch, turn + 1)()
                fetch.receive(turn)

        high, low = halves(fetch.landed[j])
        block[pl.ds(0, n), pl.ds(0, LANES)] = high
        block[pl.ds(n, n), pl.ds(0, LANES)] = high
        block[pl.ds(0, n), pl.ds(LANES, LANES)] = low
        for w in range(ops_here):
            both = bdot(lefts[pl.ds(w * n, n)], block[...])
            high, low = halves(both[:, :LANES] + both[:, LANES:])
            lp_high[:, pl.ds(w * LANES, LANES)] = high
            lp_low[:, pl.ds(w * LANES, LANES)] = low

        @pl.when(j == max(c - 3, 0))
        def _():
            if c > 1:
                turn_in(fetch, c - 1)()

        deep = pl.ds(pl.multiple_of(j * ops_here * LANES, LANES), ops_here * LANES)
        both = bdot(lp_high[...], rights[deep])
        sigma[...] += both[:, :n] + (both[:, n:] + bdot(lp_low[...], rights[deep, pl.ds(0, n)]))
        return carry

    lax.fori_loop(0, c, products, 0)

    side, core = p.o // CORES, lax.rem(p.o, CORES)
    mate = side * CORES + 1 - core
    facing = (1 - side) * CORES + core
    across_mate = (1 - side) * CORES + 1 - core
    q = p.quarter

    whole = polar_block
    polar = Polar(n, whole, cols, doubled, gram)

    def swap_cores(i, far, j):
        rows_of, at_cols = pl.ds((far * CORES + 1 - core) * q, q), pl.ds(j * LANES, LANES)
        return pltpu.make_async_remote_copy(
            sigma.at[rows_of, at_cols], first.at[i, :, at_cols], sum_sems.at[0, i, j], sum_sems.at[1, i, j],
            device_id=(p.s, mate), device_id_type=MESH)

    def over(j):
        at_cols = pl.ds(j * LANES, LANES)
        return pltpu.make_async_remote_copy(
            pair.at[:, at_cols], second.at[:, at_cols], sum_sems.at[0, 2, j], sum_sems.at[1, 2, j],
            device_id=(p.s, facing), device_id_type=MESH)

    def gather(i, sender, target, j):
        rows_of, at_cols = pl.ds(sender * q, q), pl.ds(j * LANES, LANES)
        source = quarter.at[:, at_cols] if i < 2 else whole.at[rows_of, at_cols]
        return pltpu.make_async_remote_copy(
            source, whole.at[rows_of, at_cols], gather_sems.at[0, i, j], gather_sems.at[1, i, j],
            device_id=(p.s, target), device_id_type=MESH)

    for j in range(c):
        swap_cores(0, 1 - side, j).start()
        swap_cores(1, side, j).start()
    for j in range(c + 1):
        if j < c:
            at_cols = pl.ds(j * LANES, LANES)
            swap_cores(0, 1 - side, j).wait_recv()
            pair[:, at_cols] = sigma[pl.ds(((1 - side) * CORES + core) * q, q), at_cols] + first[0, :, at_cols]
        if j:
            over(j - 1).start()
    for j in range(c + 1):
        if j < c:
            at_cols = pl.ds(j * LANES, LANES)
            swap_cores(1, side, j).wait_recv()
            over(j).wait_recv()
            quarter[:, at_cols] = sigma[pl.ds(p.o * q, q), at_cols] + first[1, :, at_cols] + second[:, at_cols]
            whole[pl.ds(p.o * q, q), at_cols] = quarter[:, at_cols]
        if j:
            again.begin(j - 1)
            gather(1, p.o, facing, j - 1).start()
            gather(0, p.o, mate, j - 1).start()
        if j > 1:
            again.send_own(j - 2)
    again.send_own(c - 1)
    for j in range(c):
        gather(1, facing, facing, j).wait_recv()
        gather(2, facing, mate, j).start()
        again.forward(j, 1)
    line(again, *middle(0))()
    for j in range(c):
        gather(0, mate, mate, j).wait_recv()
        gather(2, across_mate, mate, j).wait_recv()
        gather(2, facing, mate, j).wait_send()
    polar.normalise(whole[...])

    def group(turn):
        def event():
            line(again, *(middle(1) if turn == 0 else []), *middle(turn + 2))()
            if turn:
                turn_in(again, turn - 1)()
        return event

    def own_step(step, carry):
        polar.form_gram()
        polar.apply()
        at(step, [(turn, group(turn)) for turn in range(min(c, POLAR))])
        return carry

    lax.fori_loop(0, POLAR, own_step, 0)
    for turn in range(POLAR, c):
        group(turn)()
    tensor = (whole[...] * math.sqrt(n)).T
    whole[...] = tensor
    own_columns[...] = whole[pl.ds(pl.multiple_of(p.o * q, q), q)]
    high, low = halves(tensor)
    turned[:, pl.ds(0, n)] = high
    turned[:, pl.ds(n, n)] = high
    turned[:, pl.ds(2 * n, n)] = low

    def half_rotate(pair, carry):
        both = bdot(turned[...], stacked[pair])
        for i in range(PAIR):
            w = pair * PAIR + i
            rows_of = pl.ds(pl.multiple_of(w * n, n), n)
            rights[rows_of, pl.ds(0, n)], rights[rows_of, pl.ds(n, n)] = halves(both[:, i * n:(i + 1) * n])
            pltpu.make_async_copy(rights.at[rows_of], half_out.at[rows_of], out_sems.at[w]).start()
        at(pair, [(0, turn_in(again, c - 1))])
        return carry

    lax.fori_loop(0, ops_here // PAIR, half_rotate, 0)
    for j in range(c):
        again.receive(j)
    save = pltpu.make_async_copy(again.landed, source_out, out_sems.at[ops_here])
    save.start()
    for w in range(ops_here):
        rows_of = pl.ds(w * n, n)
        pltpu.make_async_copy(rights.at[rows_of], half_out.at[rows_of], out_sems.at[w]).wait()
    fetch.drain()
    again.drain()
    for j in range(c):
        swap_cores(0, 1 - side, j).wait_send()
        swap_cores(1, side, j).wait_send()
        over(j).wait_send()
        gather(1, p.o, facing, j).wait_send()
        gather(0, p.o, mate, j).wait_send()
    save.wait()


def last_kernel(n, ops_here, chunks, source, half, columns, own_columns, rotated, block, cols, doubled, gram, halves_in, double,
                tail, products, in_sems, out_sems):
    def load(w):
        at = pl.ds(w * n, n)
        return pltpu.make_async_copy(half.at[at], halves_in.at[at], in_sems.at[w])

    def store(w):
        return pltpu.make_async_copy(products.at[w], rotated.at[w], out_sems.at[w])

    for w in range(ops_here):
        load(w).start()
    own_columns[...] = columns[...]
    polar = Polar(n, block, cols, doubled, gram)
    polar.normalise(jnp.concatenate([source[j] for j in range(chunks)], axis=1))

    def step(_, carry):
        polar.form_gram()
        polar.apply()
        return carry

    lax.fori_loop(0, POLAR, step, 0)
    wide = n - n % WIDE
    rest = n - wide
    high, low = halves(block[...] * math.sqrt(n))
    double[pl.ds(0, n)] = high[:, :wide]
    double[pl.ds(n, n)] = high[:, :wide]
    cols[:, pl.ds(0, wide)] = low[:, :wide]
    if rest:
        tail[pl.ds(0, n), pl.ds(0, rest)] = high[:, wide:]
        tail[pl.ds(0, n), pl.ds(rest, rest)] = low[:, wide:]
        tail[pl.ds(n, n), pl.ds(0, rest)] = high[:, wide:]
        tail[pl.ds(n, n), pl.ds(rest, rest)] = jnp.zeros((n, rest), BF16)

    def rotate(w, carry):
        load(w).wait()
        rows_of = pl.ds(pl.multiple_of(w * n, n), n)
        both = halves_in[rows_of]
        products[w, :, pl.ds(0, wide)] = bdot(both, double[...]) + bdot(both[:, :n], cols[:, pl.ds(0, wide)])
        if rest:
            ends = bdot(both, tail[...])
            products[w, :, pl.ds(wide, rest)] = ends[:, :rest] + ends[:, rest:]
        store(w).start()
        return carry

    lax.fori_loop(0, ops_here, rotate, 0)
    for w in range(ops_here):
        store(w).wait()


def vmem():
    return pl.BlockSpec(memory_space=pltpu.VMEM)


def scalar():
    return pl.BlockSpec(memory_space=pltpu.SMEM)


def anywhere():
    return pl.BlockSpec(memory_space=pl.ANY)


def shards_planes(place, wavefunction, left_env, right_env, shift_map, op_counts):
    c, n, q, ops_here = place.chunks, place.states, place.quarter, left_env.shape[1]
    fetches = []
    for _ in range(2):
        held, stage, *sems = Fetch.scratch(place)
        fetches += [*held, stage, *sems, pltpu.VMEM((c, n, LANES), F32)]
    columns, half, source = pl.pallas_call(
        functools.partial(site_kernel, place, ops_here),
        out_shape=(
            jax.ShapeDtypeStruct((q, n), F32),
            jax.ShapeDtypeStruct((ops_here * n, 2 * n), BF16),
            jax.ShapeDtypeStruct((c, n, LANES), F32),
        ),
        in_specs=[anywhere(), anywhere(), anywhere(), scalar(), scalar()],
        out_specs=(vmem(), anywhere(), anywhere()),
        scratch_shapes=[
            *Maps.scratch(place), *fetches,
            pltpu.VMEM((ops_here * n, 2 * n), BF16),
            pltpu.VMEM((ops_here * n, 2 * n), BF16),
            pltpu.VMEM((2 * n, 2 * LANES), BF16),
            pltpu.VMEM((2, n, n), F32),
            pltpu.SemaphoreType.DMA((2,)),
            pltpu.VMEM((n, ops_here * LANES), BF16),
            pltpu.VMEM((n, ops_here * LANES), BF16),
            pltpu.VMEM((n, n), F32),
            pltpu.VMEM((2, q, n), F32),
            pltpu.VMEM((q, n), F32),
            pltpu.VMEM((q, n), F32),
            pltpu.SemaphoreType.DMA((2, 3, c)),
            pltpu.VMEM((q, n), F32),
            pltpu.SemaphoreType.DMA((2, 3, c)),
            pltpu.VMEM((n, n), F32),
            *Polar.scratch(n),
            pltpu.VMEM((ops_here // PAIR, 3 * n, PAIR * n), BF16),
            pltpu.VMEM((n, 3 * n), BF16),
            pltpu.SemaphoreType.DMA((ops_here + 1,)),
        ],
        compiler_params=pltpu.CompilerParams(collective_id=0, has_side_effects=True, vmem_limit_bytes=60 * 2**20),
    )(wavefunction[0], left_env[0], right_env[0], shift_map, op_counts)
    own_columns, rotated = pl.pallas_call(
        functools.partial(last_kernel, n, ops_here, c),
        out_shape=(jax.ShapeDtypeStruct((q, n), F32), jax.ShapeDtypeStruct((ops_here, n, n), F32)),
        in_specs=[vmem(), anywhere(), vmem()],
        out_specs=(vmem(), anywhere()),
        scratch_shapes=[
            pltpu.VMEM((n, n), F32),
            *Polar.scratch(n),
            pltpu.VMEM((ops_here * n, 2 * n), BF16),
            pltpu.VMEM((2 * n, n - n % WIDE), BF16),
            pltpu.VMEM((2 * n, 2 * max(n % WIDE, LANES)), BF16),
            pltpu.VMEM((ops_here, n, n), F32),
            pltpu.SemaphoreType.DMA((ops_here,)),
            pltpu.SemaphoreType.DMA((ops_here,)),
        ],
        compiler_params=pltpu.CompilerParams(vmem_limit_bytes=60 * 2**20),
    )(source, half, columns)
    return own_columns.T[None], rotated[None]


def line_split(sector_count):
    rows = 1
    while rows * 2 * rows * 2 <= sector_count and sector_count % (rows * 2) == 0:
        rows *= 2
    return rows


def solution(mesh):
    def shards(wavefunction, left_env, right_env, shift_map, op_counts):
        nsec, nops = mesh.shape["sector"], mesh.shape["ops"]
        states = wavefunction.shape[1]
        ny = line_split(nsec)
        per_group = left_env.shape[1] % PAIR == 0
        fits = per_group and nops == 2 * CORES and ny == 2 and states % LANES == 0 and states % (nops * ny * SUBLANES) == 0
        if not fits:
            return shards_general(wavefunction, left_env, right_env, shift_map, op_counts)
        place = Place(nsec, nops, ny, states)
        return shards_planes(place, wavefunction, left_env, right_env, shift_map, op_counts)

    return jax.shard_map(
        shards,
        mesh=mesh,
        in_specs=(
            P("sector", None, None),
            P("sector", "ops", None, None),
            P("sector", "ops", None, None),
            P("ops", None),
            P("ops", "sector"),
        ),
        out_specs=(P("sector", None, "ops"), P("sector", "ops", None, None)),
        check_vma=False,
    )
```

```python
import functools
import math

import jax
import jax.numpy as jnp
from jax import lax
from jax.experimental import pallas as pl
from jax.experimental.pallas import tpu as pltpu
from jax.sharding import PartitionSpec as P

POLAR = 5
LANES, SUBLANES = 128, 8
CORES = 2
AHEAD = 2
WIDE = 256
PAIR = 2
MESH = pl.DeviceIdType.MESH
F32, BF16 = jnp.float32, jnp.bfloat16

precise = lax.Precision.HIGH


def dot(a, b):
    return jnp.dot(a, b, precision=precise, preferred_element_type=jnp.float32)


def to_tiles(block, padded):
    rows, cols = block.shape
    tiles = block.reshape(rows // SUBLANES, SUBLANES, cols // LANES, LANES)
    tiles = tiles.transpose(0, 2, 1, 3).reshape(rows * cols // (SUBLANES * LANES), SUBLANES, LANES)
    return jnp.pad(tiles, ((0, padded - tiles.shape[0]), (0, 0), (0, 0)))


def from_tiles(tiles, rows, cols):
    tiles = tiles[: rows * cols // (SUBLANES * LANES)]
    tiles = tiles.reshape(rows // SUBLANES, cols // LANES, SUBLANES, LANES)
    return tiles.transpose(0, 2, 1, 3).reshape(rows, cols)


def swap(value, axis, bit):
    size = lax.axis_size(axis)
    return lax.ppermute(value, axis, [(i, i ^ bit) for i in range(size)])


def sum_scatter(tiles, axis):
    size, here = lax.axis_size(axis), lax.axis_index(axis)
    rest = tiles.reshape((size, tiles.shape[0] // size) + tiles.shape[1:])
    bit = 1
    while bit < size:
        mine = (here // bit) % 2
        pairs = rest.reshape((rest.shape[0] // 2, 2) + rest.shape[1:])
        keep = lax.dynamic_index_in_dim(pairs, mine, 1, keepdims=False)
        give = lax.dynamic_index_in_dim(pairs, 1 - mine, 1, keepdims=False)
        rest = keep + swap(give, axis, bit)
        bit *= 2
    return rest[0]


def gather_whole(quarter, axis):
    size, here = lax.axis_size(axis), lax.axis_index(axis)
    held = quarter[None]
    bit = size // 2
    while bit:
        mine = (here // bit) % 2
        other = swap(held, axis, bit)
        first = jnp.where(mine == 0, held, other)
        second = jnp.where(mine == 0, other, held)
        held = jnp.stack([first, second], axis=1).reshape((-1,) + quarter.shape)
        bit //= 2
    return held.reshape((-1,) + quarter.shape[1:])


def polar(sigma_block):
    states = sigma_block.shape[0]
    mean_sq = jnp.sum(sigma_block * sigma_block) / float(states * states)
    iterate = sigma_block * (lax.rsqrt(states * mean_sq + 1e-06) / 2.2)

    def step(_, iterate):
        gram_matrix = jnp.einsum("ab,cb->ac", iterate, iterate, precision=precise)
        return 1.5 * iterate - 0.5 * dot(gram_matrix, iterate)

    return lax.fori_loop(0, POLAR, step, iterate) * math.sqrt(states)


def shards_general(wavefunction, left_env, right_env, shift_map, op_counts):
    sector_count = lax.axis_size("sector")
    group_size = lax.axis_size("ops")
    group_here = lax.axis_index("ops")
    states = wavefunction.shape[1]
    ops_here = left_env.shape[1]
    parts = sector_count * group_size
    piece = -(-states * states // (SUBLANES * LANES * parts))
    padded = piece * parts
    quarter = piece * sector_count

    whole_map = lax.all_gather(shift_map[0], "ops").reshape(parts)

    def fetch_from_quarter(own_quarter):
        pieces = own_quarter.reshape(sector_count, piece, SUBLANES, LANES)
        spread = lax.all_to_all(pieces, "sector", split_axis=0, concat_axis=0, tiled=True)
        picked = jnp.take(spread, whole_map, axis=0)
        landed = lax.all_to_all(picked, ("ops", "sector"), split_axis=0, concat_axis=0, tiled=True)
        return from_tiles(landed.reshape(padded, SUBLANES, LANES), states, states)

    psi_tiles = to_tiles(wavefunction[0], padded)
    psi_quarter = lax.dynamic_slice_in_dim(psi_tiles, group_here * quarter, quarter, 0)
    moved_block = fetch_from_quarter(psi_quarter)

    left, right = left_env[0], right_env[0]
    count = op_counts[0, 0]
    active = (jnp.arange(ops_here) < count).astype(jnp.float32)
    left_psi = jnp.einsum("wab,bc->wac", left, moved_block, precision=precise) * active[:, None, None]
    partial_sigma = jnp.einsum("wac,wcd->ad", left_psi, right, precision=precise)

    sigma_quarter = sum_scatter(to_tiles(partial_sigma, padded), "ops")
    source_sigma = fetch_from_quarter(sigma_quarter)
    sigma_block = from_tiles(gather_whole(sigma_quarter, "ops"), states, states)

    whole_tensor = polar(sigma_block)
    column_width = states // group_size
    own_columns = lax.dynamic_slice_in_dim(whole_tensor, group_here * column_width, column_width, 1)
    half_rotated = jnp.einsum("ba,wbc->wac", whole_tensor, left, precision=precise)
    source_tensor = polar(source_sigma)
    rotated = jnp.einsum("wac,cd->wad", half_rotated, source_tensor, precision=precise)
    return (own_columns[None], rotated[None])


def halves(value):
    high = value.astype(BF16)
    return high, (value - high.astype(F32)).astype(BF16)


def bdot(a, b):
    return jnp.dot(a, b, preferred_element_type=F32)


class Place:
    def __init__(self, nsec, nops, ny, states):
        self.nsec, self.nops, self.ny, self.nz = nsec, nops, ny, nsec // ny
        self.states = states
        self.chunks = states // LANES
        self.parts = nops * ny
        self.rows = states // self.parts
        self.quarter = states // nops
        self.dests = nops * ny

    def locate(self):
        self.s, self.o = lax.axis_index("sector"), lax.axis_index("ops")
        self.z, self.y = self.s // self.ny, lax.rem(self.s, self.ny)
        self.part = self.o * self.ny + self.y

    def plane_peer(self, index, sign=1):
        dy, do = index // self.nops, index % self.nops
        if sign < 0:
            dy, do = (self.ny - dy) % self.ny, (self.nops - do) % self.nops
        return lax.rem(self.y + dy, self.ny), lax.rem(self.o + do, self.nops)

    def greet(self):
        barrier = pltpu.get_barrier_semaphore()
        for index in range(1, self.dests):
            y, o = self.plane_peer(index)
            pl.semaphore_signal(barrier, inc=1, device_id=(self.z * self.ny + y, o), device_id_type=MESH)

        @pl.when(self.z > 0)
        def _():
            pl.semaphore_signal(barrier, inc=1, device_id=(self.s - self.ny, self.o), device_id_type=MESH)

        @pl.when(self.z < self.nz - 1)
        def _():
            pl.semaphore_signal(barrier, inc=1, device_id=(self.s + self.ny, self.o), device_id_type=MESH)

        line = (self.z > 0).astype(jnp.int32) + (self.z < self.nz - 1).astype(jnp.int32)
        pl.semaphore_wait(barrier, self.dests - 1 + line)


class Maps:
    def __init__(self, place, table, own_ref, rows_ref, scalars_ref, sems):
        self.place, self.table = place, table
        self.own, self.rows, self.scalars, self.sems = own_ref, rows_ref, scalars_ref, sems

    @staticmethod
    def scratch(place):
        return [
            pltpu.VMEM((1, LANES), jnp.int32),
            pltpu.VMEM((place.nops, 1, LANES), jnp.int32),
            pltpu.SMEM((place.nops, 1, LANES), jnp.int32),
            pltpu.SemaphoreType.DMA((3, place.nops)),
        ]

    def write(self):
        lane = lax.broadcasted_iota(jnp.int32, (1, LANES), 1)
        row = jnp.zeros((1, LANES), jnp.int32)
        for sector in range(self.place.nsec):
            row = jnp.where(lane == sector, self.table[0, sector], row)
        self.own[...] = row

    def copy(self, offset, sign):
        p = self.place
        peer = lax.rem(p.o + offset, p.nops)
        slot = p.o if sign > 0 else lax.rem(p.o + p.nops - offset, p.nops)
        return pltpu.make_async_remote_copy(
            self.own, self.rows.at[slot], self.sems.at[0, offset], self.sems.at[1, offset],
            device_id=(p.s, peer), device_id_type=MESH)

    def start(self):
        for offset in range(1, self.place.nops):
            self.copy(offset, 1).start()
        pltpu.make_async_copy(self.own, self.rows.at[self.place.o], self.sems.at[2, 0]).start()

    def finish(self):
        for offset in range(1, self.place.nops):
            self.copy(offset, 1).wait_send()
            self.copy(offset, -1).wait_recv()
        pltpu.make_async_copy(self.own, self.rows.at[self.place.o], self.sems.at[2, 0]).wait()
        landed = pltpu.make_async_copy(self.rows, self.scalars, self.sems.at[2, 1])
        landed.start()
        landed.wait()

    def want(self, y, o):
        return self.scalars[o, 0, self.place.z * self.place.ny + y]


class Fetch:
    def __init__(self, place, maps, piece, held, stage, landed, up, down, across, within, local):
        self.place, self.maps, self.piece = place, maps, piece
        self.held, self.stage, self.landed = held, stage, landed
        self.up, self.down, self.across, self.within, self.local = up, down, across, within, local

    @staticmethod
    def scratch(place):
        c, dma = place.chunks, pltpu.SemaphoreType.DMA
        return (
            [pltpu.VMEM((place.nsec, place.rows, LANES), F32) for _ in range(c)],
            pltpu.VMEM((c, place.dests, place.rows, LANES), F32),
            dma((2, c, place.nz - 1)),
            dma((2, c, place.nz - 1)),
            dma((2, c, place.ny)),
            dma((2, c, place.dests)),
            dma((c,)),
        )

    def across_copy(self, j, dy, sign):
        p = self.place
        y = lax.rem(p.y + dy, p.ny)
        slot = p.s if sign > 0 else p.z * p.ny + lax.rem(p.y + p.ny - dy, p.ny)
        return pltpu.make_async_remote_copy(
            self.piece(j, y), self.held[j].at[slot], self.across.at[0, j, dy], self.across.at[1, j, dy],
            device_id=(p.z * p.ny + y, p.o), device_id_type=MESH)

    def own_copy(self, j):
        p = self.place
        return pltpu.make_async_copy(self.piece(j, p.y), self.held[j].at[p.s], self.local.at[j])

    def begin(self, j):
        for dy in range(1, self.place.ny):
            self.across_copy(j, dy, 1).start()
        self.own_copy(j).start()

    def line_copy(self, j, k, direction):
        p = self.place
        slab = self.held[j].at[pl.ds((p.z - direction * k) * p.ny, p.ny)]
        sems = self.up if direction > 0 else self.down
        return pltpu.make_async_remote_copy(
            slab, slab, sems.at[0, j, k], sems.at[1, j, k],
            device_id=(p.s + direction * p.ny, p.o), device_id_type=MESH)

    def line_wait(self, j, k, direction):
        p = self.place
        slab = self.held[j].at[pl.ds((p.z - direction * k) * p.ny, p.ny)]
        sems = self.up if direction > 0 else self.down
        pltpu.make_async_remote_copy(
            slab, slab, sems.at[0, j, k - 1], sems.at[1, j, k - 1],
            device_id=(p.s - direction * p.ny, p.o), device_id_type=MESH).wait_recv()

    def has(self, k, direction):
        return self.place.z >= k if direction > 0 else self.place.z < self.place.nz - k

    def more(self, direction):
        return self.place.z < self.place.nz - 1 if direction > 0 else self.place.z > 0

    def send_own(self, j):
        for dy in range(1, self.place.ny):
            self.across_copy(j, dy, -1).wait_recv()
        self.own_copy(j).wait()
        for direction in (1, -1):
            @pl.when(self.more(direction))
            def _():
                self.line_copy(j, 0, direction).start()

    def forward(self, j, k):
        for direction in (1, -1):
            @pl.when(self.has(k, direction))
            def _():
                self.line_wait(j, k, direction)

            if k < self.place.nz - 1:
                @pl.when(self.has(k, direction) & self.more(direction))
                def _():
                    self.line_copy(j, k, direction).start()

    def within_copy(self, j, index, sign):
        p = self.place
        y, o = p.plane_peer(index, sign)
        part = p.part if sign > 0 else o * p.ny + y
        return pltpu.make_async_remote_copy(
            self.stage.at[j, index], self.landed.at[j, pl.ds(part * p.rows, p.rows)],
            self.within.at[0, j, index], self.within.at[1, j, index],
            device_id=(p.z * p.ny + y, o), device_id_type=MESH)

    def hand_out(self, j):
        p = self.place
        order = sorted(range(p.dests), key=lambda index: -((index // p.nops > 0) + (index % p.nops > 0)))
        for index in order:
            y, o = p.plane_peer(index)
            picked = self.held[j][self.maps.want(y, o)]
            if index == 0:
                self.landed[j, pl.ds(p.part * p.rows, p.rows)] = picked
            else:
                self.stage[j, index] = picked
        for index in order:
            if index:
                self.within_copy(j, index, 1).start()

    def receive(self, j):
        for index in range(1, self.place.dests):
            self.within_copy(j, index, -1).wait_recv()

    def drain(self):
        for j in range(self.place.chunks):
            for dy in range(1, self.place.ny):
                self.across_copy(j, dy, 1).wait_send()
            for direction in (1, -1):
                for k in range(self.place.nz - 1):
                    @pl.when(self.has(k, direction) & self.more(direction))
                    def _():
                        self.line_copy(j, k, direction).wait_send()
            for index in range(1, self.place.dests):
                self.within_copy(j, index, 1).wait_send()


def tdot(a, b):
    return lax.dot_general(a, b, (((1,), (1,)), ((), ())), preferred_element_type=F32)


class Polar:
    def __init__(self, n, block, cols, rows, gram):
        self.n, self.block, self.cols, self.rows, self.gram = n, block, cols, rows, gram

    @staticmethod
    def scratch(n):
        return [pltpu.VMEM((n, 2 * n), BF16), pltpu.VMEM((2 * n, n), BF16), pltpu.VMEM((2 * n, n), BF16)]

    def normalise(self, sigma):
        n = self.n
        squares = jnp.sum(jnp.sum(sigma * sigma, axis=0, keepdims=True), axis=1, keepdims=True)
        self.block[...] = sigma * (lax.rsqrt(n * (squares / float(n * n)) + 1e-06) / 2.2)

    def form_gram(self):
        n = self.n
        high, low = halves(self.block[...])
        self.cols[:, pl.ds(0, n)] = high
        self.cols[:, pl.ds(n, n)] = low
        self.rows[pl.ds(0, n)] = high
        self.rows[pl.ds(n, n)] = low
        both = tdot(high, self.rows[...])
        cross = both[:, n:]
        self.gram[pl.ds(0, n)], self.gram[pl.ds(n, n)] = halves(both[:, :n] + (cross + cross.T))

    def apply(self, scale=None):
        n = self.n
        both = bdot(self.gram[pl.ds(0, n)], self.cols[...])
        moved = both[:, :n] + (both[:, n:] + bdot(self.gram[pl.ds(n, n)], self.cols[:, pl.ds(0, n)]))
        value = 1.5 * self.block[...] - 0.5 * moved
        self.block[...] = value if scale is None else value * scale


def site_kernel(place, ops_here, psi, left, right, table, counts, own_columns, half_out, source_out, map_row, rows,
                scalars, map_sems, *rest):
    c, n = place.chunks, place.states
    groups = []
    for _ in range(2):
        groups.append((rest[:c], rest[c:c + 6], rest[c + 6]))
        rest = rest[c + 7:]
    (lefts, rights, block, envs, env_sems, lp_high, lp_low, sigma, first, second, pair, sum_sems,
     quarter, gather_sems, polar_block, cols, doubled, gram, stacked, turned, out_sems) = rest
    place.locate()
    p = place

    def load(ref, w):
        slot = w % 2 if isinstance(w, int) else lax.rem(w, 2)
        return pltpu.make_async_copy(ref.at[w], envs.at[slot], env_sems.at[slot])

    load(left, 0).start()
    load(left, 1).start()
    maps = Maps(place, table, map_row, rows, scalars, map_sems)
    maps.write()
    place.greet()

    def fetch_of(piece, group):
        held, (stage, up, down, across, within, local), landed = group
        return Fetch(place, maps, piece, held, stage, landed, up, down, across, within, local)

    fetch = fetch_of(lambda j, y: psi.at[pl.ds((p.o * p.ny + y) * p.rows, p.rows), pl.ds(j * LANES, LANES)], groups[0])
    again = fetch_of(lambda j, y: quarter.at[pl.ds(y * p.rows, p.rows), pl.ds(j * LANES, LANES)], groups[1])
    maps.start()
    for j in range(c):
        fetch.begin(j)
    for j in range(min(AHEAD, c)):
        fetch.send_own(j)
    count = counts[0, 0]
    sigma[...] = jnp.zeros((n, n), F32)
    block[pl.ds(n, n), pl.ds(LANES, LANES)] = jnp.zeros((n, LANES), BF16)

    def at(index, events):
        for turn, event in events:
            pl.when(index == turn)(event)

    def line(which, *steps):
        def event():
            for j, k in steps:
                if j < c:
                    which.send_own(j) if k == 0 else which.forward(j, k)
        return event

    def turn_in(which, j):
        def event():
            if j < c:
                which.forward(j, p.nz - 1)
                which.hand_out(j)
        return event

    def middle(j):
        return [(j, k) for k in range(2, p.nz - 1)]

    def convert_left(w, carry):
        load(left, w).wait()
        high, low = halves(envs[lax.rem(w, 2)])
        rows_of = pl.ds(pl.multiple_of(w * n, n), n)
        lefts[rows_of, pl.ds(0, n)] = high
        lefts[rows_of, pl.ds(n, n)] = low
        beside = pl.ds(pl.multiple_of(lax.rem(w, PAIR) * n, LANES), n)
        for third, value in enumerate((high, low, high)):
            stacked[w // PAIR, pl.ds(third * n, n), beside] = value

        @pl.when(w < ops_here - 2)
        def _():
            load(left, w + 2).start()

        @pl.when(w >= ops_here - 2)
        def _():
            load(right, w + 2 - ops_here).start()

        at(w, [(1, line(fetch, (0, 1))), (2, line(fetch, (AHEAD, 0), (1, 1))), (2, maps.finish)])
        return carry

    def convert_right(w, carry):
        load(right, w).wait()
        high, low = halves(envs[lax.rem(w, 2)] * (w < count).astype(F32))
        for j in range(c):
            rows_of = pl.ds(pl.multiple_of((j * ops_here + w) * LANES, LANES), LANES)
            rights[rows_of, pl.ds(0, n)] = high[j * LANES:(j + 1) * LANES]
            rights[rows_of, pl.ds(n, n)] = low[j * LANES:(j + 1) * LANES]

        @pl.when(w < ops_here - 2)
        def _():
            load(right, w + 2).start()

        at(w, [(0, line(fetch, *middle(0))), (1, line(fetch, (AHEAD + 1, 0), (2, 1))), (3, line(fetch, *middle(1)))])
        return carry

    lax.fori_loop(0, ops_here, convert_left, 0)
    lax.fori_loop(0, ops_here, convert_right, 0)
    for j in range(AHEAD + 2, c):
        fetch.send_own(j)
    turn_in(fetch, 0)()

    side, core = p.o // CORES, lax.rem(p.o, CORES)
    mate = side * CORES + 1 - core
    facing = (1 - side) * CORES + core
    across_mate = (1 - side) * CORES + 1 - core
    q = p.quarter

    def swap_cores(i, far, j):
        rows_of, at_cols = pl.ds((far * CORES + 1 - core) * q, q), pl.ds(j * LANES, LANES)
        return pltpu.make_async_remote_copy(
            sigma.at[rows_of, at_cols], first.at[i, :, at_cols], sum_sems.at[0, i, j], sum_sems.at[1, i, j],
            device_id=(p.s, mate), device_id_type=MESH)

    def products(j, carry):
        for turn in range(c):
            @pl.when(j == turn)
            def _():
                line(fetch, (turn + 3, 1), *middle(turn + 2))()
                if turn < c - 2:
                    turn_in(fetch, turn + 1)()
                fetch.receive(turn)

        high, low = halves(fetch.landed[j])
        block[pl.ds(0, n), pl.ds(0, LANES)] = high
        block[pl.ds(n, n), pl.ds(0, LANES)] = high
        block[pl.ds(0, n), pl.ds(LANES, LANES)] = low
        for w in range(ops_here):
            both = bdot(lefts[pl.ds(w * n, n)], block[...])
            high, low = halves(both[:, :LANES] + both[:, LANES:])
            lp_high[:, pl.ds(w * LANES, LANES)] = high
            lp_low[:, pl.ds(w * LANES, LANES)] = low

        @pl.when(j == max(c - 3, 0))
        def _():
            if c > 1:
                turn_in(fetch, c - 1)()

        deep = pl.ds(pl.multiple_of(j * ops_here * LANES, LANES), ops_here * LANES)
        for i, far in ((0, 1 - side), (1, side)):
            half = pl.ds(pl.multiple_of(far * (n // 2), 2 * SUBLANES), n // 2)
            both = bdot(lp_high[half], rights[deep])
            sigma[half] += both[:, :n] + (both[:, n:] + bdot(lp_low[half], rights[deep, pl.ds(0, n)]))

            @pl.when(j == c - 1)
            def _():
                for chunk in range(c):
                    swap_cores(i, far, chunk).start()
        return carry

    lax.fori_loop(0, c, products, 0)

    whole = polar_block
    polar = Polar(n, whole, cols, doubled, gram)

    def over(j):
        at_cols = pl.ds(j * LANES, LANES)
        return pltpu.make_async_remote_copy(
            pair.at[:, at_cols], second.at[:, at_cols], sum_sems.at[0, 2, j], sum_sems.at[1, 2, j],
            device_id=(p.s, facing), device_id_type=MESH)

    def gather(i, sender, target, j):
        rows_of, at_cols = pl.ds(sender * q, q), pl.ds(j * LANES, LANES)
        source = quarter.at[:, at_cols] if i < 2 else whole.at[rows_of, at_cols]
        return pltpu.make_async_remote_copy(
            source, whole.at[rows_of, at_cols], gather_sems.at[0, i, j], gather_sems.at[1, i, j],
            device_id=(p.s, target), device_id_type=MESH)

    for j in range(c + 1):
        if j < c:
            at_cols = pl.ds(j * LANES, LANES)
            swap_cores(0, 1 - side, j).wait_recv()
            pair[:, at_cols] = sigma[pl.ds(((1 - side) * CORES + core) * q, q), at_cols] + first[0, :, at_cols]
        if j:
            over(j - 1).start()
    for j in range(c + 1):
        if j < c:
            at_cols = pl.ds(j * LANES, LANES)
            swap_cores(1, side, j).wait_recv()
            over(j).wait_recv()
            quarter[:, at_cols] = sigma[pl.ds(p.o * q, q), at_cols] + first[1, :, at_cols] + second[:, at_cols]
            whole[pl.ds(p.o * q, q), at_cols] = quarter[:, at_cols]
        if j:
            again.begin(j - 1)
            gather(1, p.o, facing, j - 1).start()
            gather(0, p.o, mate, j - 1).start()
        if j > 1:
            again.send_own(j - 2)
    again.send_own(c - 1)
    for j in range(c):
        gather(1, facing, facing, j).wait_recv()
        gather(2, facing, mate, j).start()
        again.forward(j, 1)
    line(again, *middle(0))()
    for j in range(c):
        gather(0, mate, mate, j).wait_recv()
        gather(2, across_mate, mate, j).wait_recv()
        gather(2, facing, mate, j).wait_send()
    polar.normalise(whole[...])

    def group(turn):
        def event():
            line(again, *(middle(1) if turn == 0 else []), *middle(turn + 2))()
            if turn:
                turn_in(again, turn - 1)()
        return event

    def own_step(step, carry):
        polar.form_gram()
        polar.apply()
        at(step, [(turn, group(turn)) for turn in range(min(c, POLAR))])
        return carry

    lax.fori_loop(0, POLAR, own_step, 0)
    for turn in range(POLAR, c):
        group(turn)()
    tensor = (whole[...] * math.sqrt(n)).T
    whole[...] = tensor
    own_columns[...] = whole[pl.ds(pl.multiple_of(p.o * q, q), q)]
    high, low = halves(tensor)
    turned[:, pl.ds(0, n)] = high
    turned[:, pl.ds(n, n)] = high
    turned[:, pl.ds(2 * n, n)] = low

    def half_rotate(pair, carry):
        both = bdot(turned[...], stacked[pair])
        for i in range(PAIR):
            w = pair * PAIR + i
            rows_of = pl.ds(pl.multiple_of(w * n, n), n)
            rights[rows_of, pl.ds(0, n)], rights[rows_of, pl.ds(n, n)] = halves(both[:, i * n:(i + 1) * n])
            pltpu.make_async_copy(rights.at[rows_of], half_out.at[rows_of], out_sems.at[w]).start()
        at(pair, [(0, turn_in(again, c - 1))])
        return carry

    lax.fori_loop(0, ops_here // PAIR, half_rotate, 0)
    for j in range(c):
        again.receive(j)
    save = pltpu.make_async_copy(again.landed, source_out, out_sems.at[ops_here])
    save.start()
    for w in range(ops_here):
        rows_of = pl.ds(w * n, n)
        pltpu.make_async_copy(rights.at[rows_of], half_out.at[rows_of], out_sems.at[w]).wait()
    fetch.drain()
    again.drain()
    for j in range(c):
        swap_cores(0, 1 - side, j).wait_send()
        swap_cores(1, side, j).wait_send()
        over(j).wait_send()
        gather(1, p.o, facing, j).wait_send()
        gather(0, p.o, mate, j).wait_send()
    save.wait()


def last_kernel(n, ops_here, chunks, source, half, columns, own_columns, rotated, block, cols, doubled, gram, halves_in, double,
                tail, products, in_sems, out_sems):
    def load(w):
        at = pl.ds(w * n, n)
        return pltpu.make_async_copy(half.at[at], halves_in.at[at], in_sems.at[w])

    def store(w):
        return pltpu.make_async_copy(products.at[w], rotated.at[w], out_sems.at[w])

    for w in range(ops_here):
        load(w).start()
    own_columns[...] = columns[...]
    polar = Polar(n, block, cols, doubled, gram)
    polar.normalise(jnp.concatenate([source[j] for j in range(chunks)], axis=1))

    def step(_, carry):
        polar.form_gram()
        polar.apply()
        return carry

    lax.fori_loop(0, POLAR, step, 0)
    wide = n - n % WIDE
    rest = n - wide
    high, low = halves(block[...] * math.sqrt(n))
    double[pl.ds(0, n)] = high[:, :wide]
    double[pl.ds(n, n)] = high[:, :wide]
    cols[:, pl.ds(0, wide)] = low[:, :wide]
    if rest:
        tail[pl.ds(0, n), pl.ds(0, rest)] = high[:, wide:]
        tail[pl.ds(0, n), pl.ds(rest, rest)] = low[:, wide:]
        tail[pl.ds(n, n), pl.ds(0, rest)] = high[:, wide:]
        tail[pl.ds(n, n), pl.ds(rest, rest)] = jnp.zeros((n, rest), BF16)

    def rotate(w, carry):
        load(w).wait()
        rows_of = pl.ds(pl.multiple_of(w * n, n), n)
        both = halves_in[rows_of]
        products[w, :, pl.ds(0, wide)] = bdot(both, double[...]) + bdot(both[:, :n], cols[:, pl.ds(0, wide)])
        if rest:
            ends = bdot(both, tail[...])
            products[w, :, pl.ds(wide, rest)] = ends[:, :rest] + ends[:, rest:]
        store(w).start()
        return carry

    lax.fori_loop(0, ops_here, rotate, 0)
    for w in range(ops_here):
        store(w).wait()


def vmem():
    return pl.BlockSpec(memory_space=pltpu.VMEM)


def scalar():
    return pl.BlockSpec(memory_space=pltpu.SMEM)


def anywhere():
    return pl.BlockSpec(memory_space=pl.ANY)


def shards_planes(place, wavefunction, left_env, right_env, shift_map, op_counts):
    c, n, q, ops_here = place.chunks, place.states, place.quarter, left_env.shape[1]
    fetches = []
    for _ in range(2):
        held, stage, *sems = Fetch.scratch(place)
        fetches += [*held, stage, *sems, pltpu.VMEM((c, n, LANES), F32)]
    columns, half, source = pl.pallas_call(
        functools.partial(site_kernel, place, ops_here),
        out_shape=(
            jax.ShapeDtypeStruct((q, n), F32),
            jax.ShapeDtypeStruct((ops_here * n, 2 * n), BF16),
            jax.ShapeDtypeStruct((c, n, LANES), F32),
        ),
        in_specs=[anywhere(), anywhere(), anywhere(), scalar(), scalar()],
        out_specs=(vmem(), anywhere(), anywhere()),
        scratch_shapes=[
            *Maps.scratch(place), *fetches,
            pltpu.VMEM((ops_here * n, 2 * n), BF16),
            pltpu.VMEM((ops_here * n, 2 * n), BF16),
            pltpu.VMEM((2 * n, 2 * LANES), BF16),
            pltpu.VMEM((2, n, n), F32),
            pltpu.SemaphoreType.DMA((2,)),
            pltpu.VMEM((n, ops_here * LANES), BF16),
            pltpu.VMEM((n, ops_here * LANES), BF16),
            pltpu.VMEM((n, n), F32),
            pltpu.VMEM((2, q, n), F32),
            pltpu.VMEM((q, n), F32),
            pltpu.VMEM((q, n), F32),
            pltpu.SemaphoreType.DMA((2, 3, c)),
            pltpu.VMEM((q, n), F32),
            pltpu.SemaphoreType.DMA((2, 3, c)),
            pltpu.VMEM((n, n), F32),
            *Polar.scratch(n),
            pltpu.VMEM((ops_here // PAIR, 3 * n, PAIR * n), BF16),
            pltpu.VMEM((n, 3 * n), BF16),
            pltpu.SemaphoreType.DMA((ops_here + 1,)),
        ],
        compiler_params=pltpu.CompilerParams(collective_id=0, has_side_effects=True, vmem_limit_bytes=60 * 2**20),
    )(wavefunction[0], left_env[0], right_env[0], shift_map, op_counts)
    own_columns, rotated = pl.pallas_call(
        functools.partial(last_kernel, n, ops_here, c),
        out_shape=(jax.ShapeDtypeStruct((q, n), F32), jax.ShapeDtypeStruct((ops_here, n, n), F32)),
        in_specs=[vmem(), anywhere(), vmem()],
        out_specs=(vmem(), anywhere()),
        scratch_shapes=[
            pltpu.VMEM((n, n), F32),
            *Polar.scratch(n),
            pltpu.VMEM((ops_here * n, 2 * n), BF16),
            pltpu.VMEM((2 * n, n - n % WIDE), BF16),
            pltpu.VMEM((2 * n, 2 * max(n % WIDE, LANES)), BF16),
            pltpu.VMEM((ops_here, n, n), F32),
            pltpu.SemaphoreType.DMA((ops_here,)),
            pltpu.SemaphoreType.DMA((ops_here,)),
        ],
        compiler_params=pltpu.CompilerParams(vmem_limit_bytes=60 * 2**20),
    )(source, half, columns)
    return own_columns.T[None], rotated[None]


def line_split(sector_count):
    rows = 1
    while rows * 2 * rows * 2 <= sector_count and sector_count % (rows * 2) == 0:
        rows *= 2
    return rows


def solution(mesh):
    def shards(wavefunction, left_env, right_env, shift_map, op_counts):
        nsec, nops = mesh.shape["sector"], mesh.shape["ops"]
        states = wavefunction.shape[1]
        ny = line_split(nsec)
        per_group = left_env.shape[1] % PAIR == 0
        fits = per_group and nops == 2 * CORES and ny == 2 and states % LANES == 0 and states % (nops * ny * SUBLANES) == 0
        if not fits:
            return shards_general(wavefunction, left_env, right_env, shift_map, op_counts)
        place = Place(nsec, nops, ny, states)
        return shards_planes(place, wavefunction, left_env, right_env, shift_map, op_counts)

    return jax.shard_map(
        shards,
        mesh=mesh,
        in_specs=(
            P("sector", None, None),
            P("sector", "ops", None, None),
            P("sector", "ops", None, None),
            P("ops", None),
            P("ops", "sector"),
        ),
        out_specs=(P("sector", None, "ops"), P("sector", "ops", None, None)),
        check_vma=False,
    )
```

```python
import functools
import math

import jax
import jax.numpy as jnp
from jax import lax
from jax.experimental import pallas as pl
from jax.experimental.pallas import tpu as pltpu
from jax.sharding import PartitionSpec as P

POLAR = 5
LANES, SUBLANES = 128, 8
CORES = 2
AHEAD = 2
WIDE = 256
PAIR = 2
MESH = pl.DeviceIdType.MESH
F32, BF16 = jnp.float32, jnp.bfloat16

precise = lax.Precision.HIGH


def dot(a, b):
    return jnp.dot(a, b, precision=precise, preferred_element_type=jnp.float32)


def to_tiles(block, padded):
    rows, cols = block.shape
    tiles = block.reshape(rows // SUBLANES, SUBLANES, cols // LANES, LANES)
    tiles = tiles.transpose(0, 2, 1, 3).reshape(rows * cols // (SUBLANES * LANES), SUBLANES, LANES)
    return jnp.pad(tiles, ((0, padded - tiles.shape[0]), (0, 0), (0, 0)))


def from_tiles(tiles, rows, cols):
    tiles = tiles[: rows * cols // (SUBLANES * LANES)]
    tiles = tiles.reshape(rows // SUBLANES, cols // LANES, SUBLANES, LANES)
    return tiles.transpose(0, 2, 1, 3).reshape(rows, cols)


def swap(value, axis, bit):
    size = lax.axis_size(axis)
    return lax.ppermute(value, axis, [(i, i ^ bit) for i in range(size)])


def sum_scatter(tiles, axis):
    size, here = lax.axis_size(axis), lax.axis_index(axis)
    rest = tiles.reshape((size, tiles.shape[0] // size) + tiles.shape[1:])
    bit = 1
    while bit < size:
        mine = (here // bit) % 2
        pairs = rest.reshape((rest.shape[0] // 2, 2) + rest.shape[1:])
        keep = lax.dynamic_index_in_dim(pairs, mine, 1, keepdims=False)
        give = lax.dynamic_index_in_dim(pairs, 1 - mine, 1, keepdims=False)
        rest = keep + swap(give, axis, bit)
        bit *= 2
    return rest[0]


def gather_whole(quarter, axis):
    size, here = lax.axis_size(axis), lax.axis_index(axis)
    held = quarter[None]
    bit = size // 2
    while bit:
        mine = (here // bit) % 2
        other = swap(held, axis, bit)
        first = jnp.where(mine == 0, held, other)
        second = jnp.where(mine == 0, other, held)
        held = jnp.stack([first, second], axis=1).reshape((-1,) + quarter.shape)
        bit //= 2
    return held.reshape((-1,) + quarter.shape[1:])


def polar(sigma_block):
    states = sigma_block.shape[0]
    mean_sq = jnp.sum(sigma_block * sigma_block) / float(states * states)
    iterate = sigma_block * (lax.rsqrt(states * mean_sq + 1e-06) / 2.2)

    def step(_, iterate):
        gram_matrix = jnp.einsum("ab,cb->ac", iterate, iterate, precision=precise)
        return 1.5 * iterate - 0.5 * dot(gram_matrix, iterate)

    return lax.fori_loop(0, POLAR, step, iterate) * math.sqrt(states)


def shards_general(wavefunction, left_env, right_env, shift_map, op_counts):
    sector_count = lax.axis_size("sector")
    group_size = lax.axis_size("ops")
    group_here = lax.axis_index("ops")
    states = wavefunction.shape[1]
    ops_here = left_env.shape[1]
    parts = sector_count * group_size
    piece = -(-states * states // (SUBLANES * LANES * parts))
    padded = piece * parts
    quarter = piece * sector_count

    whole_map = lax.all_gather(shift_map[0], "ops").reshape(parts)

    def fetch_from_quarter(own_quarter):
        pieces = own_quarter.reshape(sector_count, piece, SUBLANES, LANES)
        spread = lax.all_to_all(pieces, "sector", split_axis=0, concat_axis=0, tiled=True)
        picked = jnp.take(spread, whole_map, axis=0)
        landed = lax.all_to_all(picked, ("ops", "sector"), split_axis=0, concat_axis=0, tiled=True)
        return from_tiles(landed.reshape(padded, SUBLANES, LANES), states, states)

    psi_tiles = to_tiles(wavefunction[0], padded)
    psi_quarter = lax.dynamic_slice_in_dim(psi_tiles, group_here * quarter, quarter, 0)
    moved_block = fetch_from_quarter(psi_quarter)

    left, right = left_env[0], right_env[0]
    count = op_counts[0, 0]
    active = (jnp.arange(ops_here) < count).astype(jnp.float32)
    left_psi = jnp.einsum("wab,bc->wac", left, moved_block, precision=precise) * active[:, None, None]
    partial_sigma = jnp.einsum("wac,wcd->ad", left_psi, right, precision=precise)

    sigma_quarter = sum_scatter(to_tiles(partial_sigma, padded), "ops")
    source_sigma = fetch_from_quarter(sigma_quarter)
    sigma_block = from_tiles(gather_whole(sigma_quarter, "ops"), states, states)

    whole_tensor = polar(sigma_block)
    column_width = states // group_size
    own_columns = lax.dynamic_slice_in_dim(whole_tensor, group_here * column_width, column_width, 1)
    half_rotated = jnp.einsum("ba,wbc->wac", whole_tensor, left, precision=precise)
    source_tensor = polar(source_sigma)
    rotated = jnp.einsum("wac,cd->wad", half_rotated, source_tensor, precision=precise)
    return (own_columns[None], rotated[None])


def halves(value):
    high = value.astype(BF16)
    return high, (value - high.astype(F32)).astype(BF16)


def bdot(a, b):
    return jnp.dot(a, b, preferred_element_type=F32)


class Place:
    def __init__(self, nsec, nops, ny, states):
        self.nsec, self.nops, self.ny, self.nz = nsec, nops, ny, nsec // ny
        self.states = states
        self.chunks = states // LANES
        self.parts = nops * ny
        self.rows = states // self.parts
        self.quarter = states // nops
        self.dests = nops * ny

    def locate(self):
        self.s, self.o = lax.axis_index("sector"), lax.axis_index("ops")
        self.z, self.y = self.s // self.ny, lax.rem(self.s, self.ny)
        self.part = self.o * self.ny + self.y

    def plane_peer(self, index, sign=1):
        dy, do = index // self.nops, index % self.nops
        if sign < 0:
            dy, do = (self.ny - dy) % self.ny, (self.nops - do) % self.nops
        return lax.rem(self.y + dy, self.ny), lax.rem(self.o + do, self.nops)

    def greet(self):
        barrier = pltpu.get_barrier_semaphore()
        for index in range(1, self.dests):
            y, o = self.plane_peer(index)
            pl.semaphore_signal(barrier, inc=1, device_id=(self.z * self.ny + y, o), device_id_type=MESH)

        @pl.when(self.z > 0)
        def _():
            pl.semaphore_signal(barrier, inc=1, device_id=(self.s - self.ny, self.o), device_id_type=MESH)

        @pl.when(self.z < self.nz - 1)
        def _():
            pl.semaphore_signal(barrier, inc=1, device_id=(self.s + self.ny, self.o), device_id_type=MESH)

        line = (self.z > 0).astype(jnp.int32) + (self.z < self.nz - 1).astype(jnp.int32)
        pl.semaphore_wait(barrier, self.dests - 1 + line)


class Maps:
    def __init__(self, place, table, own_ref, rows_ref, scalars_ref, sems):
        self.place, self.table = place, table
        self.own, self.rows, self.scalars, self.sems = own_ref, rows_ref, scalars_ref, sems

    @staticmethod
    def scratch(place):
        return [
            pltpu.VMEM((1, LANES), jnp.int32),
            pltpu.VMEM((place.nops, 1, LANES), jnp.int32),
            pltpu.SMEM((place.nops, 1, LANES), jnp.int32),
            pltpu.SemaphoreType.DMA((3, place.nops)),
        ]

    def write(self):
        lane = lax.broadcasted_iota(jnp.int32, (1, LANES), 1)
        row = jnp.zeros((1, LANES), jnp.int32)
        for sector in range(self.place.nsec):
            row = jnp.where(lane == sector, self.table[0, sector], row)
        self.own[...] = row

    def copy(self, offset, sign):
        p = self.place
        peer = lax.rem(p.o + offset, p.nops)
        slot = p.o if sign > 0 else lax.rem(p.o + p.nops - offset, p.nops)
        return pltpu.make_async_remote_copy(
            self.own, self.rows.at[slot], self.sems.at[0, offset], self.sems.at[1, offset],
            device_id=(p.s, peer), device_id_type=MESH)

    def start(self):
        for offset in range(1, self.place.nops):
            self.copy(offset, 1).start()
        pltpu.make_async_copy(self.own, self.rows.at[self.place.o], self.sems.at[2, 0]).start()

    def finish(self):
        for offset in range(1, self.place.nops):
            self.copy(offset, 1).wait_send()
            self.copy(offset, -1).wait_recv()
        pltpu.make_async_copy(self.own, self.rows.at[self.place.o], self.sems.at[2, 0]).wait()
        landed = pltpu.make_async_copy(self.rows, self.scalars, self.sems.at[2, 1])
        landed.start()
        landed.wait()

    def want(self, y, o):
        return self.scalars[o, 0, self.place.z * self.place.ny + y]


class Fetch:
    def __init__(self, place, maps, piece, held, stage, landed, up, down, across, within, local):
        self.place, self.maps, self.piece = place, maps, piece
        self.held, self.stage, self.landed = held, stage, landed
        self.up, self.down, self.across, self.within, self.local = up, down, across, within, local

    @staticmethod
    def scratch(place):
        c, dma = place.chunks, pltpu.SemaphoreType.DMA
        return (
            [pltpu.VMEM((place.nsec, place.rows, LANES), F32) for _ in range(c)],
            pltpu.VMEM((c, place.dests, place.rows, LANES), F32),
            dma((2, c, place.nz - 1)),
            dma((2, c, place.nz - 1)),
            dma((2, c, place.ny)),
            dma((2, c, place.dests)),
            dma((c,)),
        )

    def across_copy(self, j, dy, sign):
        p = self.place
        y = lax.rem(p.y + dy, p.ny)
        slot = p.s if sign > 0 else p.z * p.ny + lax.rem(p.y + p.ny - dy, p.ny)
        return pltpu.make_async_remote_copy(
            self.piece(j, y), self.held[j].at[slot], self.across.at[0, j, dy], self.across.at[1, j, dy],
            device_id=(p.z * p.ny + y, p.o), device_id_type=MESH)

    def own_copy(self, j):
        p = self.place
        return pltpu.make_async_copy(self.piece(j, p.y), self.held[j].at[p.s], self.local.at[j])

    def begin(self, j):
        for dy in range(1, self.place.ny):
            self.across_copy(j, dy, 1).start()
        self.own_copy(j).start()

    def line_copy(self, j, k, direction):
        p = self.place
        slab = self.held[j].at[pl.ds((p.z - direction * k) * p.ny, p.ny)]
        sems = self.up if direction > 0 else self.down
        return pltpu.make_async_remote_copy(
            slab, slab, sems.at[0, j, k], sems.at[1, j, k],
            device_id=(p.s + direction * p.ny, p.o), device_id_type=MESH)

    def line_wait(self, j, k, direction):
        p = self.place
        slab = self.held[j].at[pl.ds((p.z - direction * k) * p.ny, p.ny)]
        sems = self.up if direction > 0 else self.down
        pltpu.make_async_remote_copy(
            slab, slab, sems.at[0, j, k - 1], sems.at[1, j, k - 1],
            device_id=(p.s - direction * p.ny, p.o), device_id_type=MESH).wait_recv()

    def has(self, k, direction):
        return self.place.z >= k if direction > 0 else self.place.z < self.place.nz - k

    def more(self, direction):
        return self.place.z < self.place.nz - 1 if direction > 0 else self.place.z > 0

    def send_own(self, j):
        for dy in range(1, self.place.ny):
            self.across_copy(j, dy, -1).wait_recv()
        self.own_copy(j).wait()
        for direction in (1, -1):
            @pl.when(self.more(direction))
            def _():
                self.line_copy(j, 0, direction).start()

    def forward(self, j, k):
        for direction in (1, -1):
            @pl.when(self.has(k, direction))
            def _():
                self.line_wait(j, k, direction)

            if k < self.place.nz - 1:
                @pl.when(self.has(k, direction) & self.more(direction))
                def _():
                    self.line_copy(j, k, direction).start()

    def within_copy(self, j, index, sign):
        p = self.place
        y, o = p.plane_peer(index, sign)
        part = p.part if sign > 0 else o * p.ny + y
        return pltpu.make_async_remote_copy(
            self.stage.at[j, index], self.landed.at[j, pl.ds(part * p.rows, p.rows)],
            self.within.at[0, j, index], self.within.at[1, j, index],
            device_id=(p.z * p.ny + y, o), device_id_type=MESH)

    def hand_out(self, j):
        p = self.place
        order = sorted(range(p.dests), key=lambda index: -((index // p.nops > 0) + (index % p.nops > 0)))
        for index in order:
            y, o = p.plane_peer(index)
            picked = self.held[j][self.maps.want(y, o)]
            if index == 0:
                self.landed[j, pl.ds(p.part * p.rows, p.rows)] = picked
            else:
                self.stage[j, index] = picked
        for index in order:
            if index:
                self.within_copy(j, index, 1).start()

    def receive(self, j):
        for index in range(1, self.place.dests):
            self.within_copy(j, index, -1).wait_recv()

    def drain(self):
        for j in range(self.place.chunks):
            for dy in range(1, self.place.ny):
                self.across_copy(j, dy, 1).wait_send()
            for direction in (1, -1):
                for k in range(self.place.nz - 1):
                    @pl.when(self.has(k, direction) & self.more(direction))
                    def _():
                        self.line_copy(j, k, direction).wait_send()
            for index in range(1, self.place.dests):
                self.within_copy(j, index, 1).wait_send()


def tdot(a, b):
    return lax.dot_general(a, b, (((1,), (1,)), ((), ())), preferred_element_type=F32)


class Polar:
    def __init__(self, n, block, cols, rows, gram):
        self.n, self.block, self.cols, self.rows, self.gram = n, block, cols, rows, gram

    @staticmethod
    def scratch(n):
        return [pltpu.VMEM((n, 2 * n), BF16), pltpu.VMEM((2 * n, n), BF16), pltpu.VMEM((2 * n, n), BF16)]

    def normalise(self, sigma):
        n = self.n
        squares = jnp.sum(jnp.sum(sigma * sigma, axis=0, keepdims=True), axis=1, keepdims=True)
        self.block[...] = sigma * (lax.rsqrt(n * (squares / float(n * n)) + 1e-06) / 2.2)

    def form_gram(self):
        n = self.n
        high, low = halves(self.block[...])
        self.cols[:, pl.ds(0, n)] = high
        self.cols[:, pl.ds(n, n)] = low
        self.rows[pl.ds(0, n)] = high
        self.rows[pl.ds(n, n)] = low
        both = tdot(high, self.rows[...])
        cross = both[:, n:]
        self.gram[pl.ds(0, n)], self.gram[pl.ds(n, n)] = halves(both[:, :n] + (cross + cross.T))

    def apply(self, scale=None):
        n = self.n
        both = bdot(self.gram[pl.ds(0, n)], self.cols[...])
        moved = both[:, :n] + (both[:, n:] + bdot(self.gram[pl.ds(n, n)], self.cols[:, pl.ds(0, n)]))
        value = 1.5 * self.block[...] - 0.5 * moved
        self.block[...] = value if scale is None else value * scale


def site_kernel(place, ops_here, psi, left, right, table, counts, own_columns, half_out, source_out, map_row, rows,
                scalars, map_sems, *rest):
    c, n = place.chunks, place.states
    groups = []
    for _ in range(2):
        groups.append((rest[:c], rest[c:c + 6], rest[c + 6]))
        rest = rest[c + 7:]
    (lefts, rights, block, envs, env_sems, lp_high, lp_low, sigma, first, second, pair, sum_sems,
     quarter, gather_sems, polar_block, cols, doubled, gram, stacked, turned, out_sems) = rest
    place.locate()
    p = place

    def load(ref, w):
        slot = w % 2 if isinstance(w, int) else lax.rem(w, 2)
        return pltpu.make_async_copy(ref.at[w], envs.at[slot], env_sems.at[slot])

    load(left, 0).start()
    load(left, 1).start()
    maps = Maps(place, table, map_row, rows, scalars, map_sems)
    maps.write()
    place.greet()

    def fetch_of(piece, group):
        held, (stage, up, down, across, within, local), landed = group
        return Fetch(place, maps, piece, held, stage, landed, up, down, across, within, local)

    fetch = fetch_of(lambda j, y: psi.at[pl.ds((p.o * p.ny + y) * p.rows, p.rows), pl.ds(j * LANES, LANES)], groups[0])
    again = fetch_of(lambda j, y: quarter.at[pl.ds(y * p.rows, p.rows), pl.ds(j * LANES, LANES)], groups[1])
    maps.start()
    for j in range(c):
        fetch.begin(j)
    for j in range(min(AHEAD, c)):
        fetch.send_own(j)
    count = counts[0, 0]
    sigma[...] = jnp.zeros((n, n), F32)
    block[pl.ds(n, n), pl.ds(LANES, LANES)] = jnp.zeros((n, LANES), BF16)

    def at(index, events):
        for turn, event in events:
            pl.when(index == turn)(event)

    def line(which, *steps):
        def event():
            for j, k in steps:
                if j < c:
                    which.send_own(j) if k == 0 else which.forward(j, k)
        return event

    def turn_in(which, j):
        def event():
            if j < c:
                which.forward(j, p.nz - 1)
                which.hand_out(j)
        return event

    def middle(j):
        return [(j, k) for k in range(2, p.nz - 1)]

    def convert_left(w, carry):
        load(left, w).wait()
        high, low = halves(envs[lax.rem(w, 2)])
        rows_of = pl.ds(pl.multiple_of(w * n, n), n)
        lefts[rows_of, pl.ds(0, n)] = high
        lefts[rows_of, pl.ds(n, n)] = low
        beside = pl.ds(pl.multiple_of(lax.rem(w, PAIR) * n, LANES), n)
        for third, value in enumerate((high, low, high)):
            stacked[w // PAIR, pl.ds(third * n, n), beside] = value

        @pl.when(w < ops_here - 2)
        def _():
            load(left, w + 2).start()

        @pl.when(w >= ops_here - 2)
        def _():
            load(right, w + 2 - ops_here).start()

        at(w, [(0, line(fetch, (0, 1))), (2, line(fetch, (AHEAD, 0), (1, 1))), (2, maps.finish)])
        return carry

    def convert_right(w, carry):
        load(right, w).wait()
        high, low = halves(envs[lax.rem(w, 2)] * (w < count).astype(F32))
        for j in range(c):
            rows_of = pl.ds(pl.multiple_of((j * ops_here + w) * LANES, LANES), LANES)
            rights[rows_of, pl.ds(0, n)] = high[j * LANES:(j + 1) * LANES]
            rights[rows_of, pl.ds(n, n)] = low[j * LANES:(j + 1) * LANES]

        @pl.when(w < ops_here - 2)
        def _():
            load(right, w + 2).start()

        at(w, [(0, line(fetch, *middle(0))), (1, line(fetch, (AHEAD + 1, 0), (2, 1))), (3, line(fetch, *middle(1)))])
        return carry

    lax.fori_loop(0, ops_here, convert_left, 0)
    lax.fori_loop(0, ops_here, convert_right, 0)
    for j in range(AHEAD + 2, c):
        fetch.send_own(j)
    turn_in(fetch, 0)()

    side, core = p.o // CORES, lax.rem(p.o, CORES)
    mate = side * CORES + 1 - core
    facing = (1 - side) * CORES + core
    across_mate = (1 - side) * CORES + 1 - core
    q = p.quarter

    def swap_cores(i, far, j):
        rows_of, at_cols = pl.ds((far * CORES + 1 - core) * q, q), pl.ds(j * LANES, LANES)
        return pltpu.make_async_remote_copy(
            sigma.at[rows_of, at_cols], first.at[i, :, at_cols], sum_sems.at[0, i, j], sum_sems.at[1, i, j],
            device_id=(p.s, mate), device_id_type=MESH)

    def products(j, carry):
        for turn in range(c):
            @pl.when(j == turn)
            def _():
                line(fetch, (turn + 3, 1), *middle(turn + 2))()
                if turn < c - 2:
                    turn_in(fetch, turn + 1)()
                fetch.receive(turn)

        high, low = halves(fetch.landed[j])
        block[pl.ds(0, n), pl.ds(0, LANES)] = high
        block[pl.ds(n, n), pl.ds(0, LANES)] = high
        block[pl.ds(0, n), pl.ds(LANES, LANES)] = low
        for w in range(ops_here):
            both = bdot(lefts[pl.ds(w * n, n)], block[...])
            high, low = halves(both[:, :LANES] + both[:, LANES:])
            lp_high[:, pl.ds(w * LANES, LANES)] = high
            lp_low[:, pl.ds(w * LANES, LANES)] = low

        @pl.when(j == max(c - 3, 0))
        def _():
            if c > 1:
                turn_in(fetch, c - 1)()

        deep = pl.ds(pl.multiple_of(j * ops_here * LANES, LANES), ops_here * LANES)
        for i, far in ((0, 1 - side), (1, side)):
            half = pl.ds(pl.multiple_of(far * (n // 2), 2 * SUBLANES), n // 2)
            both = bdot(lp_high[half], rights[deep])
            sigma[half] += both[:, :n] + (both[:, n:] + bdot(lp_low[half], rights[deep, pl.ds(0, n)]))

            @pl.when(j == c - 1)
            def _():
                for chunk in range(c):
                    swap_cores(i, far, chunk).start()
        return carry

    lax.fori_loop(0, c, products, 0)

    whole = polar_block
    polar = Polar(n, whole, cols, doubled, gram)

    def over(j):
        at_cols = pl.ds(j * LANES, LANES)
        return pltpu.make_async_remote_copy(
            pair.at[:, at_cols], second.at[:, at_cols], sum_sems.at[0, 2, j], sum_sems.at[1, 2, j],
            device_id=(p.s, facing), device_id_type=MESH)

    def gather(i, sender, target, j):
        rows_of, at_cols = pl.ds(sender * q, q), pl.ds(j * LANES, LANES)
        source = quarter.at[:, at_cols] if i < 2 else whole.at[rows_of, at_cols]
        return pltpu.make_async_remote_copy(
            source, whole.at[rows_of, at_cols], gather_sems.at[0, i, j], gather_sems.at[1, i, j],
            device_id=(p.s, target), device_id_type=MESH)

    for j in range(c + 1):
        if j < c:
            at_cols = pl.ds(j * LANES, LANES)
            swap_cores(0, 1 - side, j).wait_recv()
            pair[:, at_cols] = sigma[pl.ds(((1 - side) * CORES + core) * q, q), at_cols] + first[0, :, at_cols]
        if j:
            over(j - 1).start()
    for j in range(c + 1):
        if j < c:
            at_cols = pl.ds(j * LANES, LANES)
            swap_cores(1, side, j).wait_recv()
            over(j).wait_recv()
            quarter[:, at_cols] = sigma[pl.ds(p.o * q, q), at_cols] + first[1, :, at_cols] + second[:, at_cols]
            whole[pl.ds(p.o * q, q), at_cols] = quarter[:, at_cols]
        if j:
            again.begin(j - 1)
            gather(1, p.o, facing, j - 1).start()
            gather(0, p.o, mate, j - 1).start()
        if j > 1:
            again.send_own(j - 2)
    again.send_own(c - 1)
    for j in range(c):
        gather(1, facing, facing, j).wait_recv()
        gather(2, facing, mate, j).start()
        again.forward(j, 1)
    line(again, *middle(0))()
    for j in range(c):
        gather(0, mate, mate, j).wait_recv()
        gather(2, across_mate, mate, j).wait_recv()
        gather(2, facing, mate, j).wait_send()
    polar.normalise(whole[...])

    def group(turn):
        def event():
            line(again, *(middle(1) if turn == 0 else []), *middle(turn + 2))()
            if turn:
                turn_in(again, turn - 1)()
        return event

    def own_step(step, carry):
        polar.form_gram()
        polar.apply()
        at(step, [(turn, group(turn)) for turn in range(min(c, POLAR))])
        return carry

    lax.fori_loop(0, POLAR, own_step, 0)
    for turn in range(POLAR, c):
        group(turn)()
    tensor = (whole[...] * math.sqrt(n)).T
    whole[...] = tensor
    own_columns[...] = whole[pl.ds(pl.multiple_of(p.o * q, q), q)]
    high, low = halves(tensor)
    turned[:, pl.ds(0, n)] = high
    turned[:, pl.ds(n, n)] = high
    turned[:, pl.ds(2 * n, n)] = low

    def half_rotate(pair, carry):
        both = bdot(turned[...], stacked[pair])
        for i in range(PAIR):
            w = pair * PAIR + i
            rows_of = pl.ds(pl.multiple_of(w * n, n), n)
            rights[rows_of, pl.ds(0, n)], rights[rows_of, pl.ds(n, n)] = halves(both[:, i * n:(i + 1) * n])
            pltpu.make_async_copy(rights.at[rows_of], half_out.at[rows_of], out_sems.at[w]).start()
        at(pair, [(0, turn_in(again, c - 1))])
        return carry

    lax.fori_loop(0, ops_here // PAIR, half_rotate, 0)
    for j in range(c):
        again.receive(j)
    save = pltpu.make_async_copy(again.landed, source_out, out_sems.at[ops_here])
    save.start()
    for w in range(ops_here):
        rows_of = pl.ds(w * n, n)
        pltpu.make_async_copy(rights.at[rows_of], half_out.at[rows_of], out_sems.at[w]).wait()
    fetch.drain()
    again.drain()
    for j in range(c):
        swap_cores(0, 1 - side, j).wait_send()
        swap_cores(1, side, j).wait_send()
        over(j).wait_send()
        gather(1, p.o, facing, j).wait_send()
        gather(0, p.o, mate, j).wait_send()
    save.wait()


def last_kernel(n, ops_here, chunks, source, half, columns, own_columns, rotated, block, cols, doubled, gram, halves_in, double,
                tail, products, in_sems, out_sems):
    def load(w):
        at = pl.ds(w * n, n)
        return pltpu.make_async_copy(half.at[at], halves_in.at[at], in_sems.at[w])

    def store(w, part):
        rows_of = pl.ds(part * (n // 2), n // 2)
        return pltpu.make_async_copy(products.at[w, rows_of], rotated.at[w, rows_of], out_sems.at[w, part])

    for w in range(ops_here):
        load(w).start()
    own_columns[...] = columns[...]
    polar = Polar(n, block, cols, doubled, gram)
    polar.normalise(jnp.concatenate([source[j] for j in range(chunks)], axis=1))

    def step(_, carry):
        polar.form_gram()
        polar.apply()
        return carry

    lax.fori_loop(0, POLAR, step, 0)
    wide = n - n % WIDE
    rest = n - wide
    high, low = halves(block[...] * math.sqrt(n))
    double[pl.ds(0, n)] = high[:, :wide]
    double[pl.ds(n, n)] = high[:, :wide]
    cols[:, pl.ds(0, wide)] = low[:, :wide]
    if rest:
        tail[pl.ds(0, n), pl.ds(0, rest)] = high[:, wide:]
        tail[pl.ds(0, n), pl.ds(rest, rest)] = low[:, wide:]
        tail[pl.ds(n, n), pl.ds(0, rest)] = high[:, wide:]
        tail[pl.ds(n, n), pl.ds(rest, rest)] = jnp.zeros((n, rest), BF16)

    def rotate(w, carry):
        load(w).wait()
        for part in range(2):
            rows_of = pl.ds(pl.multiple_of(w * n + part * (n // 2), n // 2), n // 2)
            here = pl.ds(part * (n // 2), n // 2)
            both = halves_in[rows_of]
            products[w, here, pl.ds(0, wide)] = bdot(both, double[...]) + bdot(both[:, :n], cols[:, pl.ds(0, wide)])
            if rest:
                ends = bdot(both, tail[...])
                products[w, here, pl.ds(wide, rest)] = ends[:, :rest] + ends[:, rest:]
            store(w, part).start()
        return carry

    lax.fori_loop(0, ops_here, rotate, 0)
    for w in range(ops_here):
        for part in range(2):
            store(w, part).wait()


def vmem():
    return pl.BlockSpec(memory_space=pltpu.VMEM)


def scalar():
    return pl.BlockSpec(memory_space=pltpu.SMEM)


def anywhere():
    return pl.BlockSpec(memory_space=pl.ANY)


def shards_planes(place, wavefunction, left_env, right_env, shift_map, op_counts):
    c, n, q, ops_here = place.chunks, place.states, place.quarter, left_env.shape[1]
    fetches = []
    for _ in range(2):
        held, stage, *sems = Fetch.scratch(place)
        fetches += [*held, stage, *sems, pltpu.VMEM((c, n, LANES), F32)]
    columns, half, source = pl.pallas_call(
        functools.partial(site_kernel, place, ops_here),
        out_shape=(
            jax.ShapeDtypeStruct((q, n), F32),
            jax.ShapeDtypeStruct((ops_here * n, 2 * n), BF16),
            jax.ShapeDtypeStruct((c, n, LANES), F32),
        ),
        in_specs=[anywhere(), anywhere(), anywhere(), scalar(), scalar()],
        out_specs=(vmem(), anywhere(), anywhere()),
        scratch_shapes=[
            *Maps.scratch(place), *fetches,
            pltpu.VMEM((ops_here * n, 2 * n), BF16),
            pltpu.VMEM((ops_here * n, 2 * n), BF16),
            pltpu.VMEM((2 * n, 2 * LANES), BF16),
            pltpu.VMEM((2, n, n), F32),
            pltpu.SemaphoreType.DMA((2,)),
            pltpu.VMEM((n, ops_here * LANES), BF16),
            pltpu.VMEM((n, ops_here * LANES), BF16),
            pltpu.VMEM((n, n), F32),
            pltpu.VMEM((2, q, n), F32),
            pltpu.VMEM((q, n), F32),
            pltpu.VMEM((q, n), F32),
            pltpu.SemaphoreType.DMA((2, 3, c)),
            pltpu.VMEM((q, n), F32),
            pltpu.SemaphoreType.DMA((2, 3, c)),
            pltpu.VMEM((n, n), F32),
            *Polar.scratch(n),
            pltpu.VMEM((ops_here // PAIR, 3 * n, PAIR * n), BF16),
            pltpu.VMEM((n, 3 * n), BF16),
            pltpu.SemaphoreType.DMA((ops_here + 1,)),
        ],
        compiler_params=pltpu.CompilerParams(collective_id=0, has_side_effects=True, vmem_limit_bytes=60 * 2**20),
    )(wavefunction[0], left_env[0], right_env[0], shift_map, op_counts)
    own_columns, rotated = pl.pallas_call(
        functools.partial(last_kernel, n, ops_here, c),
        out_shape=(jax.ShapeDtypeStruct((q, n), F32), jax.ShapeDtypeStruct((ops_here, n, n), F32)),
        in_specs=[vmem(), anywhere(), vmem()],
        out_specs=(vmem(), anywhere()),
        scratch_shapes=[
            pltpu.VMEM((n, n), F32),
            *Polar.scratch(n),
            pltpu.VMEM((ops_here * n, 2 * n), BF16),
            pltpu.VMEM((2 * n, n - n % WIDE), BF16),
            pltpu.VMEM((2 * n, 2 * max(n % WIDE, LANES)), BF16),
            pltpu.VMEM((ops_here, n, n), F32),
            pltpu.SemaphoreType.DMA((ops_here,)),
            pltpu.SemaphoreType.DMA((ops_here, 2)),
        ],
        compiler_params=pltpu.CompilerParams(vmem_limit_bytes=60 * 2**20),
    )(source, half, columns)
    return own_columns.T[None], rotated[None]


def line_split(sector_count):
    rows = 1
    while rows * 2 * rows * 2 <= sector_count and sector_count % (rows * 2) == 0:
        rows *= 2
    return rows


def solution(mesh):
    def shards(wavefunction, left_env, right_env, shift_map, op_counts):
        nsec, nops = mesh.shape["sector"], mesh.shape["ops"]
        states = wavefunction.shape[1]
        ny = line_split(nsec)
        per_group = left_env.shape[1] % PAIR == 0
        fits = per_group and nops == 2 * CORES and ny == 2 and states % LANES == 0 and states % (nops * ny * SUBLANES) == 0
        if not fits:
            return shards_general(wavefunction, left_env, right_env, shift_map, op_counts)
        place = Place(nsec, nops, ny, states)
        return shards_planes(place, wavefunction, left_env, right_env, shift_map, op_counts)

    return jax.shard_map(
        shards,
        mesh=mesh,
        in_specs=(
            P("sector", None, None),
            P("sector", "ops", None, None),
            P("sector", "ops", None, None),
            P("ops", None),
            P("ops", "sector"),
        ),
        out_specs=(P("sector", None, "ops"), P("sector", "ops", None, None)),
        check_vma=False,
    )
```
